32 devices in a mesh: data: 4 (over x, y), stage: 8 (over z, core).
Axes of the slice: x: 2, y: 2, z: 4, core: 2. Of those that a mesh axis runs over, the one named last changes fastest.
Arguments:
- X: bfloat16 [32, 256, 768], P('data'), parts along dimension 0
- G: bfloat16 [32, 256, 768], P('data'), parts along dimension 0
- W1: bfloat16 [8, 768, 3072], P('stage')
- W2: bfloat16 [8, 3072, 768], P('stage')
Outputs:
- output 1: bfloat16 [32, 256, 768], P('data'), parts along dimension 0
- output 2: bfloat16 [32, 256, 768], P('data'), parts along dimension 0
- output 3: float32 [32, 768, 3072], P(('data', 'stage')), parts along dimension 0
- output 4: float32 [32, 3072, 768], P(('data', 'stage')), parts along dimension 0
There are 4 independent parts. The reference program is written for one: setup_inputs(seed, part) draws one part's arguments, and reference() takes and returns one part's arrays. A program takes and returns all parts, laid end to end along the dimension named above; an argument that names none is the same for every part.
All inputs are finite; a program needn't handle non-finite values.
Results may differ from the reference program's by a relative error of at most 0.0131113.
Values are sent between devices in bfloat16 or wider.
A program may use at most 1 GiB of HBM per device.

```python
import jax
import jax.numpy as jnp
from jax import lax

D = 768
F = 3072
LAYERS = 8
M = 8
B = 256


def setup_inputs(seed: int = 0, part: int = 0) -> dict:
    key = jax.random.PRNGKey(seed)
    ks, kpb = jax.random.split(key)
    kp = jax.random.fold_in(kpb, part)
    kx, kg = jax.random.split(kp)
    k1, k2 = jax.random.split(ks)
    X = jax.random.normal(kx, (M, B, D), jnp.float32).astype(jnp.bfloat16)
    G = jax.random.normal(kg, (M, B, D), jnp.float32).astype(jnp.bfloat16)
    W1 = (jax.random.normal(k1, (LAYERS, D, F), jnp.float32) * D ** -0.5).astype(jnp.bfloat16)
    W2 = (jax.random.normal(k2, (LAYERS, F, D), jnp.float32) * (F * LAYERS) ** -0.5).astype(jnp.bfloat16)
    return {'X': X, 'G': G, 'W1': W1, 'W2': W2}


def _fwd_layer(h, w1, w2):
    z = jnp.dot(h, w1, preferred_element_type=jnp.float32)
    u = jax.nn.gelu(z, approximate=True).astype(jnp.bfloat16)
    return (h.astype(jnp.float32) + jnp.dot(u, w2, preferred_element_type=jnp.float32)).astype(jnp.bfloat16)


def _bwd_layer(h, g, w1, w2):
    z = jnp.dot(h, w1, preferred_element_type=jnp.float32)
    u, gelu_vjp = jax.vjp(lambda t: jax.nn.gelu(t, approximate=True), z)
    du = jnp.dot(g, w2.T, preferred_element_type=jnp.float32)
    dz = gelu_vjp(du)[0].astype(jnp.bfloat16)
    dw2 = jnp.dot(u.astype(jnp.bfloat16).T, g, preferred_element_type=jnp.float32)
    dw1 = jnp.dot(h.T, dz, preferred_element_type=jnp.float32)
    dh = (g.astype(jnp.float32) + jnp.dot(dz, w1.T, preferred_element_type=jnp.float32)).astype(jnp.bfloat16)
    return dh, dw1, dw2


def reference(X, G, W1, W2):
    def one(carry, xg):
        a1, a2 = carry
        x, g = xg

        def fstep(h, w):
            return _fwd_layer(h, w[0], w[1]), h
        y, hs = lax.scan(fstep, x, (W1, W2))

        def bstep(gh, inp):
            w1, w2, h, c1, c2 = inp
            dh, dw1, dw2 = _bwd_layer(h, gh, w1, w2)
            return dh, (c1 + dw1, c2 + dw2)
        dx, (a1, a2) = lax.scan(bstep, g, (W1, W2, hs, a1, a2), reverse=True)
        return (a1, a2), (y, dx)

    init = (jnp.zeros(W1.shape, jnp.float32), jnp.zeros(W2.shape, jnp.float32))
    (dW1, dW2), (Y, dX) = lax.scan(one, init, (X, G))
    return Y, dX, dW1, dW2
```

```python
import functools

import jax
import jax.numpy as jnp
from jax import lax
from jax.experimental import pallas as pl
from jax.experimental.pallas import tpu as pltpu
from jax.sharding import PartitionSpec as P

MESH = pl.DeviceIdType.MESH
f32 = jnp.float32
bf16 = jnp.bfloat16
D = 768
F = 3072
C = 128
G = 2
RING = 4
TN = 512
C0 = 0.7978845608028654
C1 = 0.044715

WORDS = (
    (0, 204734464, 338466073, 156340875, 422098187, 579749972, 1073727780),
    (5, 555745280, 560252185, 428163866, 591762210, 577115404, 1073726668),
    (5, 203423744, 338466073, 439456395, 422098185, 609339476, 1073727780),
    (5, 153092096, 208187987, 591763554, 176531553, 579650841, 1073727780),
    (5, 404885504, 338465825, 438973003, 422098185, 343033940, 1073727780),
    (5, 134578696, 153944601, 439399514, 608999585, 613501137, 1073727780),
    (17858565, 137105675, 142872644, 189022728, 613553825, 323832100, 1073718483),
    (137105477, 17043544, 17043521, 445452353, 443168026, 613565716, 1073727780),
)
STEPS = 10


def _dot(a, b):
    return jnp.dot(a, b, preferred_element_type=f32)


def _dot_t(a, b):
    return lax.dot_general(a, b, (((0,), (0,)), ((), ())), preferred_element_type=f32)


def _when(cond):
    return pl.when(cond)


def _pipeline(n_st, n_ch, x, g, w1h, w2h, y, dx, a1, a2, zh, uh, dh,
              w1, w2, w1t, w2t, hb, gb, zb, ub, db, uw, dw, fo, bo,
              wsem, hsem, gsem, ysem, xsem, fsem, bsem, osem, rsem, zwsem, zrsem, udsem, rdsem):
    d = lax.axis_index("data")
    s = lax.axis_index("stage")
    last = n_st - 1
    spill = s < n_st - 2
    even = s % 2 == 0

    def peer(k):
        return (d, k)

    loads = [pltpu.make_async_copy(w1h.at[0], w1, wsem.at[0]), pltpu.make_async_copy(w2h.at[0], w2, wsem.at[1])]
    for c in loads:
        c.start()

    @_when(s == 0)
    def _():
        def f(i, _):
            pltpu.make_async_copy(x.at[i], hb.at[i], hsem.at[i]).start()
            return 0
        lax.fori_loop(0, n_ch, f, 0)

    @_when(s == last)
    def _():
        def f(i, _):
            pltpu.make_async_copy(g.at[i], gb.at[i], gsem.at[i]).start()
            return 0
        lax.fori_loop(0, n_ch, f, 0)

    bar = pltpu.get_barrier_semaphore()
    for off in (-2, -1, 1, 2):
        @_when((s + off >= 0) & (s + off < n_st))
        def _(off=off):
            pl.semaphore_signal(bar, inc=1, device_id=peer(s + off), device_id_type=MESH)
    peers = jnp.minimum(s, 2) + jnp.minimum(last - s, 2)
    pl.semaphore_wait(bar, peers)

    for c in loads:
        c.wait()

    def send_f(i, r):
        return pltpu.make_async_remote_copy(src_ref=fo.at[r], dst_ref=hb.at[i], send_sem=fsem.at[r], recv_sem=hsem.at[i],
                                            device_id=peer(s + 1), device_id_type=MESH)

    def send_y(i, r):
        return pltpu.make_async_remote_copy(src_ref=fo.at[r], dst_ref=y.at[i], send_sem=fsem.at[r], recv_sem=ysem.at[i],
                                            device_id=peer(s - 1), device_id_type=MESH)

    def own_y(i, r):
        return pltpu.make_async_copy(fo.at[r], y.at[i], osem.at[r])

    def send_b(i, r):
        return pltpu.make_async_remote_copy(src_ref=bo.at[r], dst_ref=gb.at[i], send_sem=bsem.at[r], recv_sem=gsem.at[i],
                                            device_id=peer(s - 1), device_id_type=MESH)

    def send_x(i, r):
        return pltpu.make_async_remote_copy(src_ref=bo.at[r], dst_ref=dx.at[i], send_sem=bsem.at[r], recv_sem=xsem.at[i],
                                            device_id=peer(s + 1), device_id_type=MESH)

    def own_x(i, r):
        return pltpu.make_async_copy(bo.at[r], dx.at[i], osem.at[r])

    def relay(ref, i, sem, k, dev):
        return pltpu.make_async_remote_copy(src_ref=ref.at[i], dst_ref=ref.at[i], send_sem=rsem.at[k, i], recv_sem=sem.at[i],
                                            device_id=peer(dev), device_id_type=MESH)

    def write_z(i):
        return pltpu.make_async_copy(zb.at[i % 2], zh.at[i], zwsem.at[i % 2])

    def read_z(i):
        return pltpu.make_async_copy(zh.at[i], zb.at[2 + i % 2], zrsem.at[i % 2])

    def write_ud(i):
        rows = pl.ds(pl.multiple_of((i % G) * C, C), C)
        return (pltpu.make_async_copy(ub.at[i % 2], uh.at[i // G, rows], udsem.at[0, i % 2]),
                pltpu.make_async_copy(db.at[i % 2], dh.at[i // G, rows], udsem.at[1, i % 2]))

    def read_ud(k):
        return (pltpu.make_async_copy(uh.at[k], uw.at[k % 2], rdsem.at[0, k % 2]),
                pltpu.make_async_copy(dh.at[k], dw.at[k % 2], rdsem.at[1, k % 2]))

    def ensure_z(done, want):
        for j in range(2):
            @_when(done + j < want)
            def _(j=j):
                write_z(done + j).wait()

    def ensure_ud(done, want):
        for j in range(2):
            @_when(done + j < want)
            def _(j=j):
                for c in write_ud(done + j):
                    c.wait()

    def forward(i, zw):
        r = i % RING
        zs = jnp.where(spill, i % 2, i % 4)

        @_when(spill)
        def _():
            ensure_z(zw, i - 1)

        pltpu.make_async_copy(x.at[i], hb.at[i], hsem.at[i]).wait()

        @_when(i >= RING)
        def _():
            send_f(i, r).wait_send()

            @_when(s == last)
            def _():
                own_y(i, r).wait()

        h = hb[i]
        us = []
        for n in range(F // TN):
            sl = pl.ds(n * TN, TN)
            z = _dot(h, w1[:, sl])
            zb[zs, :, sl] = z
            t = jnp.tanh(z * (C0 + (C0 * C1) * (z * z)))
            us.append((z * (0.5 * (1.0 + t))).astype(bf16))
        u = jnp.concatenate(us, axis=1)
        fo[r] = (h.astype(f32) + _dot(u, w2[...])).astype(bf16)

        @_when(s < last)
        def _():
            send_f(i, r).start()

        @_when(s == last)
        def _():
            send_y(i, r).start()
            own_y(i, r).start()

        @_when(spill)
        def _():
            write_z(i).start()

            @_when(i == 4)
            def _():
                read_z(0).start()

    def backward(i, zw, ud):
        r = i % RING
        zs = jnp.where(spill, 2 + i % 2, i % 4)

        @_when(spill)
        def _():
            read_z(i).wait()
            ensure_z(zw, jnp.minimum(i + 2, n_ch))

            @_when(i + 1 < n_ch)
            def _():
                read_z(i + 1).start()

        ensure_ud(ud, i - 1)
        pltpu.make_async_copy(g.at[i], gb.at[i], gsem.at[i]).wait()

        @_when(i >= RING)
        def _():
            send_b(i, r).wait_send()

            @_when(s == 0)
            def _():
                own_x(i, r).wait()

        gg = gb[i]
        q = i % 2
        for n in range(F // TN):
            sl = pl.ds(n * TN, TN)
            du = _dot(gg, w2t[:, sl])
            z = zb[zs, :, sl]
            z2 = z * z
            t = jnp.tanh(z * (C0 + (C0 * C1) * z2))
            p = 0.5 * (1.0 + t)
            ub[q, :, sl] = (z * p).astype(bf16)
            dg = p + ((0.5 * z) * (1.0 - t * t)) * (C0 + (3.0 * C0 * C1) * z2)
            db[q, :, sl] = (dg * du).astype(bf16)
        bo[r] = (gg.astype(f32) + _dot(db[q], w1t[...])).astype(bf16)

        @_when(s > 0)
        def _():
            send_b(i, r).start()

        @_when(s == 0)
        def _():
            send_x(i, r).start()
            own_x(i, r).start()

        for c in write_ud(i):
            c.start()

    def prefetch(k, ud):
        ensure_ud(ud, G * (k + 1))
        for c in read_ud(k):
            c.start()

    def weights(k):
        for c in read_ud(k):
            c.wait()
        q = k % 2
        rows = pl.ds(G * k, G)
        h = hb[rows].reshape(G * C, D)
        gg = gb[rows].reshape(G * C, D)
        for n in range(F // TN):
            sl = pl.ds(n * TN, TN)
            a1[:, sl] += _dot_t(h, dw[q, :, sl])
        for n in range(F // TN):
            sl = pl.ds(n * TN, TN)
            a2[sl, :] += _dot_t(uw[q, :, sl], gg)

    def relay_step(i):
        @_when(even)
        def _():
            pltpu.make_async_copy(y.at[i], y.at[i], ysem.at[i]).wait()

            @_when(s < n_st - 2)
            def _():
                relay(y, i, ysem, 0, s + 1).start()

            @_when(s >= 2)
            def _():
                relay(y, i, ysem, 1, s - 2).start()

        @_when(jnp.logical_not(even))
        def _():
            pltpu.make_async_copy(dx.at[i], dx.at[i], xsem.at[i]).wait()

            @_when(s > 1)
            def _():
                relay(dx, i, xsem, 0, s - 1).start()

            @_when(s < last)
            def _():
                relay(dx, i, xsem, 1, s + 2).start()

    def transposes():
        def f(n, _):
            sl = pl.ds(pl.multiple_of(n * 256, 256), 256)
            w1t[sl, :] = w1[:, sl].T
            w2t[:, sl] = w2[sl, :].T
            a1[:, sl] = jnp.zeros((D, 256), f32)
            a2[sl, :] = jnp.zeros((256, D), f32)
            return 0
        lax.fori_loop(0, F // 256, f, 0)

    def step(j, carry):
        word, nf, nb, nw, npf, nr, zw, ud = carry
        op = word % 8
        is_f, is_b, is_p = op == 0, op == 1, op == 3

        @_when(is_f)
        def _():
            forward(nf, zw)

        @_when(is_b)
        def _():
            backward(nb, zw, ud)

        @_when(op == 2)
        def _():
            weights(nw)

        @_when(is_p)
        def _():
            prefetch(npf, ud)

        @_when(op == 4)
        def _():
            relay_step(nr)

        @_when(op == 5)
        def _():
            transposes()

        zw = jnp.where(is_f, jnp.maximum(zw, nf - 1), zw)
        zw = jnp.where(is_b, jnp.maximum(zw, jnp.minimum(nb + 2, n_ch)), zw)
        ud = jnp.where(is_b, jnp.maximum(ud, nb - 1), ud)
        ud = jnp.where(is_p, jnp.maximum(ud, G * (npf + 1)), ud)
        one = lambda k: jnp.where(op == k, 1, 0)
        return (word // 8, nf + one(0), nb + one(1), nw + one(2), npf + one(3), nr + one(4), zw, ud)

    zero = s * 0
    state = (zero,) * 7
    for k in range(len(WORDS[0])):
        word = zero
        for q in range(n_st):
            word = jnp.where(s == q, WORDS[q][k], word)
        if k == 0:
            words = [word]
        else:
            words.append(word)

    def block(k, carry):
        word = words[0]
        for q in range(1, len(words)):
            word = jnp.where(k == q, words[q], word)
        out = lax.fori_loop(0, STEPS, step, (word, *carry))
        return out[1:]

    lax.fori_loop(0, len(words), block, state)

    for j in range(RING):
        i = n_ch - RING + j
        r = i % RING
        send_f(i, r).wait_send()
        send_b(i, r).wait_send()

        @_when(s == last)
        def _(i=i, r=r):
            own_y(i, r).wait()

        @_when(s == 0)
        def _(i=i, r=r):
            own_x(i, r).wait()

    def finish(i, _):
        @_when(even)
        def _():
            @_when(s < n_st - 2)
            def _():
                relay(y, i, ysem, 0, s + 1).wait_send()

            @_when(s >= 2)
            def _():
                relay(y, i, ysem, 1, s - 2).wait_send()

            @_when(s > 0)
            def _():
                pltpu.make_async_copy(dx.at[i], dx.at[i], xsem.at[i]).wait()

        @_when(jnp.logical_not(even))
        def _():
            @_when(s > 1)
            def _():
                relay(dx, i, xsem, 0, s - 1).wait_send()

            @_when(s < last)
            def _():
                relay(dx, i, xsem, 1, s + 2).wait_send()
                pltpu.make_async_copy(y.at[i], y.at[i], ysem.at[i]).wait()
        return 0
    lax.fori_loop(0, n_ch, finish, 0)


def _write_out(n_ch, y, dx, a1, a2, yo, dxo, d1, d2, yb, xb, sem_w, sem_r, sem_o):
    parts = 4
    big = []
    for p in range(parts):
        r1 = pl.ds(p * (D // parts), D // parts)
        r2 = pl.ds(p * (F // parts), F // parts)
        big.append(pltpu.make_async_copy(a1.at[r1], d1.at[0, r1], sem_w.at[0, p]))
        big.append(pltpu.make_async_copy(a2.at[r2], d2.at[0, r2], sem_w.at[1, p]))
    ins = [pltpu.make_async_copy(y, yb, sem_r.at[0]), pltpu.make_async_copy(dx, xb, sem_r.at[1])]
    outs = [pltpu.make_async_copy(yb, yo, sem_o.at[0]), pltpu.make_async_copy(xb, dxo, sem_o.at[1])]
    for c in ins:
        c.start()
    for c in big:
        c.start()
    for c, o in zip(ins, outs):
        c.wait()
        o.start()
    for c in big:
        c.wait()
    for o in outs:
        o.wait()


def solution(mesh):
    n_st = mesh.shape["stage"]

    def body(x, g, w1, w2):
        n_mb, rows, _ = x.shape
        n_ch = n_mb * rows // C
        xc = x.reshape(n_ch, C, D)
        gc = g.reshape(n_ch, C, D)
        hbm = pl.BlockSpec(memory_space=pltpu.HBM)
        vmem = pl.BlockSpec(memory_space=pltpu.VMEM)
        dma = pltpu.SemaphoreType.DMA
        chunk = (n_ch, C, D)
        y, dx, a1, a2, _, _, _ = pl.pallas_call(
            functools.partial(_pipeline, n_st, n_ch),
            out_shape=[pltpu.HBM(chunk, bf16), pltpu.HBM(chunk, bf16), pltpu.VMEM((D, F), f32), pltpu.VMEM((F, D), f32),
                       pltpu.HBM((n_ch, C, F), f32), pltpu.HBM((n_ch // G, G * C, F), bf16), pltpu.HBM((n_ch // G, G * C, F), bf16)],
            in_specs=[hbm] * 4,
            out_specs=[hbm, hbm, vmem, vmem, hbm, hbm, hbm],
            scratch_shapes=[
                pltpu.VMEM((D, F), bf16), pltpu.VMEM((F, D), bf16), pltpu.VMEM((F, D), bf16), pltpu.VMEM((D, F), bf16),
                pltpu.VMEM(chunk, bf16), pltpu.VMEM(chunk, bf16), pltpu.VMEM((4, C, F), f32),
                pltpu.VMEM((2, C, F), bf16), pltpu.VMEM((2, C, F), bf16),
                pltpu.VMEM((2, G * C, F), bf16), pltpu.VMEM((2, G * C, F), bf16),
                pltpu.VMEM((RING, C, D), bf16), pltpu.VMEM((RING, C, D), bf16),
                dma((2,)), dma((n_ch,)), dma((n_ch,)), dma((n_ch,)), dma((n_ch,)), dma((RING,)), dma((RING,)), dma((RING,)),
                dma((2, n_ch)), dma((2,)), dma((2,)), dma((2, 2)), dma((2, 2)),
            ],
            compiler_params=pltpu.CompilerParams(collective_id=0, has_side_effects=True, vmem_limit_bytes=46_000_000),
            name="pipeline",
        )(xc, gc, w1, w2)
        y, dx, d1, d2 = pl.pallas_call(
            functools.partial(_write_out, n_ch),
            out_shape=[pltpu.HBM(chunk, bf16), pltpu.HBM(chunk, bf16), pltpu.HBM((1, D, F), f32), pltpu.HBM((1, F, D), f32)],
            in_specs=[hbm, hbm, vmem, vmem],
            out_specs=[hbm] * 4,
            scratch_shapes=[pltpu.VMEM(chunk, bf16), pltpu.VMEM(chunk, bf16), dma((2, 4)), dma((2,)), dma((2,))],
            compiler_params=pltpu.CompilerParams(has_side_effects=True, vmem_limit_bytes=7_000_000),
            name="write_out",
        )(*(pltpu.with_memory_space_constraint(v, pltpu.HBM) for v in (y, dx)), a1, a2)
        return y.reshape(x.shape), dx.reshape(x.shape), d1, d2

    return jax.shard_map(body, mesh=mesh,
                         in_specs=(P("data"), P("data"), P("stage"), P("stage")),
                         out_specs=(P("data"), P("data"), P(("data", "stage")), P(("data", "stage"))),
                         check_vma=False)
```

```python
import functools

import jax
import jax.numpy as jnp
from jax import lax
from jax.experimental import pallas as pl
from jax.experimental.pallas import tpu as pltpu
from jax.sharding import PartitionSpec as P

MESH = pl.DeviceIdType.MESH
f32 = jnp.float32
bf16 = jnp.bfloat16
D = 768
F = 3072
C = 128
H = 64
RING = 4
TN = 256
TW = 512
C0 = 0.7978845608028654
C1 = 0.044715

WORDS = (
    (0, 614465536, 472959076, 439399505, 294228753, 208181387, 592582754, 344601890, 613558548, 1073741820),
    (0, 564133888, 210286857, 439490842, 589710436, 210585684, 189928226, 344246436, 307341587, 1073741818),
    (5, 603996160, 193337440, 591705186, 438965897, 560600140, 592595018, 344601890, 613558548, 1073741820),
    (5, 134479872, 157853785, 610834644, 208279825, 592495884, 338827425, 340895907, 613558548, 1073741820),
    (67108869, 142612736, 539771396, 157849809, 156284002, 591799066, 445270281, 579971236, 613500194, 1073741820),
    (16777221, 23101504, 555778753, 562370186, 444999770, 445257996, 445265172, 609305876, 613566756, 1073741820),
    (75501829, 540115713, 201595073, 25215041, 205914657, 613566554, 613566756, 308884644, 307046035, 1073741818),
    (184815685, 17045000, 17043521, 293634572, 579683540, 344802586, 342501588, 613500180, 613566756, 1073741820),
)
STEPS = 10


def _dot(a, b):
    return jnp.dot(a, b, preferred_element_type=f32)


def _dot_t(a, b):
    return lax.dot_general(a, b, (((0,), (0,)), ((), ())), preferred_element_type=f32)


def _gelu(z):
    q = (C0 * C1) * (z * z)
    p = 0.5 * jnp.tanh(z * (C0 + q)) + 0.5
    u = z * p
    return u.astype(bf16), p + (u * (1.0 - p)) * (2.0 * C0 + 6.0 * q)


def _pipeline(n_st, n_ch, x, g, w1h, w2h, lf, rb, a1, a2, zh, uh, dh,
              w1, w2, w1t, w2t, hb, gb, zb, ub, db, uw, dw, fo, bo,
              wsem, hsem, gsem, psem, lsem, fsem, bsem, osem, rsem, zwsem, zrsem, uwsem, dwsem, ursem, drsem):
    d = lax.axis_index("data")
    s = lax.axis_index("stage")
    last = n_st - 1
    end = n_ch - 1
    pieces = 2 * end
    spill = s < n_st - 2
    even = s % 2 == 0
    top, low = pl.ds(0, H), pl.ds(H, H)

    def peer(k):
        return (d, k)

    def sized(i, small, full):
        short = (i == 0) | (i == end)
        pl.when(short)(small)
        pl.when(jnp.logical_not(short))(full)

    def row(i):
        return jnp.maximum(i * C - H, 0)

    def load(src, dst, sem, i, rows):
        at = pl.ds(pl.multiple_of(row(i), H), rows)
        return pltpu.make_async_copy(src.at[at], dst.at[i, pl.ds(0, rows)], sem.at[i])

    def landed(buf, sem, i):
        def wait(rows):
            part = buf.at[i, pl.ds(0, rows)]
            pltpu.make_async_copy(part, part, sem.at[i]).wait()
        sized(i, lambda: wait(H), lambda: wait(C))

    loads = [pltpu.make_async_copy(w1h.at[0], w1, wsem.at[0]), pltpu.make_async_copy(w2h.at[0], w2, wsem.at[1])]

    def load_all(src, dst, sem):
        def f(i, _):
            sized(i, lambda: load(src, dst, sem, i, H).start(), lambda: load(src, dst, sem, i, C).start())
            return 0
        return f

    @pl.when(s == 0)
    def _():
        load(x, hb, hsem, 0, H).start()

    for c in loads:
        c.start()

    @pl.when(s == 0)
    def _():
        lax.fori_loop(1, n_ch, load_all(x, hb, hsem), 0)

    @pl.when(s == last)
    def _():
        lax.fori_loop(0, n_ch, load_all(g, gb, gsem), 0)

    hb[0, low, :] = jnp.zeros((H, D), bf16)
    gb[0, low, :] = jnp.zeros((H, D), bf16)

    bar = pltpu.get_barrier_semaphore()
    near = (-2, -1, 1, 2)
    for off in near:
        @pl.when((s + off >= 0) & (s + off < n_st))
        def _(off=off):
            pl.semaphore_signal(bar, inc=1, device_id=peer(s + off), device_id_type=MESH)
    for k in range(3, n_st, 2):
        @pl.when(s == 0)
        def _(k=k):
            pl.semaphore_signal(bar, inc=1, device_id=peer(k), device_id_type=MESH)

        @pl.when(s == k)
        def _(k=k):
            pl.semaphore_signal(bar, inc=1, device_id=peer(0), device_id_type=MESH)
    far = jnp.where(s == 0, (n_st - 2) // 2, jnp.where((s % 2 == 1) & (s >= 3), 1, 0))
    pl.semaphore_wait(bar, jnp.minimum(s, 2) + jnp.minimum(last - s, 2) + far)

    for c in loads:
        c.wait()

    def send(src, r, dst, i, ssem, rsem_, dev, rows):
        return pltpu.make_async_remote_copy(src_ref=src.at[r, pl.ds(0, rows)], dst_ref=dst.at[i, pl.ds(0, rows)],
                                            send_sem=ssem.at[0, r], recv_sem=rsem_.at[i], device_id=peer(dev), device_id_type=MESH)

    def send_f(i, r, rows):
        return send(fo, r, hb, i, fsem, hsem, s + 1, rows)

    def send_b(i, r, rows):
        return send(bo, r, gb, i, bsem, gsem, s - 1, rows)

    def first_piece(i):
        return jnp.maximum(2 * i - 1, 0)

    def hand(src, r, k, p, ssem, dev):
        return pltpu.make_async_remote_copy(src_ref=src.at[r, pl.ds(k * H, H)], dst_ref=rb.at[p], send_sem=ssem.at[k, r],
                                            recv_sem=psem.at[p], device_id=peer(dev), device_id_type=MESH)

    def keep(src, r, k, p):
        return pltpu.make_async_copy(src.at[r, pl.ds(k * H, H)], lf.at[p], osem.at[k, r])

    def out_start(src, r, i, ssem, dev):
        p = first_piece(i)
        hand(src, r, 0, p, ssem, dev).start()
        keep(src, r, 0, p).start()

        def more():
            hand(src, r, 1, p + 1, ssem, dev).start()
            keep(src, r, 1, p + 1).start()
        sized(i, lambda: None, more)

    def out_wait(src, r, i, ssem, dev):
        p = first_piece(i)
        hand(src, r, 0, p, ssem, dev).wait_send()
        keep(src, r, 0, p).wait()

        def more():
            hand(src, r, 1, p + 1, ssem, dev).wait_send()
            keep(src, r, 1, p + 1).wait()
        sized(i, lambda: None, more)

    def direct(r, k):
        return pltpu.make_async_remote_copy(src_ref=bo.at[r, top], dst_ref=rb.at[pieces - 1], send_sem=lsem.at[0, k],
                                            recv_sem=psem.at[pieces - 1], device_id=peer(k), device_id_type=MESH)

    def onward(p, dev):
        return pltpu.make_async_remote_copy(src_ref=rb.at[p], dst_ref=rb.at[p], send_sem=rsem.at[0, p], recv_sem=psem.at[p],
                                            device_id=peer(dev), device_id_type=MESH)

    def across(p, dev):
        return pltpu.make_async_remote_copy(src_ref=rb.at[p], dst_ref=lf.at[p], send_sem=rsem.at[1, p], recv_sem=lsem.at[1, p],
                                            device_id=peer(dev), device_id_type=MESH)

    def write_z(i):
        return pltpu.make_async_copy(zb.at[i % 2], zh.at[i], zwsem.at[i % 2])

    def read_z(i):
        return pltpu.make_async_copy(zh.at[i], zb.at[2 + i % 2], zrsem.at[i % 2])

    def group_rows(i):
        return (i - 1) // 2, pl.ds(pl.multiple_of(((i - 1) % 2) * C, C), C)

    def write_u(i):
        k, rows = group_rows(i)
        return pltpu.make_async_copy(ub.at[i % 2], uh.at[k, rows], uwsem.at[i % 2])

    def write_d(i):
        k, rows = group_rows(i)
        return pltpu.make_async_copy(db.at[i % 2], dh.at[k, rows], dwsem.at[i % 2])

    def read_u(k):
        return pltpu.make_async_copy(uh.at[k], uw.at[k % 2], ursem.at[k % 2])

    def read_d(k):
        return pltpu.make_async_copy(dh.at[k], dw.at[k % 2], drsem.at[k % 2])

    def ensure(write, done, want, low_=0):
        for j in range(2):
            @pl.when((done + j < want) & (done + j >= low_))
            def _(j=j):
                write(done + j).wait()

    def forward(i, zw, uc):
        r = i % RING
        zs = jnp.where(spill, i % 2, i % 4)
        q = i % 2

        @pl.when(spill)
        def _():
            ensure(write_z, zw, i - 1)

        ensure(write_u, uc, i - 1, 1)
        landed(hb, hsem, i)

        @pl.when(i >= RING)
        def _():
            @pl.when(s < last)
            def _():
                sized(i - RING, lambda: send_f(i, r, H).wait_send(), lambda: send_f(i, r, C).wait_send())

            @pl.when(s == last)
            def _():
                out_wait(fo, r, i - RING, fsem, s - 1)

        @pl.when(i == 0)
        def _():
            hb[end, low, :] = hb[0, top, :]

        h = hb[i]
        for n in range(F // TN):
            sl = pl.ds(n * TN, TN)
            u, gp = _gelu(_dot(h, w1[:, sl]))
            zb[zs, :, sl] = gp
            ub[q, :, sl] = u
        acc = h.astype(f32)
        for n in range(F // TN):
            sl = pl.ds(n * TN, TN)
            part = _dot(ub[q, :, sl], w2[sl, :])
            tot = part if n == 0 else tot + part
        fo[r] = (acc + tot).astype(bf16)

        @pl.when(s < last)
        def _():
            sized(i, lambda: send_f(i, r, H).start(), lambda: send_f(i, r, C).start())

        @pl.when(s == last)
        def _():
            out_start(fo, r, i, fsem, s - 1)

        @pl.when(i > 0)
        def _():
            write_u(i).start()

        @pl.when(spill)
        def _():
            write_z(i).start()

            @pl.when(i == 4)
            def _():
                read_z(0).start()

    def backward(i, zw, dc):
        r = i % RING
        zs = jnp.where(spill, 2 + i % 2, i % 4)
        q = i % 2

        @pl.when(spill)
        def _():
            read_z(i).wait()
            ensure(write_z, zw, jnp.minimum(i + 2, n_ch))

            @pl.when(i + 1 < n_ch)
            def _():
                read_z(i + 1).start()

        ensure(write_d, dc, i - 1, 1)
        landed(gb, gsem, i)

        @pl.when(i >= RING)
        def _():
            @pl.when(s > 0)
            def _():
                sized(i - RING, lambda: send_b(i, r, H).wait_send(), lambda: send_b(i, r, C).wait_send())

            @pl.when(s == 0)
            def _():
                out_wait(bo, r, i - RING, bsem, s + 1)

        @pl.when(i == 0)
        def _():
            gb[end, low, :] = gb[0, top, :]

        gg = gb[i]
        for n in range(F // TN):
            sl = pl.ds(n * TN, TN)
            db[q, :, sl] = (zb[zs, :, sl] * _dot(gg, w2t[:, sl])).astype(bf16)
        for n in range(F // TN):
            sl = pl.ds(n * TN, TN)
            part = _dot(db[q, :, sl], w1t[sl, :])
            tot = part if n == 0 else tot + part
        bo[r] = (gg.astype(f32) + tot).astype(bf16)

        @pl.when(s > 0)
        def _():
            sized(i, lambda: send_b(i, r, H).start(), lambda: send_b(i, r, C).start())

        @pl.when(s == 0)
        def _():
            @pl.when(i == end)
            def _():
                for k in range(last, 2, -2):
                    direct(r, k).start()
            out_start(bo, r, i, bsem, s + 1)

        @pl.when(i > 0)
        def _():
            write_d(i).start()

    def prefetch(k, uc, dc):
        ensure(write_u, uc, 2 * k + 3, 1)
        ensure(write_d, dc, 2 * k + 3, 1)
        read_d(k).start()
        read_u(k).start()

    def weights(w):
        k = w // 2
        q = k % 2
        rows = pl.ds(2 * k + 1, 2)

        @pl.when(w % 2 == 0)
        def _():
            read_d(k).wait()
            h = hb[rows].reshape(2 * C, D)
            for n in range(F // TW):
                sl = pl.ds(n * TW, TW)
                a1[:, sl] += _dot_t(h, dw[q, :, sl])

        @pl.when(w % 2 == 1)
        def _():
            read_u(k).wait()
            gg = gb[rows].reshape(2 * C, D)
            for n in range(F // TW):
                sl = pl.ds(n * TW, TW)
                a2[sl, :] += _dot_t(uw[q, :, sl], gg)

    def relay_step(p):
        piece = rb.at[p]
        pltpu.make_async_copy(piece, piece, psem.at[p]).wait()

        @pl.when(even)
        def _():
            @pl.when(s >= 2)
            def _():
                onward(p, s - 2).start()

            @pl.when(s < n_st - 2)
            def _():
                across(p, s + 1).start()

        @pl.when(jnp.logical_not(even))
        def _():
            @pl.when((s < last) & (p < pieces - 1))
            def _():
                onward(p, s + 2).start()

            @pl.when(s > 1)
            def _():
                across(p, s - 1).start()

    def transposes():
        def f(n, _):
            sl = pl.ds(pl.multiple_of(n * 256, 256), 256)
            w1t[sl, :] = w1[:, sl].T
            w2t[:, sl] = w2[sl, :].T
            a1[:, sl] = jnp.zeros((D, 256), f32)
            a2[sl, :] = jnp.zeros((256, D), f32)
            return 0
        lax.fori_loop(0, F // 256, f, 0)

    def step(j, carry):
        word, nf, nb, nw, npf, nr, zw, uc, dc = carry
        op = word % 8
        is_f, is_b, is_p = op == 0, op == 1, op == 3

        @pl.when(is_f)
        def _():
            forward(nf, zw, uc)

        @pl.when(is_b)
        def _():
            backward(nb, zw, dc)

        @pl.when(op == 2)
        def _():
            weights(nw)

        @pl.when(is_p)
        def _():
            prefetch(npf, uc, dc)

        @pl.when(op == 4)
        def _():
            relay_step(nr)

        @pl.when(op == 5)
        def _():
            transposes()

        zw = jnp.where(is_f, jnp.maximum(zw, nf - 1), zw)
        zw = jnp.where(is_b, jnp.maximum(zw, jnp.minimum(nb + 2, n_ch)), zw)
        uc = jnp.where(is_f, jnp.maximum(uc, nf - 1), uc)
        uc = jnp.where(is_p, jnp.maximum(uc, 2 * npf + 3), uc)
        dc = jnp.where(is_b, jnp.maximum(dc, nb - 1), dc)
        dc = jnp.where(is_p, jnp.maximum(dc, 2 * npf + 3), dc)
        one = lambda k: jnp.where(op == k, 1, 0)
        return (word // 8, nf + one(0), nb + one(1), nw + one(2), npf + one(3), nr + one(4), zw, uc, dc)

    zero = s * 0
    words = []
    for k in range(len(WORDS[0])):
        word = zero
        for q in range(n_st):
            word = jnp.where(s == q, WORDS[q][k], word)
        words.append(word)

    def block(k, carry):
        word = words[0]
        for q in range(1, len(words)):
            word = jnp.where(k == q, words[q], word)
        out = lax.fori_loop(0, STEPS, step, (word, *carry))
        return out[1:]

    lax.fori_loop(0, len(words), block, (zero, zero, zero, zero, zero, zero, zero + 1, zero + 1))

    for j in range(RING):
        i = n_ch - RING + j
        r = i % RING
        rows = H if i == end else C

        @pl.when(s < last)
        def _(i=i, r=r, rows=rows):
            send_f(i, r, rows).wait_send()

        @pl.when(s == last)
        def _(i=i, r=r):
            out_wait(fo, r, i, fsem, s - 1)

        @pl.when(s > 0)
        def _(i=i, r=r, rows=rows):
            send_b(i, r, rows).wait_send()

        @pl.when(s == 0)
        def _(i=i, r=r):
            out_wait(bo, r, i, bsem, s + 1)

    @pl.when(s == 0)
    def _():
        for k in range(last, 2, -2):
            direct(end % RING, k).wait_send()

    def leaf(p):
        part = lf.at[p]
        pltpu.make_async_copy(part, part, lsem.at[1, p]).wait()

    def finish(p, _):
        @pl.when(even)
        def _():
            @pl.when(s >= 2)
            def _():
                onward(p, s - 2).wait_send()

            @pl.when(s < n_st - 2)
            def _():
                across(p, s + 1).wait_send()

            @pl.when(s > 0)
            def _():
                leaf(p)

        @pl.when(jnp.logical_not(even))
        def _():
            @pl.when((s < last) & (p < pieces - 1))
            def _():
                onward(p, s + 2).wait_send()

            @pl.when(s > 1)
            def _():
                across(p, s - 1).wait_send()

            @pl.when(s < last)
            def _():
                leaf(p)
        return 0
    lax.fori_loop(0, pieces, finish, 0)


def _write_out(lf, rb, a1, a2, y, dx, d1, d2, lb, sem_w, sem_r, sem_o):
    s = lax.axis_index("stage")
    parts = 4
    big = []
    for p in range(parts):
        r1 = pl.ds(p * (D // parts), D // parts)
        r2 = pl.ds(p * (F // parts), F // parts)
        big.append(pltpu.make_async_copy(a1.at[r1], d1.at[0, r1], sem_w.at[0, p]))
        big.append(pltpu.make_async_copy(a2.at[r2], d2.at[0, r2], sem_w.at[1, p]))
    back = pltpu.make_async_copy(lf, lb, sem_r)
    back.start()
    for c in big:
        c.start()

    def rest(mine, other):
        near = pltpu.make_async_copy(rb, mine, sem_o.at[0])
        near.start()
        back.wait()
        far = pltpu.make_async_copy(lb, other, sem_o.at[1])
        far.start()
        near.wait()
        far.wait()

    @pl.when(s % 2 == 0)
    def _():
        rest(y, dx)

    @pl.when(s % 2 == 1)
    def _():
        rest(dx, y)

    for c in big:
        c.wait()


def solution(mesh):
    n_st = mesh.shape["stage"]

    def body(x, g, w1, w2):
        tokens = x.shape[0] * x.shape[1]
        n_ch = tokens // C + 1
        hbm = pl.BlockSpec(memory_space=pltpu.HBM)
        vmem = pl.BlockSpec(memory_space=pltpu.VMEM)
        dma = pltpu.SemaphoreType.DMA
        pieces = (tokens // H, H, D)
        groups = (tokens // (2 * C), 2 * C, F)
        params = dict(has_side_effects=True)
        lf, rb, a1, a2, _, _, _ = pl.pallas_call(
            functools.partial(_pipeline, n_st, n_ch),
            out_shape=[pltpu.HBM(pieces, bf16), pltpu.VMEM(pieces, bf16), pltpu.VMEM((D, F), f32), pltpu.VMEM((F, D), f32),
                       pltpu.HBM((n_ch, C, F), f32), pltpu.HBM(groups, bf16), pltpu.HBM(groups, bf16)],
            in_specs=[hbm] * 4,
            out_specs=[hbm, vmem, vmem, vmem, hbm, hbm, hbm],
            scratch_shapes=[
                pltpu.VMEM((D, F), bf16), pltpu.VMEM((F, D), bf16), pltpu.VMEM((F, D), bf16), pltpu.VMEM((D, F), bf16),
                pltpu.VMEM((n_ch, C, D), bf16), pltpu.VMEM((n_ch, C, D), bf16), pltpu.VMEM((4, C, F), f32),
                pltpu.VMEM((2, C, F), bf16), pltpu.VMEM((2, C, F), bf16),
                pltpu.VMEM((2, 2 * C, F), bf16), pltpu.VMEM((2, 2 * C, F), bf16),
                pltpu.VMEM((RING, C, D), bf16), pltpu.VMEM((RING, C, D), bf16),
                dma((2,)), dma((n_ch,)), dma((n_ch,)), dma((pieces[0],)), dma((2, pieces[0])), dma((2, RING)), dma((2, RING)),
                dma((2, RING)), dma((2, pieces[0])), dma((2,)), dma((2,)), dma((2,)), dma((2,)), dma((2,)), dma((2,)),
            ],
            compiler_params=pltpu.CompilerParams(collective_id=0, vmem_limit_bytes=45_000_000, **params),
            name="pipeline",
        )(x.reshape(tokens, D), g.reshape(tokens, D), w1, w2)
        y, dx, d1, d2 = pl.pallas_call(
            _write_out,
            out_shape=[pltpu.HBM(pieces, bf16), pltpu.HBM(pieces, bf16), pltpu.HBM((1, D, F), f32), pltpu.HBM((1, F, D), f32)],
            in_specs=[hbm, vmem, vmem, vmem],
            out_specs=[hbm] * 4,
            scratch_shapes=[pltpu.VMEM(pieces, bf16), dma((2, 4)), dma, dma((2,))],
            compiler_params=pltpu.CompilerParams(vmem_limit_bytes=4_000_000, **params),
            name="write_out",
        )(pltpu.with_memory_space_constraint(lf, pltpu.HBM), rb, a1, a2)
        return y.reshape(x.shape), dx.reshape(x.shape), d1, d2

    return jax.shard_map(body, mesh=mesh,
                         in_specs=(P("data"), P("data"), P("stage"), P("stage")),
                         out_specs=(P("data"), P("data"), P(("data", "stage")), P(("data", "stage"))),
                         check_vma=False)
```

```python
import functools

import jax
import jax.numpy as jnp
from jax import lax
from jax.experimental import pallas as pl
from jax.experimental.pallas import tpu as pltpu
from jax.sharding import PartitionSpec as P

MESH = pl.DeviceIdType.MESH
f32 = jnp.float32
bf16 = jnp.bfloat16
D = 768
F = 3072
C = 128
H = 64
RING = 4
K = 256
LAG = 6
TW = 512
NS = F // K
C0 = 0.7978845608028654
C1 = 0.044715

WORDS = (
    (0, 629145600, 606647049, 445683994, 579191882, 445686481, 292624673, 608807201, 580004132, 1073741820),
    (671088640, 150994944, 294754572, 575805217, 606749409, 613029986, 210126475, 608584482, 307050643, 1073741818),
    (5, 68159488, 158372612, 193282772, 189835348, 204576866, 575816290, 596265116, 608848026, 1073741818),
    (5, 151027712, 558211672, 191513249, 344267042, 611456268, 611358860, 340932770, 340867364, 1073741820),
    (8388613, 75515968, 142914081, 562315809, 292656394, 344245004, 592069916, 613497122, 307053850, 1073741818),
    (16777221, 19140672, 17045017, 591798945, 606411041, 579938532, 579942626, 478824604, 609364242, 1073741820),
    (545263877, 19927329, 201720577, 540020804, 193331969, 580008097, 579488028, 575482147, 308884690, 1073741818),
    (17043525, 17043521, 17043521, 612995137, 575743644, 328288036, 577390244, 610879780, 613566610, 1073741820),
)
STEPS = 10


def _dot(a, b):
    return jnp.dot(a, b, preferred_element_type=f32)


def _dot_t(a, b):
    return lax.dot_general(a, b, (((0,), (0,)), ((), ())), preferred_element_type=f32)


def _gelu(z):
    q = (C0 * C1) * (z * z)
    p = 0.5 * jnp.tanh(z * (C0 + q)) + 0.5
    u = z * p
    return u.astype(bf16), p + (u * (1.0 - p)) * (2.0 * C0 + 6.0 * q)


def _pipeline(n_st, n_ch, x, g, w1h, w2h, lf, rb, a1, a2, zh, uh, dh,
              w1, w2, w1t, w2t, hb, gb, zb, ub, db, uw, dw, fo, bo,
              wsem, hsem, gsem, psem, lsem, esem, fsem, bsem, osem, rsem, zwsem, zrsem, uwsem, dwsem, ursem, drsem):
    d = lax.axis_index("data")
    s = lax.axis_index("stage")
    last = n_st - 1
    end = n_ch - 1
    pieces = 2 * end
    spill = s < n_st - 2
    even = s % 2 == 0
    top, low = pl.ds(0, H), pl.ds(H, H)

    def peer(k):
        return (d, k)

    def sized(i, small, full):
        short = (i == 0) | (i == end)
        pl.when(short)(small)
        pl.when(jnp.logical_not(short))(full)

    def row(i):
        return jnp.maximum(i * C - H, 0)

    def cols(k):
        return pl.ds(k * K, K)

    def load(src, dst, sem, i):
        at = pl.ds(pl.multiple_of(row(i), H), C)
        return pltpu.make_async_copy(src.at[at], dst.at[i], sem.at[i])

    def load_end(src, dst, sem, i):
        at = pl.ds(0 if i == 0 else (2 * end - 1) * H, H)
        return pltpu.make_async_copy(src.at[at], dst.at[i, top], sem.at[i])

    def landed(buf, sem, i, rows):
        part = buf.at[i, pl.ds(0, rows)]
        pltpu.make_async_copy(part, part, sem.at[i]).wait()

    get_w1 = pltpu.make_async_copy(w1h.at[0], w1, wsem.at[0])
    get_w2 = pltpu.make_async_copy(w2h.at[0], w2, wsem.at[1])

    def load_all(src, dst, sem):
        load_end(src, dst, sem, end).start()

        def f(i, _):
            load(src, dst, sem, i).start()
            return 0
        lax.fori_loop(1, end, f, 0)

    @pl.when(s == 0)
    def _():
        load_end(x, hb, hsem, 0).start()

    get_w1.start()
    get_w2.start()

    @pl.when(s == 0)
    def _():
        load_all(x, hb, hsem)

    @pl.when(s == last)
    def _():
        load_end(g, gb, gsem, 0).start()
        load_all(g, gb, gsem)

    bar = pltpu.get_barrier_semaphore()
    near = (-2, -1, 1, 2)
    for off in near:
        @pl.when((s + off >= 0) & (s + off < n_st))
        def _(off=off):
            pl.semaphore_signal(bar, inc=1, device_id=peer(s + off), device_id_type=MESH)
    for k in range(3, n_st, 2):
        @pl.when(s == 0)
        def _(k=k):
            pl.semaphore_signal(bar, inc=1, device_id=peer(k), device_id_type=MESH)

        @pl.when(s == k)
        def _(k=k):
            pl.semaphore_signal(bar, inc=1, device_id=peer(0), device_id_type=MESH)
    far = jnp.where(s == 0, (n_st - 2) // 2, jnp.where((s % 2 == 1) & (s >= 3), 1, 0))
    peers = jnp.minimum(s, 2) + jnp.minimum(last - s, 2) + far

    def send(src, r, dst, i, ssem, to, dev, rows):
        part = pl.ds(0, rows)
        return pltpu.make_async_remote_copy(src_ref=src.at[r, part], dst_ref=dst.at[i, part], send_sem=ssem.at[0, r],
                                            recv_sem=to.at[i], device_id=peer(dev), device_id_type=MESH)

    def send_f(i, r, rows):
        return send(fo, r, hb, i, fsem, hsem, s + 1, rows)

    def send_b(i, r, rows):
        return send(bo, r, gb, i, bsem, gsem, s - 1, rows)

    def sent_f(i, r):
        sized(i, lambda: send_f(i, r, H).wait_send(), lambda: send_f(i, r, C).wait_send())

    def sent_b(i, r):
        sized(i, lambda: send_b(i, r, H).wait_send(), lambda: send_b(i, r, C).wait_send())

    def first_piece(i):
        return jnp.maximum(2 * i - 1, 0)

    def hand(src, r, k, p, ssem, dev):
        return pltpu.make_async_remote_copy(src_ref=src.at[r, pl.ds(k * H, H)], dst_ref=rb.at[p], send_sem=ssem.at[k, r],
                                            recv_sem=psem.at[p], device_id=peer(dev), device_id_type=MESH)

    def keep(src, r, k, p):
        return pltpu.make_async_copy(src.at[r, pl.ds(k * H, H)], lf.at[p], osem.at[k, r])

    def out_start(src, r, i, ssem, dev):
        p = first_piece(i)
        hand(src, r, 0, p, ssem, dev).start()
        keep(src, r, 0, p).start()

        def more():
            hand(src, r, 1, p + 1, ssem, dev).start()
            keep(src, r, 1, p + 1).start()
        sized(i, lambda: None, more)

    def out_wait(src, r, i, ssem, dev):
        p = first_piece(i)
        hand(src, r, 0, p, ssem, dev).wait_send()
        keep(src, r, 0, p).wait()

        def more():
            hand(src, r, 1, p + 1, ssem, dev).wait_send()
            keep(src, r, 1, p + 1).wait()
        sized(i, lambda: None, more)

    def direct(r, k):
        return pltpu.make_async_remote_copy(src_ref=bo.at[r, top], dst_ref=rb.at[pieces - 1], send_sem=esem.at[k // 2 - 1],
                                            recv_sem=psem.at[pieces - 1], device_id=peer(k), device_id_type=MESH)

    def onward(p, dev):
        return pltpu.make_async_remote_copy(src_ref=rb.at[p], dst_ref=rb.at[p], send_sem=rsem.at[0], recv_sem=psem.at[p],
                                            device_id=peer(dev), device_id_type=MESH)

    def across(p, dev):
        return pltpu.make_async_remote_copy(src_ref=rb.at[p], dst_ref=lf.at[p], send_sem=rsem.at[1], recv_sem=lsem,
                                            device_id=peer(dev), device_id_type=MESH)

    def write_z(i):
        q = lax.rem(i, 2)
        return pltpu.make_async_copy(zb.at[q], zh.at[i], zwsem.at[q])

    def read_z(i):
        q = lax.rem(i, 2)
        return pltpu.make_async_copy(zh.at[i], zb.at[2 + q], zrsem.at[q])

    def rows_of(i, rows):
        first = i == 0
        k = jnp.where(first, end // 2 - 1, lax.div(i - 1, 2))
        at = jnp.where(first, C + H, lax.rem(i - 1, 2) * C)
        return k, pl.ds(pl.multiple_of(at, H), rows)

    def write_ud(src, dst, sem, i, rows):
        k, at = rows_of(i, rows)
        q = lax.rem(i, 2)
        return pltpu.make_async_copy(src.at[q, pl.ds(0, rows)], dst.at[k, at], sem.at[q])

    def put_ud(src, dst, sem, i):
        sized(i, lambda: write_ud(src, dst, sem, i, H).start(), lambda: write_ud(src, dst, sem, i, C).start())

    def done_u(i):
        sized(i, lambda: write_ud(ub, uh, uwsem, i, H).wait(), lambda: write_ud(ub, uh, uwsem, i, C).wait())

    def done_d(i):
        sized(i, lambda: write_ud(db, dh, dwsem, i, H).wait(), lambda: write_ud(db, dh, dwsem, i, C).wait())

    def read_u(k):
        q = lax.rem(k, 2)
        return pltpu.make_async_copy(uh.at[k], uw.at[q], ursem.at[q])

    def read_d(k):
        q = lax.rem(k, 2)
        return pltpu.make_async_copy(dh.at[k], dw.at[q], drsem.at[q])

    def ensure(wait, done, want):
        for j in range(2):
            @pl.when(done + j < want)
            def _(j=j):
                wait(done + j)

    def forward_rows(i, r, zs, q, rows):
        landed(hb, hsem, i, rows)
        part = pl.ds(0, rows)
        h = hb[i, part, :]
        tot = None
        for n in range(NS + LAG):
            if n < NS:
                z = _dot(h, w1[:, cols(n)])
            if n >= LAG:
                m = n - LAG
                y = _dot(ub[q, part, cols(m)], w2[cols(m), :])
                tot = y if m == 0 else tot + y
            if n < NS:
                u, gp = _gelu(z)
                zb[zs, part, cols(n)] = gp
                ub[q, part, cols(n)] = u
        fo[r, part, :] = (h.astype(f32) + tot).astype(bf16)

        if rows == H:
            @pl.when(i == 0)
            def _():
                pl.semaphore_wait(bar, peers)

        @pl.when(s < last)
        def _():
            send_f(i, r, rows).start()

    def forward_end(i, r, zs, q, fresh):
        @pl.when(fresh)
        def _():
            get_w1.wait()
            get_w2.wait()

        forward_rows(i, r, zs, q, H)

        @pl.when(i == 0)
        def _():
            hb[end, low, :] = hb[0, top, :]

    def forward(i, zw, uc, fresh):
        r = lax.rem(i, RING)
        q = lax.rem(i, 2)
        zs = jnp.where(spill, q, lax.rem(i, 4))

        @pl.when(spill)
        def _():
            ensure(lambda j: write_z(j).wait(), zw, i - 1)

        ensure(done_u, uc, i - 1)

        @pl.when(i >= RING)
        def _():
            @pl.when(s < last)
            def _():
                sent_f(i - RING, r)

            @pl.when(s == last)
            def _():
                out_wait(fo, r, i - RING, fsem, s - 1)

        sized(i, lambda: forward_end(i, r, zs, q, fresh), lambda: forward_rows(i, r, zs, q, C))

        @pl.when(s == last)
        def _():
            out_start(fo, r, i, fsem, s - 1)

        put_ud(ub, uh, uwsem, i)

        @pl.when(spill)
        def _():
            write_z(i).start()

            @pl.when(i == 4)
            def _():
                read_z(0).start()

    def backward_rows(i, r, zs, q, rows):
        landed(gb, gsem, i, rows)
        part = pl.ds(0, rows)
        gg = gb[i, part, :]
        tot = None
        for n in range(NS + LAG):
            if n < NS:
                du = _dot(gg, w2t[:, cols(n)])
            if n >= LAG:
                m = n - LAG
                y = _dot(db[q, part, cols(m)], w1t[cols(m), :])
                tot = y if m == 0 else tot + y
            if n < NS:
                db[q, part, cols(n)] = (zb[zs, part, cols(n)] * du).astype(bf16)
        bo[r, part, :] = (gg.astype(f32) + tot).astype(bf16)

        @pl.when(s > 0)
        def _():
            send_b(i, r, rows).start()

    def backward_end(i, r, zs, q):
        backward_rows(i, r, zs, q, H)

        @pl.when(i == 0)
        def _():
            gb[end, low, :] = gb[0, top, :]

    def backward(i, zw, dc):
        r = lax.rem(i, RING)
        q = lax.rem(i, 2)
        zs = jnp.where(spill, 2 + q, lax.rem(i, 4))

        @pl.when(spill)
        def _():
            read_z(i).wait()
            ensure(lambda j: write_z(j).wait(), zw, jnp.minimum(i + 2, n_ch))

            @pl.when(i + 1 < n_ch)
            def _():
                read_z(i + 1).start()

        ensure(done_d, dc, i - 1)

        @pl.when(i >= RING)
        def _():
            @pl.when(s > 0)
            def _():
                sent_b(i - RING, r)

            @pl.when(s == 0)
            def _():
                out_wait(bo, r, i - RING, bsem, s + 1)

        sized(i, lambda: backward_end(i, r, zs, q), lambda: backward_rows(i, r, zs, q, C))

        @pl.when(s == 0)
        def _():
            @pl.when(i == end)
            def _():
                for k in range(last, 2, -2):
                    direct(r, k).start()
            out_start(bo, r, i, bsem, s + 1)

        put_ud(db, dh, dwsem, i)

    def prefetch(k, uc, dc):
        ensure(done_u, uc, 2 * k + 3)
        ensure(done_d, dc, 2 * k + 3)
        read_d(k).start()
        read_u(k).start()

    def weights(w):
        k = lax.div(w, 2)
        q = lax.rem(k, 2)
        rows = pl.ds(2 * k + 1, 2)
        odd = lax.rem(w, 2)

        @pl.when(odd == 0)
        def _():
            read_d(k).wait()
            h = hb[rows].reshape(2 * C, D)
            for n in range(F // TW):
                sl = pl.ds(n * TW, TW)
                a1[:, sl] += _dot_t(h, dw[q, :, sl])

        @pl.when(odd == 1)
        def _():
            read_u(k).wait()
            gg = gb[rows].reshape(2 * C, D)
            for n in range(F // TW):
                sl = pl.ds(n * TW, TW)
                a2[sl, :] += _dot_t(uw[q, :, sl], gg)

    def relay_step(p):
        piece = rb.at[p]
        pltpu.make_async_copy(piece, piece, psem.at[p]).wait()

        @pl.when(even)
        def _():
            @pl.when(s >= 2)
            def _():
                onward(p, s - 2).start()

            @pl.when(s < n_st - 2)
            def _():
                across(p, s + 1).start()

        @pl.when(jnp.logical_not(even))
        def _():
            @pl.when((s < last) & (p < pieces - 1))
            def _():
                onward(p, s + 2).start()

            @pl.when(s > 1)
            def _():
                across(p, s - 1).start()

    def transposes(fresh):
        @pl.when(fresh)
        def _():
            get_w1.wait()
            get_w2.wait()

        def f(n, _):
            sl = pl.ds(pl.multiple_of(n * 256, 256), 256)
            w1t[sl, :] = w1[:, sl].T
            w2t[:, sl] = w2[sl, :].T
            a1[:, sl] = jnp.zeros((D, 256), f32)
            a2[sl, :] = jnp.zeros((256, D), f32)
            return 0
        lax.fori_loop(0, F // 256, f, 0)

    def step(j, carry):
        word, nf, nb, nw, npf, nr, nt, zw, uc, dc = carry
        op = lax.rem(word, 8)
        is_f, is_b, is_p = op == 0, op == 1, op == 3

        @pl.when(op < 2)
        def _():
            @pl.when(is_f)
            def _():
                forward(nf, zw, uc, (nf == 0) & (nt == 0))

            @pl.when(is_b)
            def _():
                backward(nb, zw, dc)

        @pl.when(op >= 2)
        def _():
            @pl.when(op == 2)
            def _():
                weights(nw)

            @pl.when(op == 4)
            def _():
                relay_step(nr)

            @pl.when(is_p)
            def _():
                prefetch(npf, uc, dc)

            @pl.when(op == 5)
            def _():
                transposes(nf == 0)

        zw = jnp.where(is_f, jnp.maximum(zw, nf - 1), zw)
        zw = jnp.where(is_b, jnp.maximum(zw, jnp.minimum(nb + 2, n_ch)), zw)
        uc = jnp.where(is_f, jnp.maximum(uc, nf - 1), uc)
        uc = jnp.where(is_p, jnp.maximum(uc, 2 * npf + 3), uc)
        dc = jnp.where(is_b, jnp.maximum(dc, nb - 1), dc)
        dc = jnp.where(is_p, jnp.maximum(dc, 2 * npf + 3), dc)
        one = lambda k: jnp.where(op == k, 1, 0)
        return (lax.div(word, 8), nf + one(0), nb + one(1), nw + one(2), npf + one(3), nr + one(4), nt + one(5), zw, uc, dc)

    zero = s * 0
    words = []
    for k in range(len(WORDS[0])):
        word = zero
        for q in range(n_st):
            word = jnp.where(s == q, WORDS[q][k], word)
        words.append(word)

    def work(k, carry):
        word = words[0]
        for q in range(1, len(words)):
            word = jnp.where(k == q, words[q], word)
        out = lax.fori_loop(0, STEPS, step, (word, *carry))
        return out[1:]

    lax.fori_loop(0, len(words), work, (zero,) * 9)

    for j in range(RING):
        i = zero + (n_ch - RING + j)
        r = (n_ch - RING + j) % RING

        @pl.when(s < last)
        def _(i=i, r=r):
            sent_f(i, r)

        @pl.when(s == last)
        def _(i=i, r=r):
            out_wait(fo, r, i, fsem, s - 1)

        @pl.when(s > 0)
        def _(i=i, r=r):
            sent_b(i, r)

        @pl.when(s == 0)
        def _(i=i, r=r):
            out_wait(bo, r, i, bsem, s + 1)

    @pl.when(s == 0)
    def _():
        for k in range(last, 2, -2):
            direct(end % RING, k).wait_send()

    def all_of(ref, sem, count):
        part = ref.at[pl.ds(0, count)]
        pltpu.make_async_copy(part, part, sem).wait()

    @pl.when(even)
    def _():
        @pl.when(s >= 2)
        def _():
            all_of(rb, rsem.at[0], pieces)

        @pl.when(s < n_st - 2)
        def _():
            all_of(rb, rsem.at[1], pieces)

        @pl.when(s > 0)
        def _():
            all_of(lf, lsem, pieces)

    @pl.when(jnp.logical_not(even))
    def _():
        @pl.when(s < last)
        def _():
            all_of(rb, rsem.at[0], pieces - 1)
            all_of(lf, lsem, pieces)

        @pl.when(s > 1)
        def _():
            all_of(rb, rsem.at[1], pieces)


def _write_out(lf, rb, a1, a2, y, dx, d1, d2, lb, sem_w, sem_r, sem_o):
    s = lax.axis_index("stage")
    parts = 4
    big = []
    for p in range(parts):
        r1 = pl.ds(p * (D // parts), D // parts)
        r2 = pl.ds(p * (F // parts), F // parts)
        big.append(pltpu.make_async_copy(a1.at[r1], d1.at[0, r1], sem_w.at[0, p]))
        big.append(pltpu.make_async_copy(a2.at[r2], d2.at[0, r2], sem_w.at[1, p]))
    back = pltpu.make_async_copy(lf, lb, sem_r)
    back.start()
    for c in big:
        c.start()

    def rest(mine, other):
        near = pltpu.make_async_copy(rb, mine, sem_o.at[0])
        near.start()
        back.wait()
        far = pltpu.make_async_copy(lb, other, sem_o.at[1])
        far.start()
        near.wait()
        far.wait()

    @pl.when(s % 2 == 0)
    def _():
        rest(y, dx)

    @pl.when(s % 2 == 1)
    def _():
        rest(dx, y)

    for c in big:
        c.wait()


def solution(mesh):
    n_st = mesh.shape["stage"]

    def body(x, g, w1, w2):
        tokens = x.shape[0] * x.shape[1]
        n_ch = tokens // C + 1
        hbm = pl.BlockSpec(memory_space=pltpu.HBM)
        vmem = pl.BlockSpec(memory_space=pltpu.VMEM)
        dma = pltpu.SemaphoreType.DMA
        pieces = (tokens // H, H, D)
        groups = (tokens // (2 * C), 2 * C, F)
        params = dict(has_side_effects=True)
        lf, rb, a1, a2, _, _, _ = pl.pallas_call(
            functools.partial(_pipeline, n_st, n_ch),
            out_shape=[pltpu.HBM(pieces, bf16), pltpu.VMEM(pieces, bf16), pltpu.VMEM((D, F), f32), pltpu.VMEM((F, D), f32),
                       pltpu.HBM((n_ch, C, F), f32), pltpu.HBM(groups, bf16), pltpu.HBM(groups, bf16)],
            in_specs=[hbm] * 4,
            out_specs=[hbm, vmem, vmem, vmem, hbm, hbm, hbm],
            scratch_shapes=[
                pltpu.VMEM((D, F), bf16), pltpu.VMEM((F, D), bf16), pltpu.VMEM((F, D), bf16), pltpu.VMEM((D, F), bf16),
                pltpu.VMEM((n_ch, C, D), bf16), pltpu.VMEM((n_ch, C, D), bf16), pltpu.VMEM((4, C, F), f32),
                pltpu.VMEM((2, C, F), bf16), pltpu.VMEM((2, C, F), bf16),
                pltpu.VMEM((2, 2 * C, F), bf16), pltpu.VMEM((2, 2 * C, F), bf16),
                pltpu.VMEM((RING, C, D), bf16), pltpu.VMEM((RING, C, D), bf16),
                dma((2,)), dma((n_ch,)), dma((n_ch,)), dma((pieces[0],)), dma, dma((n_st // 2 - 1,)), dma((2, RING)), dma((2, RING)),
                dma((2, RING)), dma((2,)), dma((2,)), dma((2,)), dma((2,)), dma((2,)), dma((2,)), dma((2,)),
            ],
            compiler_params=pltpu.CompilerParams(collective_id=0, vmem_limit_bytes=45_000_000, **params),
            name="pipeline",
        )(x.reshape(tokens, D), g.reshape(tokens, D), w1, w2)
        y, dx, d1, d2 = pl.pallas_call(
            _write_out,
            out_shape=[pltpu.HBM(pieces, bf16), pltpu.HBM(pieces, bf16), pltpu.HBM((1, D, F), f32), pltpu.HBM((1, F, D), f32)],
            in_specs=[hbm, vmem, vmem, vmem],
            out_specs=[hbm] * 4,
            scratch_shapes=[pltpu.VMEM(pieces, bf16), dma((2, 4)), dma, dma((2,))],
            compiler_params=pltpu.CompilerParams(vmem_limit_bytes=4_000_000, **params),
            name="write_out",
        )(pltpu.with_memory_space_constraint(lf, pltpu.HBM), rb, a1, a2)
        return y.reshape(x.shape), dx.reshape(x.shape), d1, d2

    return jax.shard_map(body, mesh=mesh,
                         in_specs=(P("data"), P("data"), P("stage"), P("stage")),
                         out_specs=(P("data"), P("data"), P(("data", "stage")), P(("data", "stage"))),
                         check_vma=False)
```

```python
import functools

import jax
import jax.numpy as jnp
from jax import lax
from jax.experimental import pallas as pl
from jax.experimental.pallas import tpu as pltpu
from jax.sharding import PartitionSpec as P

MESH = pl.DeviceIdType.MESH
f32 = jnp.float32
bf16 = jnp.bfloat16
D = 768
F = 3072
C = 128
H = 64
RING = 4
K = 256
LAG = 6
TW = 512
NS = F // K
C0 = 0.7978845608028654
C1 = 0.044715

WORDS = (
    (0, 0, 26230864, 20222273, 51647560, 37954580, 43192849, 36782609, 20070721, 159986706, 153633849, 268431945, 268435455),
    (0, 0, 21038336, 69284929, 20517156, 54673988, 68293652, 51463234, 71450948, 71440660, 70337585, 54669956, 268435336),
    (0, 67108864, 71319557, 68162628, 18953236, 26415426, 37831457, 21107473, 68232212, 71534915, 75711560, 142885955, 268435455),
    (5, 0, 1118208, 21045523, 68424739, 26427793, 69282073, 68260417, 38020163, 70402617, 35865636, 260342596, 268435455),
    (5, 67108928, 67387412, 26218516, 21106740, 34878465, 17908033, 36782402, 137662740, 69806403, 154289188, 35857027, 268435455),
    (5, 1048592, 19927056, 1053458, 54599937, 43065665, 21074964, 69482563, 69419588, 52707908, 37962308, 71864900, 268435268),
    (66640, 26251289, 73484550, 73687878, 1054278, 69407745, 38027585, 38028323, 37962308, 71508532, 58925602, 268435234, 268435455),
    (100729093, 1054209, 16843009, 1052688, 70320385, 59909187, 76096553, 69481027, 70554162, 71443490, 153367620, 267993668, 268435455),
)
STEPS = 7


def _dot(a, b):
    return jnp.dot(a, b, preferred_element_type=f32)


def _dot_t(a, b):
    return lax.dot_general(a, b, (((0,), (0,)), ((), ())), preferred_element_type=f32)


def _gelu(z):
    q = (C0 * C1) * (z * z)
    p = 0.5 * jnp.tanh(z * (C0 + q)) + 0.5
    u = z * p
    return u.astype(bf16), p + (u * (1.0 - p)) * (2.0 * C0 + 6.0 * q)


def _pipeline(n_st, n_ch, x, g, w1h, w2h, lf, rb, a1, a2, zh, uh, dh,
              w1, w2, w1t, w2t, hb, gb, uw, dw, zb, ub, db, fo, bo,
              wsem, hsem, gsem, psem, lsem, esem, fsem, bsem, osem, rsem, zwsem, zrsem, uwsem, dwsem, ursem, drsem):
    d = lax.axis_index("data")
    s = lax.axis_index("stage")
    last = n_st - 1
    end = n_ch - 1
    pieces = 2 * end
    spill = s < n_st - 2
    even = s % 2 == 0
    top, low = pl.ds(0, H), pl.ds(H, H)

    def peer(k):
        return (d, k)

    def sized(i, small, full):
        short = (i == 0) | (i == end)
        pl.when(short)(small)
        pl.when(jnp.logical_not(short))(full)

    def row(i):
        return jnp.maximum(i * C - H, 0)

    def cols(k):
        return pl.ds(k * K, K)

    def load(src, dst, sem, i):
        at = pl.ds(pl.multiple_of(row(i), H), C)
        return pltpu.make_async_copy(src.at[at], dst.at[i], sem.at[i])

    def load_end(src, dst, sem, i):
        at = pl.ds(0 if i == 0 else (2 * end - 1) * H, H)
        return pltpu.make_async_copy(src.at[at], dst.at[i, top], sem.at[i])

    def landed(buf, sem, i, rows):
        part = buf.at[i, pl.ds(0, rows)]
        pltpu.make_async_copy(part, part, sem.at[i]).wait()

    get_w1 = pltpu.make_async_copy(w1h.at[0], w1, wsem.at[0])
    get_w2 = pltpu.make_async_copy(w2h.at[0], w2, wsem.at[1])

    def load_all(src, dst, sem):
        load_end(src, dst, sem, end).start()

        def f(i, _):
            load(src, dst, sem, i).start()
            return 0
        lax.fori_loop(1, end, f, 0)

    @pl.when(s == 0)
    def _():
        load_end(x, hb, hsem, 0).start()

    get_w1.start()
    get_w2.start()

    @pl.when(s == 0)
    def _():
        load_all(x, hb, hsem)

    @pl.when(s == last)
    def _():
        load_end(g, gb, gsem, 0).start()
        load_all(g, gb, gsem)

    bar = pltpu.get_barrier_semaphore()
    near = (-2, -1, 1, 2)
    for off in near:
        @pl.when((s + off >= 0) & (s + off < n_st))
        def _(off=off):
            pl.semaphore_signal(bar, inc=1, device_id=peer(s + off), device_id_type=MESH)
    for k in range(3, n_st, 2):
        @pl.when(s == 0)
        def _(k=k):
            pl.semaphore_signal(bar, inc=1, device_id=peer(k), device_id_type=MESH)

        @pl.when(s == k)
        def _(k=k):
            pl.semaphore_signal(bar, inc=1, device_id=peer(0), device_id_type=MESH)
    far = jnp.where(s == 0, (n_st - 2) // 2, jnp.where((s % 2 == 1) & (s >= 3), 1, 0))
    peers = jnp.minimum(s, 2) + jnp.minimum(last - s, 2) + far

    def send(src, r, dst, i, ssem, to, dev, rows):
        part = pl.ds(0, rows)
        return pltpu.make_async_remote_copy(src_ref=src.at[r, part], dst_ref=dst.at[i, part], send_sem=ssem.at[0, r],
                                            recv_sem=to.at[i], device_id=peer(dev), device_id_type=MESH)

    def send_f(i, r, rows):
        return send(fo, r, hb, i, fsem, hsem, s + 1, rows)

    def send_b(i, r, rows):
        return send(bo, r, gb, i, bsem, gsem, s - 1, rows)

    def sent_f(i, r):
        sized(i, lambda: send_f(i, r, H).wait_send(), lambda: send_f(i, r, C).wait_send())

    def sent_b(i, r):
        sized(i, lambda: send_b(i, r, H).wait_send(), lambda: send_b(i, r, C).wait_send())

    def first_piece(i):
        return jnp.maximum(2 * i - 1, 0)

    def hand(src, r, k, p, ssem, dev):
        return pltpu.make_async_remote_copy(src_ref=src.at[r, pl.ds(k * H, H)], dst_ref=rb.at[p], send_sem=ssem.at[k, r],
                                            recv_sem=psem.at[p], device_id=peer(dev), device_id_type=MESH)

    def keep(src, r, k, p):
        return pltpu.make_async_copy(src.at[r, pl.ds(k * H, H)], lf.at[p], osem.at[k, r])

    def out_start(src, r, i, ssem, dev):
        p = first_piece(i)
        hand(src, r, 0, p, ssem, dev).start()
        keep(src, r, 0, p).start()

        def more():
            hand(src, r, 1, p + 1, ssem, dev).start()
            keep(src, r, 1, p + 1).start()
        sized(i, lambda: None, more)

    def out_wait(src, r, i, ssem, dev):
        p = first_piece(i)
        hand(src, r, 0, p, ssem, dev).wait_send()
        keep(src, r, 0, p).wait()

        def more():
            hand(src, r, 1, p + 1, ssem, dev).wait_send()
            keep(src, r, 1, p + 1).wait()
        sized(i, lambda: None, more)

    def direct(r, k):
        return pltpu.make_async_remote_copy(src_ref=bo.at[r, top], dst_ref=rb.at[pieces - 1], send_sem=esem.at[k // 2 - 1],
                                            recv_sem=psem.at[pieces - 1], device_id=peer(k), device_id_type=MESH)

    def onward(p, dev):
        return pltpu.make_async_remote_copy(src_ref=rb.at[p], dst_ref=rb.at[p], send_sem=rsem.at[0], recv_sem=psem.at[p],
                                            device_id=peer(dev), device_id_type=MESH)

    def across(p, dev):
        return pltpu.make_async_remote_copy(src_ref=rb.at[p], dst_ref=lf.at[p], send_sem=rsem.at[1], recv_sem=lsem,
                                            device_id=peer(dev), device_id_type=MESH)

    def write_z(i):
        q = lax.rem(i, 2)
        return pltpu.make_async_copy(zb.at[q], zh.at[i], zwsem.at[q])

    def read_z(i):
        q = lax.rem(i, 2)
        return pltpu.make_async_copy(zh.at[i], zb.at[2 + q], zrsem.at[q])

    def rows_of(i, rows):
        first = i == 0
        k = jnp.where(first, end // 2 - 1, lax.div(i - 1, 2))
        at = jnp.where(first, C + H, lax.rem(i - 1, 2) * C)
        return k, pl.ds(pl.multiple_of(at, H), rows)

    def write_ud(src, dst, sem, i, rows):
        k, at = rows_of(i, rows)
        q = lax.rem(i, 2)
        return pltpu.make_async_copy(src.at[q, pl.ds(0, rows)], dst.at[k, at], sem.at[q])

    def done_u(i):
        sized(i, lambda: write_ud(ub, uh, uwsem, i, H).wait(), lambda: write_ud(ub, uh, uwsem, i, C).wait())

    def done_d(i):
        sized(i, lambda: write_ud(db, dh, dwsem, i, H).wait(), lambda: write_ud(db, dh, dwsem, i, C).wait())

    def read_u(k):
        q = lax.rem(k, 2)
        return pltpu.make_async_copy(uh.at[k], uw.at[q], ursem.at[q])

    def read_d(k):
        q = lax.rem(k, 2)
        return pltpu.make_async_copy(dh.at[k], dw.at[q], drsem.at[q])

    def ensure(wait, done, want):
        for j in range(2):
            @pl.when(done + j < want)
            def _(j=j):
                wait(done + j)

    def f_slots(i):
        q = lax.rem(i, 2)
        return lax.rem(i, RING), jnp.where(spill, q, lax.rem(i, 4)), q

    def b_slots(i):
        q = lax.rem(i, 2)
        return lax.rem(i, RING), jnp.where(spill, 2 + q, lax.rem(i, 4)), q

    def f_ready(i, zw, uc):
        r, _, _ = f_slots(i)

        @pl.when(spill)
        def _():
            ensure(lambda j: write_z(j).wait(), zw, i - 1)

        ensure(done_u, uc, i - 1)

        @pl.when(i >= RING)
        def _():
            @pl.when(s < last)
            def _():
                sent_f(i - RING, r)

            @pl.when(s == last)
            def _():
                out_wait(fo, r, i - RING, fsem, s - 1)

    def f_body(i, rows):
        r, zs, q = f_slots(i)
        part = pl.ds(0, rows)
        h = hb[i, part, :]
        tot = None
        for n in range(NS + LAG):
            if n < NS:
                z = _dot(h, w1[:, cols(n)])
            if n >= LAG:
                m = n - LAG
                y = _dot(ub[q, part, cols(m)], w2[cols(m), :])
                tot = y if m == 0 else tot + y
            if n < NS:
                u, gp = _gelu(z)
                zb[zs, part, cols(n)] = gp
                ub[q, part, cols(n)] = u
        fo[r, part, :] = (h.astype(f32) + tot).astype(bf16)

    def f_first(i):
        r, zs, q = f_slots(i)
        get_w1.wait()
        landed(hb, hsem, i, H)
        h = hb[i, top, :]
        for n in range(NS):
            u, gp = _gelu(_dot(h, w1[:, cols(n)]))
            zb[zs, top, cols(n)] = gp
            ub[q, top, cols(n)] = u
        get_w2.wait()
        tot = None
        for n in range(NS):
            y = _dot(ub[q, top, cols(n)], w2[cols(n), :])
            tot = y if n == 0 else tot + y
        fo[r, top, :] = (h.astype(f32) + tot).astype(bf16)

    def f_send(i, rows):
        r, _, _ = f_slots(i)

        @pl.when(s < last)
        def _():
            send_f(i, r, rows).start()

        @pl.when(s == last)
        def _():
            out_start(fo, r, i, fsem, s - 1)

        write_ud(ub, uh, uwsem, i, rows).start()

        @pl.when(spill)
        def _():
            write_z(i).start()

    def forward(i, zw, uc, fresh):
        f_ready(i, zw, uc)

        def small():
            @pl.when(fresh)
            def _():
                f_first(i)

            @pl.when(jnp.logical_not(fresh))
            def _():
                landed(hb, hsem, i, H)
                f_body(i, H)

            @pl.when(i == 0)
            def _():
                pl.semaphore_wait(bar, peers)
                hb[end, low, :] = hb[0, top, :]
            f_send(i, H)

        def full():
            landed(hb, hsem, i, C)
            f_body(i, C)
            f_send(i, C)

            @pl.when(spill & (i == 4))
            def _():
                read_z(0).start()
        sized(i, small, full)

    def b_ready(i, zw, dc):
        r, _, _ = b_slots(i)

        @pl.when(spill)
        def _():
            read_z(i).wait()
            ensure(lambda j: write_z(j).wait(), zw, jnp.minimum(i + 2, n_ch))

            @pl.when(i + 1 < n_ch)
            def _():
                read_z(i + 1).start()

        ensure(done_d, dc, i - 1)

        @pl.when(i >= RING)
        def _():
            @pl.when(s > 0)
            def _():
                sent_b(i - RING, r)

            @pl.when(s == 0)
            def _():
                out_wait(bo, r, i - RING, bsem, s + 1)

    def b_body(i):
        r, zs, q = b_slots(i)
        gg = gb[i]
        tot = None
        for n in range(NS + LAG):
            if n < NS:
                du = _dot(gg, w2t[:, cols(n)])
            if n >= LAG:
                m = n - LAG
                y = _dot(db[q, :, cols(m)], w1t[cols(m), :])
                tot = y if m == 0 else tot + y
            if n < NS:
                db[q, :, cols(n)] = (zb[zs, :, cols(n)] * du).astype(bf16)
        bo[r] = (gg.astype(f32) + tot).astype(bf16)

    def b_send(i, rows):
        r, _, _ = b_slots(i)

        @pl.when(s > 0)
        def _():
            send_b(i, r, rows).start()

        @pl.when(s == 0)
        def _():
            if rows == H:
                @pl.when(i == end)
                def _():
                    for k in range(last, 2, -2):
                        direct(r, k).start()
            out_start(bo, r, i, bsem, s + 1)

        write_ud(db, dh, dwsem, i, rows).start()

    def backward(i, zw, dc):
        b_ready(i, zw, dc)
        sized(i, lambda: landed(gb, gsem, i, H), lambda: landed(gb, gsem, i, C))
        b_body(i)

        def small():
            @pl.when(i == 0)
            def _():
                gb[end, low, :] = gb[0, top, :]
            b_send(i, H)
        sized(i, small, lambda: b_send(i, C))

    def both(i, j, zw, uc, dc):
        f_ready(i, zw, uc)
        b_ready(j, jnp.maximum(zw, i - 1), dc)
        landed(hb, hsem, i, C)
        landed(gb, gsem, j, C)
        f_body(i, C)
        b_body(j)
        b_send(j, C)
        f_send(i, C)

    def prefetch(k, uc, dc):
        ensure(done_u, uc, 2 * k + 3)
        ensure(done_d, dc, 2 * k + 3)
        read_d(k).start()
        read_u(k).start()

    def grad1(k):
        q = lax.rem(k, 2)
        h = hb[pl.ds(2 * k + 1, 2)].reshape(2 * C, D)
        for n in range(F // TW):
            sl = pl.ds(n * TW, TW)
            a1[:, sl] += _dot_t(h, dw[q, :, sl])

    def grad2(k):
        q = lax.rem(k, 2)
        gg = gb[pl.ds(2 * k + 1, 2)].reshape(2 * C, D)
        for n in range(F // TW):
            sl = pl.ds(n * TW, TW)
            a2[sl, :] += _dot_t(uw[q, :, sl], gg)

    def weights(w):
        k = lax.div(w, 2)
        odd = lax.rem(w, 2)

        @pl.when(odd == 0)
        def _():
            read_d(k).wait()
            grad1(k)

        @pl.when(odd == 1)
        def _():
            read_u(k).wait()
            grad2(k)

    def weights_both(w):
        k = lax.div(w, 2)
        read_d(k).wait()
        read_u(k).wait()
        grad1(k)
        grad2(k)

    def relay_step(p):
        piece = rb.at[p]
        pltpu.make_async_copy(piece, piece, psem.at[p]).wait()

        @pl.when(even)
        def _():
            @pl.when(s >= 2)
            def _():
                onward(p, s - 2).start()

            @pl.when(s < n_st - 2)
            def _():
                across(p, s + 1).start()

        @pl.when(jnp.logical_not(even))
        def _():
            @pl.when((s < last) & (p < pieces - 1))
            def _():
                onward(p, s + 2).start()

            @pl.when(s > 1)
            def _():
                across(p, s - 1).start()

    def transposes(fresh):
        @pl.when(fresh)
        def _():
            get_w1.wait()
            get_w2.wait()

        def f(n, _):
            sl = pl.ds(pl.multiple_of(n * 256, 256), 256)
            w1t[sl, :] = w1[:, sl].T
            w2t[:, sl] = w2[sl, :].T
            a1[:, sl] = jnp.zeros((D, 256), f32)
            a2[sl, :] = jnp.zeros((256, D), f32)
            return 0
        lax.fori_loop(0, F // 256, f, 0)

    def step(j, carry):
        word, nf, nb, nw, npf, nr, nt, zw, uc, dc = carry
        op = lax.rem(word, 16)
        is_x = op == 6
        is_f, is_b, is_p = (op == 0) | is_x, (op == 1) | is_x, op == 3

        @pl.when(op < 2)
        def _():
            @pl.when(op == 0)
            def _():
                forward(nf, zw, uc, (nf == 0) & (nt == 0))

            @pl.when(op == 1)
            def _():
                backward(nb, zw, dc)

        @pl.when((op >= 2) & (op < 6))
        def _():
            @pl.when(op == 2)
            def _():
                weights(nw)

            @pl.when(op == 4)
            def _():
                relay_step(nr)

            @pl.when(is_p)
            def _():
                prefetch(npf, uc, dc)

            @pl.when(op == 5)
            def _():
                transposes(nf == 0)

        @pl.when(op >= 6)
        def _():
            @pl.when(is_x)
            def _():
                both(nf, nb, zw, uc, dc)

            @pl.when(op == 8)
            def _():
                weights_both(nw)

            @pl.when(op == 9)
            def _():
                relay_step(nr)
                relay_step(nr + 1)

        zw = jnp.where(is_f, jnp.maximum(zw, nf - 1), zw)
        zw = jnp.where(is_b, jnp.maximum(zw, jnp.minimum(nb + 2, n_ch)), zw)
        uc = jnp.where(is_f, jnp.maximum(uc, nf - 1), uc)
        uc = jnp.where(is_p, jnp.maximum(uc, 2 * npf + 3), uc)
        dc = jnp.where(is_b, jnp.maximum(dc, nb - 1), dc)
        dc = jnp.where(is_p, jnp.maximum(dc, 2 * npf + 3), dc)
        one = lambda k: jnp.where(k, 1, 0)
        two = lambda k, m: jnp.where(op == k, 1, jnp.where(op == m, 2, 0))
        return (lax.div(word, 16), nf + one(is_f), nb + one(is_b), nw + two(2, 8), npf + one(is_p), nr + two(4, 9), nt + one(op == 5),
                zw, uc, dc)

    zero = s * 0
    words = []
    for k in range(len(WORDS[0])):
        word = zero
        for q in range(n_st):
            word = jnp.where(s == q, WORDS[q][k], word)
        words.append(word)

    def work(k, carry):
        word = words[0]
        for q in range(1, len(words)):
            word = jnp.where(k == q, words[q], word)
        out = lax.fori_loop(0, STEPS, step, (word, *carry))
        return out[1:]

    lax.fori_loop(0, len(words), work, (zero,) * 9)

    for j in range(RING):
        i = zero + (n_ch - RING + j)
        r = (n_ch - RING + j) % RING

        @pl.when(s < last)
        def _(i=i, r=r):
            sent_f(i, r)

        @pl.when(s == last)
        def _(i=i, r=r):
            out_wait(fo, r, i, fsem, s - 1)

        @pl.when(s > 0)
        def _(i=i, r=r):
            sent_b(i, r)

        @pl.when(s == 0)
        def _(i=i, r=r):
            out_wait(bo, r, i, bsem, s + 1)

    @pl.when(s == 0)
    def _():
        for k in range(last, 2, -2):
            direct(end % RING, k).wait_send()

    def all_of(ref, sem, count):
        part = ref.at[pl.ds(0, count)]
        pltpu.make_async_copy(part, part, sem).wait()

    @pl.when(even)
    def _():
        @pl.when(s >= 2)
        def _():
            all_of(rb, rsem.at[0], pieces)

        @pl.when(s < n_st - 2)
        def _():
            all_of(rb, rsem.at[1], pieces)

        @pl.when(s > 0)
        def _():
            all_of(lf, lsem, pieces)

    @pl.when(jnp.logical_not(even))
    def _():
        @pl.when(s < last)
        def _():
            all_of(rb, rsem.at[0], pieces - 1)
            all_of(lf, lsem, pieces)

        @pl.when(s > 1)
        def _():
            all_of(rb, rsem.at[1], pieces)


def _write_out(lf, rb, a1, a2, y, dx, d1, d2, lb, sem_w, sem_r, sem_o):
    s = lax.axis_index("stage")
    parts = 4
    big = []
    for p in range(parts):
        r1 = pl.ds(p * (D // parts), D // parts)
        r2 = pl.ds(p * (F // parts), F // parts)
        big.append(pltpu.make_async_copy(a1.at[r1], d1.at[0, r1], sem_w.at[0, p]))
        big.append(pltpu.make_async_copy(a2.at[r2], d2.at[0, r2], sem_w.at[1, p]))
    back = pltpu.make_async_copy(lf, lb, sem_r)
    back.start()
    for c in big:
        c.start()

    def rest(mine, other):
        near = pltpu.make_async_copy(rb, mine, sem_o.at[0])
        near.start()
        back.wait()
        far = pltpu.make_async_copy(lb, other, sem_o.at[1])
        far.start()
        near.wait()
        far.wait()

    @pl.when(s % 2 == 0)
    def _():
        rest(y, dx)

    @pl.when(s % 2 == 1)
    def _():
        rest(dx, y)

    for c in big:
        c.wait()


def solution(mesh):
    n_st = mesh.shape["stage"]

    def body(x, g, w1, w2):
        tokens = x.shape[0] * x.shape[1]
        n_ch = tokens // C + 1
        hbm = pl.BlockSpec(memory_space=pltpu.HBM)
        vmem = pl.BlockSpec(memory_space=pltpu.VMEM)
        dma = pltpu.SemaphoreType.DMA
        pieces = (tokens // H, H, D)
        groups = (tokens // (2 * C), 2 * C, F)
        params = dict(has_side_effects=True)
        rows = (n_ch, C, D)
        slabs = (2, 2 * C, F)
        lf, rb, a1, a2, _, _, _ = pl.pallas_call(
            functools.partial(_pipeline, n_st, n_ch),
            out_shape=[pltpu.HBM(pieces, bf16), pltpu.VMEM(pieces, bf16), pltpu.VMEM((D, F), f32), pltpu.VMEM((F, D), f32),
                       pltpu.HBM((n_ch, C, F), f32), pltpu.HBM(groups, bf16), pltpu.HBM(groups, bf16)],
            in_specs=[hbm] * 4,
            out_specs=[hbm] + [vmem] * 3 + [hbm] * 3,
            scratch_shapes=[
                pltpu.VMEM((D, F), bf16), pltpu.VMEM((F, D), bf16), pltpu.VMEM((F, D), bf16), pltpu.VMEM((D, F), bf16),
                pltpu.VMEM(rows, bf16), pltpu.VMEM(rows, bf16), pltpu.VMEM(slabs, bf16), pltpu.VMEM(slabs, bf16),
                pltpu.VMEM((4, C, F), f32), pltpu.VMEM((2, C, F), bf16), pltpu.VMEM((2, C, F), bf16),
                pltpu.VMEM((RING, C, D), bf16), pltpu.VMEM((RING, C, D), bf16),
                dma((2,)), dma((n_ch,)), dma((n_ch,)), dma((pieces[0],)), dma, dma((n_st // 2 - 1,)), dma((2, RING)), dma((2, RING)),
                dma((2, RING)), dma((2,)), dma((2,)), dma((2,)), dma((2,)), dma((2,)), dma((2,)), dma((2,)),
            ],
            compiler_params=pltpu.CompilerParams(collective_id=0, vmem_limit_bytes=45_000_000, **params),
            name="pipeline",
        )(x.reshape(tokens, D), g.reshape(tokens, D), w1, w2)
        y, dx, d1, d2 = pl.pallas_call(
            _write_out,
            out_shape=[pltpu.HBM(pieces, bf16), pltpu.HBM(pieces, bf16), pltpu.HBM((1, D, F), f32), pltpu.HBM((1, F, D), f32)],
            in_specs=[hbm, vmem, vmem, vmem],
            out_specs=[hbm] * 4,
            scratch_shapes=[pltpu.VMEM(pieces, bf16), dma((2, 4)), dma, dma((2,))],
            compiler_params=pltpu.CompilerParams(vmem_limit_bytes=4_000_000, **params),
            name="write_out",
        )(pltpu.with_memory_space_constraint(lf, pltpu.HBM), rb, a1, a2)
        return y.reshape(x.shape), dx.reshape(x.shape), d1, d2

    return jax.shard_map(body, mesh=mesh,
                         in_specs=(P("data"), P("data"), P("stage"), P("stage")),
                         out_specs=(P("data"), P("data"), P(("data", "stage")), P(("data", "stage"))),
                         check_vma=False)
```

```python
import functools

import jax
import jax.numpy as jnp
from jax import lax
from jax.experimental import pallas as pl
from jax.experimental.pallas import tpu as pltpu
from jax.sharding import PartitionSpec as P

MESH = pl.DeviceIdType.MESH
f32 = jnp.float32
bf16 = jnp.bfloat16
D = 768
F = 3072
C = 128
H = 64
RING = 4
K = 256
LAG = 6
TW = 512
SL = 3
NS = F // K
C0 = 0.7978845608028654
C1 = 0.044715

WORDS = (
    (0, 0, 17892608, 38016049, 18121010, 59905076, 17965348, 153171092, 19997076, 69481490, 75798915, 268387401, 268435455),
    (0, 0, 21038336, 153172241, 71440675, 152322833, 37831730, 21053732, 34882116, 71383321, 70796337, 268404792, 268435455),
    (5, 0, 71565316, 21038148, 71439121, 51462466, 54796865, 21107219, 70390337, 76820753, 155460132, 160662083, 268435234),
    (0, 5242880, 16781328, 52502833, 69309457, 71385906, 68428098, 71573828, 26293281, 52707985, 71582276, 36254275, 268435332),
    (5, 67108928, 21250068, 18092036, 17379728, 21039377, 54596424, 17908242, 70534212, 138691362, 54805033, 267944835, 268435455),
    (5, 1048592, 50336016, 2167041, 51978257, 21107265, 71504708, 69485076, 35930948, 43136066, 71516745, 76096547, 268435268),
    (66565, 151585092, 67702801, 1054992, 1052817, 20975641, 68423940, 71582532, 36848195, 153240626, 136520242, 253895219, 268435455),
    (65797, 1052689, 16843009, 1052688, 16843009, 70395955, 43222073, 69411881, 160580754, 76751764, 76827010, 268435444, 268435455),
)
STEPS = 7


def _dot(a, b):
    return jnp.dot(a, b, preferred_element_type=f32)


def _dot_t(a, b):
    return lax.dot_general(a, b, (((0,), (0,)), ((), ())), preferred_element_type=f32)


def _gelu(z):
    q = (C0 * C1) * (z * z)
    p = 0.5 * jnp.tanh(z * (C0 + q)) + 0.5
    u = z * p
    return u.astype(bf16), p + (u * (1.0 - p)) * (2.0 * C0 + 6.0 * q)


def _pipeline(n_st, n_ch, *refs):
    dma = pltpu.SemaphoreType.DMA
    pl.run_scoped(functools.partial(_work, n_st, n_ch, *refs), dma((2, SL)), dma((n_st // 2 - 1,)), dma((RING,)), dma((RING,)), dma((RING,)),
                  dma((2,)), dma((2,)), dma((2,)), dma((2,)), dma((2,)), dma((2,)), dma((2,)))


def _work(n_st, n_ch, x, g, w1h, w2h, lf, rb, a1, a2, zh, uh, dh,
          w1, w2, w1t, w2t, hb, gb, uw, dw, zb, ub, db, fo, bo,
          hsem, gsem, psem, lsem, wsem, esem, fsem, bsem, osem, rsem, zwsem, zrsem, uwsem, dwsem, ursem, drsem):
    d = lax.axis_index("data")
    s = lax.axis_index("stage")
    last = n_st - 1
    end = n_ch - 1
    pieces = 2 * end
    spill = s < n_st - 2
    even = s % 2 == 0
    top, low = pl.ds(0, H), pl.ds(H, H)

    def peer(k):
        return (d, k)

    def sized(i, small, full):
        short = (i == 0) | (i == end)
        pl.when(short)(small)
        pl.when(jnp.logical_not(short))(full)

    def row(i):
        return jnp.maximum(i * C - H, 0)

    def cols(k):
        return pl.ds(k * K, K)

    def load(src, dst, sem, i):
        at = pl.ds(pl.multiple_of(row(i), H), C)
        return pltpu.make_async_copy(src.at[at], dst.at[i], sem.at[i])

    def load_end(src, dst, sem, i):
        at = pl.ds(0 if i == 0 else (2 * end - 1) * H, H)
        return pltpu.make_async_copy(src.at[at], dst.at[i, top], sem.at[i])

    def landed(buf, sem, i, rows):
        part = buf.at[i, pl.ds(0, rows)]
        pltpu.make_async_copy(part, part, sem.at[i]).wait()

    def piece(n):
        return pl.ds(n * (F // SL), F // SL)

    def get_w1(n):
        return pltpu.make_async_copy(w1h.at[0, :, piece(n)], w1.at[:, piece(n)], wsem.at[0, n])

    def get_w2(n):
        return pltpu.make_async_copy(w2h.at[0, piece(n)], w2.at[piece(n)], wsem.at[1, n])

    def have_weights():
        for n in range(SL):
            get_w1(n).wait()
        for n in range(SL):
            get_w2(n).wait()

    def load_all(src, dst, sem):
        load_end(src, dst, sem, end).start()

        def f(i, _):
            load(src, dst, sem, i).start()
            return 0
        lax.fori_loop(1, end, f, 0)

    @pl.when(s == 0)
    def _():
        load_end(x, hb, hsem, 0).start()

    for n in range(SL):
        get_w1(n).start()
    for n in range(SL):
        get_w2(n).start()

    @pl.when(s == 0)
    def _():
        load_all(x, hb, hsem)

    @pl.when(s == last)
    def _():
        load_end(g, gb, gsem, 0).start()
        load_all(g, gb, gsem)

    bar = pltpu.get_barrier_semaphore()
    near = (-2, -1, 1, 2)
    for off in near:
        @pl.when((s + off >= 0) & (s + off < n_st))
        def _(off=off):
            pl.semaphore_signal(bar, inc=1, device_id=peer(s + off), device_id_type=MESH)
    for k in range(3, n_st, 2):
        @pl.when(s == 0)
        def _(k=k):
            pl.semaphore_signal(bar, inc=1, device_id=peer(k), device_id_type=MESH)

        @pl.when(s == k)
        def _(k=k):
            pl.semaphore_signal(bar, inc=1, device_id=peer(0), device_id_type=MESH)
    far = jnp.where(s == 0, (n_st - 2) // 2, jnp.where((s % 2 == 1) & (s >= 3), 1, 0))
    peers = jnp.minimum(s, 2) + jnp.minimum(last - s, 2) + far

    def send(src, r, dst, i, ssem, to, dev, rows):
        part = pl.ds(0, rows)
        return pltpu.make_async_remote_copy(src_ref=src.at[r, part], dst_ref=dst.at[i, part], send_sem=ssem.at[r],
                                            recv_sem=to.at[i], device_id=peer(dev), device_id_type=MESH)

    def send_f(i, r, rows):
        return send(fo, r, hb, i, fsem, hsem, s + 1, rows)

    def send_b(i, r, rows):
        return send(bo, r, gb, i, bsem, gsem, s - 1, rows)

    def sent_f(i, r):
        sized(i, lambda: send_f(i, r, H).wait_send(), lambda: send_f(i, r, C).wait_send())

    def sent_b(i, r):
        sized(i, lambda: send_b(i, r, H).wait_send(), lambda: send_b(i, r, C).wait_send())

    def first_piece(i):
        return jnp.maximum(2 * i - 1, 0)

    def hand(src, r, k, p, ssem, dev):
        return pltpu.make_async_remote_copy(src_ref=src.at[r, pl.ds(k * H, H)], dst_ref=rb.at[p], send_sem=ssem.at[r],
                                            recv_sem=psem.at[p], device_id=peer(dev), device_id_type=MESH)

    def keep(src, r, k, p):
        return pltpu.make_async_copy(src.at[r, pl.ds(k * H, H)], lf.at[p], osem.at[r])

    def out_start(src, r, i, ssem, dev):
        p = first_piece(i)
        hand(src, r, 0, p, ssem, dev).start()
        keep(src, r, 0, p).start()

        def more():
            hand(src, r, 1, p + 1, ssem, dev).start()
            keep(src, r, 1, p + 1).start()
        sized(i, lambda: None, more)

    def out_wait(src, r, i, ssem):
        def both(rows):
            part = src.at[r, pl.ds(0, rows)]
            pltpu.make_async_copy(part, part, ssem.at[r]).wait()
            pltpu.make_async_copy(part, part, osem.at[r]).wait()
        sized(i, lambda: both(H), lambda: both(C))

    def direct(r, k):
        return pltpu.make_async_remote_copy(src_ref=bo.at[r, top], dst_ref=rb.at[pieces - 1], send_sem=esem.at[k // 2 - 1],
                                            recv_sem=psem.at[pieces - 1], device_id=peer(k), device_id_type=MESH)

    def onward(p, dev):
        return pltpu.make_async_remote_copy(src_ref=rb.at[p], dst_ref=rb.at[p], send_sem=rsem.at[0], recv_sem=psem.at[p],
                                            device_id=peer(dev), device_id_type=MESH)

    def across(p, dev):
        return pltpu.make_async_remote_copy(src_ref=rb.at[p], dst_ref=lf.at[p], send_sem=rsem.at[1], recv_sem=lsem,
                                            device_id=peer(dev), device_id_type=MESH)

    def write_z(i):
        q = lax.rem(i, 2)
        return pltpu.make_async_copy(zb.at[q], zh.at[i], zwsem.at[q])

    def read_z(i):
        q = lax.rem(i, 2)
        return pltpu.make_async_copy(zh.at[i], zb.at[2 + q], zrsem.at[q])

    def rows_of(i, rows):
        first = i == 0
        k = jnp.where(first, end // 2 - 1, lax.div(i - 1, 2))
        at = jnp.where(first, C + H, lax.rem(i - 1, 2) * C)
        return k, pl.ds(pl.multiple_of(at, H), rows)

    def write_ud(src, dst, sem, i, rows):
        k, at = rows_of(i, rows)
        q = lax.rem(i, 2)
        return pltpu.make_async_copy(src.at[q, pl.ds(0, rows)], dst.at[k, at], sem.at[q])

    def done_u(i):
        sized(i, lambda: write_ud(ub, uh, uwsem, i, H).wait(), lambda: write_ud(ub, uh, uwsem, i, C).wait())

    def done_d(i):
        sized(i, lambda: write_ud(db, dh, dwsem, i, H).wait(), lambda: write_ud(db, dh, dwsem, i, C).wait())

    def read_u(k):
        q = lax.rem(k, 2)
        return pltpu.make_async_copy(uh.at[k], uw.at[q], ursem.at[q])

    def read_d(k):
        q = lax.rem(k, 2)
        return pltpu.make_async_copy(dh.at[k], dw.at[q], drsem.at[q])

    def ensure(wait, done, want):
        for j in range(2):
            @pl.when(done + j < want)
            def _(j=j):
                wait(done + j)

    def f_slots(i):
        q = lax.rem(i, 2)
        return lax.rem(i, RING), jnp.where(spill, q, lax.rem(i, 4)), q

    def b_slots(i):
        q = lax.rem(i, 2)
        return lax.rem(i, RING), jnp.where(spill, 2 + q, lax.rem(i, 4)), q

    def f_ready(i, r, zw, uc):
        @pl.when(spill)
        def _():
            ensure(lambda j: write_z(j).wait(), zw, i - 1)

        ensure(done_u, uc, i - 1)

        @pl.when(i >= RING)
        def _():
            @pl.when(s < last)
            def _():
                sent_f(i - RING, r)

            @pl.when(s == last)
            def _():
                out_wait(fo, r, i - RING, fsem)

    def f_body(i, rows, slots):
        r, zs, q = slots
        part = pl.ds(0, rows)
        h = hb[i, part, :]
        tot = None
        for n in range(NS + LAG):
            if n < NS:
                z = _dot(h, w1[:, cols(n)])
            if n >= LAG:
                m = n - LAG
                y = _dot(ub[q, part, cols(m)], w2[cols(m), :])
                tot = y if m == 0 else tot + y
            if n < NS:
                u, gp = _gelu(z)
                zb[zs, part, cols(n)] = gp
                ub[q, part, cols(n)] = u
        fo[r, part, :] = (h.astype(f32) + tot).astype(bf16)

    def f_first(i, slots):
        r, zs, q = slots
        landed(hb, hsem, i, H)
        h = hb[i, top, :]
        per = NS // SL
        for n in range(NS):
            if n % per == 0:
                get_w1(n // per).wait()
            u, gp = _gelu(_dot(h, w1[:, cols(n)]))
            zb[zs, top, cols(n)] = gp
            ub[q, top, cols(n)] = u
        tot = None
        for n in range(SL):
            get_w2(n).wait()
            y = _dot(ub[q, top, piece(n)], w2[piece(n), :])
            tot = y if n == 0 else tot + y
        fo[r, top, :] = (h.astype(f32) + tot).astype(bf16)

    def f_send(i, rows, r):
        @pl.when(s < last)
        def _():
            send_f(i, r, rows).start()

        @pl.when(s == last)
        def _():
            out_start(fo, r, i, fsem, s - 1)

        write_ud(ub, uh, uwsem, i, rows).start()

        @pl.when(spill)
        def _():
            write_z(i).start()

    def forward(i, zw, uc, fresh):
        slots = f_slots(i)
        r = slots[0]
        f_ready(i, r, zw, uc)

        def small():
            @pl.when(fresh)
            def _():
                f_first(i, slots)

            @pl.when(jnp.logical_not(fresh))
            def _():
                landed(hb, hsem, i, H)
                f_body(i, H, slots)

            @pl.when(i == 0)
            def _():
                pl.semaphore_wait(bar, peers)
                hb[end, low, :] = hb[0, top, :]
            f_send(i, H, r)

        def full():
            landed(hb, hsem, i, C)
            f_body(i, C, slots)
            f_send(i, C, r)

            @pl.when(spill & (i == 4))
            def _():
                read_z(0).start()
        sized(i, small, full)

    def b_ready(i, r, zw, dc):
        @pl.when(spill)
        def _():
            read_z(i).wait()
            ensure(lambda j: write_z(j).wait(), zw, jnp.minimum(i + 2, n_ch))

            @pl.when(i + 1 < n_ch)
            def _():
                read_z(i + 1).start()

        ensure(done_d, dc, i - 1)

        @pl.when(i >= RING)
        def _():
            @pl.when(s > 0)
            def _():
                sent_b(i - RING, r)

            @pl.when(s == 0)
            def _():
                out_wait(bo, r, i - RING, bsem)

    def b_body(i, slots):
        r, zs, q = slots
        gg = gb[i]
        tot = None
        for n in range(NS + LAG):
            if n < NS:
                du = _dot(gg, w2t[:, cols(n)])
            if n >= LAG:
                m = n - LAG
                y = _dot(db[q, :, cols(m)], w1t[cols(m), :])
                tot = y if m == 0 else tot + y
            if n < NS:
                db[q, :, cols(n)] = (zb[zs, :, cols(n)] * du).astype(bf16)
        bo[r] = (gg.astype(f32) + tot).astype(bf16)

    def b_send(i, rows, r):
        @pl.when(s > 0)
        def _():
            send_b(i, r, rows).start()

        @pl.when(s == 0)
        def _():
            if rows == H:
                @pl.when(i == end)
                def _():
                    for k in range(last, 2, -2):
                        direct(r, k).start()
            out_start(bo, r, i, bsem, s + 1)

        write_ud(db, dh, dwsem, i, rows).start()

    def backward(i, zw, dc):
        slots = b_slots(i)
        r = slots[0]
        b_ready(i, r, zw, dc)

        def small():
            landed(gb, gsem, i, H)
            b_body(i, slots)

            @pl.when(i == 0)
            def _():
                gb[end, low, :] = gb[0, top, :]
            b_send(i, H, r)

        def full():
            landed(gb, gsem, i, C)
            b_body(i, slots)
            b_send(i, C, r)
        sized(i, small, full)

    def prefetch(k, uc, dc):
        ensure(done_u, uc, 2 * k + 3)
        ensure(done_d, dc, 2 * k + 3)
        read_d(k).start()
        read_u(k).start()

    def grad1(k):
        q = lax.rem(k, 2)
        h = hb[pl.ds(2 * k + 1, 2)].reshape(2 * C, D)
        for n in range(F // TW):
            sl = pl.ds(n * TW, TW)
            a1[:, sl] += _dot_t(h, dw[q, :, sl])

    def grad2(k):
        q = lax.rem(k, 2)
        gg = gb[pl.ds(2 * k + 1, 2)].reshape(2 * C, D)
        for n in range(F // TW):
            sl = pl.ds(n * TW, TW)
            a2[sl, :] += _dot_t(uw[q, :, sl], gg)

    def weights(w):
        k = lax.div(w, 2)
        odd = lax.rem(w, 2)

        @pl.when(odd == 0)
        def _():
            read_d(k).wait()
            grad1(k)

        @pl.when(odd == 1)
        def _():
            read_u(k).wait()
            grad2(k)

    def weights_both(w):
        k = lax.div(w, 2)
        read_d(k).wait()
        read_u(k).wait()
        grad1(k)
        grad2(k)

    def relay_step(p):
        piece = rb.at[p]
        pltpu.make_async_copy(piece, piece, psem.at[p]).wait()

        @pl.when(even)
        def _():
            @pl.when(s >= 2)
            def _():
                onward(p, s - 2).start()

            @pl.when(s < n_st - 2)
            def _():
                across(p, s + 1).start()

        @pl.when(jnp.logical_not(even))
        def _():
            @pl.when((s < last) & (p < pieces - 1))
            def _():
                onward(p, s + 2).start()

            @pl.when(s > 1)
            def _():
                across(p, s - 1).start()

    def transposes(fresh):
        pl.when(fresh)(have_weights)

        def f(n, _):
            sl = pl.ds(pl.multiple_of(n * 256, 256), 256)
            w1t[sl, :] = w1[:, sl].T
            w2t[:, sl] = w2[sl, :].T
            a1[:, sl] = jnp.zeros((D, 256), f32)
            a2[sl, :] = jnp.zeros((256, D), f32)
            return 0
        lax.fori_loop(0, F // 256, f, 0)

    def step(j, carry):
        word, nf, nb, nw, npf, nr, nt, zw, uc, dc = carry
        op = lax.rem(word, 16)
        is_f, is_b, is_p = op == 0, op == 1, op == 3

        @pl.when(op < 2)
        def _():
            @pl.when(is_f)
            def _():
                forward(nf, zw, uc, (nf == 0) & (nt == 0))

            @pl.when(is_b)
            def _():
                backward(nb, zw, dc)

        @pl.when((op >= 2) & (op < 6))
        def _():
            @pl.when(op == 2)
            def _():
                weights(nw)

            @pl.when(op == 4)
            def _():
                relay_step(nr)

            @pl.when(is_p)
            def _():
                prefetch(npf, uc, dc)

            @pl.when(op == 5)
            def _():
                transposes(nf == 0)

        @pl.when(op >= 6)
        def _():
            @pl.when(op == 8)
            def _():
                weights_both(nw)

            @pl.when(op == 9)
            def _():
                relay_step(nr)
                relay_step(nr + 1)

        zw = jnp.where(is_f, jnp.maximum(zw, nf - 1), zw)
        zw = jnp.where(is_b, jnp.maximum(zw, jnp.minimum(nb + 2, n_ch)), zw)
        uc = jnp.where(is_f, jnp.maximum(uc, nf - 1), uc)
        uc = jnp.where(is_p, jnp.maximum(uc, 2 * npf + 3), uc)
        dc = jnp.where(is_b, jnp.maximum(dc, nb - 1), dc)
        dc = jnp.where(is_p, jnp.maximum(dc, 2 * npf + 3), dc)
        one = lambda k: jnp.where(k, 1, 0)
        two = lambda k, m: jnp.where(op == k, 1, jnp.where(op == m, 2, 0))
        return (lax.div(word, 16), nf + one(is_f), nb + one(is_b), nw + two(2, 8), npf + one(is_p), nr + two(4, 9), nt + one(op == 5),
                zw, uc, dc)

    zero = s * 0
    words = []
    for k in range(len(WORDS[0])):
        word = zero
        for q in range(n_st):
            word = jnp.where(s == q, WORDS[q][k], word)
        words.append(word)

    def work(k, carry):
        word = words[0]
        for q in range(1, len(words)):
            word = jnp.where(k == q, words[q], word)
        out = lax.fori_loop(0, STEPS, step, (word, *carry))
        return out[1:]

    lax.fori_loop(0, len(words), work, (zero,) * 9)

    for j in range(RING):
        i = zero + (n_ch - RING + j)
        r = (n_ch - RING + j) % RING

        @pl.when(s < last)
        def _(i=i, r=r):
            sent_f(i, r)

        @pl.when(s == last)
        def _(i=i, r=r):
            out_wait(fo, r, i, fsem)

        @pl.when(s > 0)
        def _(i=i, r=r):
            sent_b(i, r)

        @pl.when(s == 0)
        def _(i=i, r=r):
            out_wait(bo, r, i, bsem)

    @pl.when(s == 0)
    def _():
        for k in range(last, 2, -2):
            direct(end % RING, k).wait_send()

    def all_of(ref, sem, count):
        part = ref.at[pl.ds(0, count)]
        pltpu.make_async_copy(part, part, sem).wait()

    @pl.when(even)
    def _():
        @pl.when(s >= 2)
        def _():
            all_of(rb, rsem.at[0], pieces)

        @pl.when(s < n_st - 2)
        def _():
            all_of(rb, rsem.at[1], pieces)

        @pl.when(s > 0)
        def _():
            all_of(lf, lsem, pieces)

    @pl.when(jnp.logical_not(even))
    def _():
        @pl.when(s < last)
        def _():
            all_of(rb, rsem.at[0], pieces - 1)
            all_of(lf, lsem, pieces)

        @pl.when(s > 1)
        def _():
            all_of(rb, rsem.at[1], pieces)


def _write_out(lf, rb, a1, a2, y, dx, d1, d2, lb, sem_w, sem_r, sem_o):
    s = lax.axis_index("stage")
    parts = 4
    big = []
    for p in range(parts):
        r1 = pl.ds(p * (D // parts), D // parts)
        r2 = pl.ds(p * (F // parts), F // parts)
        big.append(pltpu.make_async_copy(a1.at[r1], d1.at[0, r1], sem_w.at[0, p]))
        big.append(pltpu.make_async_copy(a2.at[r2], d2.at[0, r2], sem_w.at[1, p]))
    back = pltpu.make_async_copy(lf, lb, sem_r)
    back.start()
    for c in big:
        c.start()

    def rest(mine, other):
        near = pltpu.make_async_copy(rb, mine, sem_o.at[0])
        near.start()
        back.wait()
        far = pltpu.make_async_copy(lb, other, sem_o.at[1])
        far.start()
        near.wait()
        far.wait()

    @pl.when(s % 2 == 0)
    def _():
        rest(y, dx)

    @pl.when(s % 2 == 1)
    def _():
        rest(dx, y)

    for c in big:
        c.wait()


def solution(mesh):
    n_st = mesh.shape["stage"]

    def body(x, g, w1, w2):
        tokens = x.shape[0] * x.shape[1]
        n_ch = tokens // C + 1
        hbm = pl.BlockSpec(memory_space=pltpu.HBM)
        vmem = pl.BlockSpec(memory_space=pltpu.VMEM)
        dma = pltpu.SemaphoreType.DMA
        pieces = (tokens // H, H, D)
        groups = (tokens // (2 * C), 2 * C, F)
        params = dict(has_side_effects=True)
        rows = (n_ch, C, D)
        slabs = (2, 2 * C, F)
        lf, rb, a1, a2, _, _, _ = pl.pallas_call(
            functools.partial(_pipeline, n_st, n_ch),
            out_shape=[pltpu.HBM(pieces, bf16), pltpu.VMEM(pieces, bf16), pltpu.VMEM((D, F), f32), pltpu.VMEM((F, D), f32),
                       pltpu.HBM((n_ch, C, F), f32), pltpu.HBM(groups, bf16), pltpu.HBM(groups, bf16)],
            in_specs=[hbm] * 4,
            out_specs=[hbm] + [vmem] * 3 + [hbm] * 3,
            scratch_shapes=[
                pltpu.VMEM((D, F), bf16), pltpu.VMEM((F, D), bf16), pltpu.VMEM((F, D), bf16), pltpu.VMEM((D, F), bf16),
                pltpu.VMEM(rows, bf16), pltpu.VMEM(rows, bf16), pltpu.VMEM(slabs, bf16), pltpu.VMEM(slabs, bf16),
                pltpu.VMEM((4, C, F), f32), pltpu.VMEM((2, C, F), bf16), pltpu.VMEM((2, C, F), bf16),
                pltpu.VMEM((RING, C, D), bf16), pltpu.VMEM((RING, C, D), bf16),
                dma((n_ch,)), dma((n_ch,)), dma((pieces[0],)), dma,
            ],
            compiler_params=pltpu.CompilerParams(collective_id=0, vmem_limit_bytes=45_000_000, **params),
            name="pipeline",
        )(x.reshape(tokens, D), g.reshape(tokens, D), w1, w2)
        y, dx, d1, d2 = pl.pallas_call(
            _write_out,
            out_shape=[pltpu.HBM(pieces, bf16), pltpu.HBM(pieces, bf16), pltpu.HBM((1, D, F), f32), pltpu.HBM((1, F, D), f32)],
            in_specs=[hbm, vmem, vmem, vmem],
            out_specs=[hbm] * 4,
            scratch_shapes=[pltpu.VMEM(pieces, bf16), dma((2, 4)), dma, dma((2,))],
            compiler_params=pltpu.CompilerParams(vmem_limit_bytes=4_000_000, **params),
            name="write_out",
        )(pltpu.with_memory_space_constraint(lf, pltpu.HBM), rb, a1, a2)
        return y.reshape(x.shape), dx.reshape(x.shape), d1, d2

    return jax.shard_map(body, mesh=mesh,
                         in_specs=(P("data"), P("data"), P("stage"), P("stage")),
                         out_specs=(P("data"), P("data"), P(("data", "stage")), P(("data", "stage"))),
                         check_vma=False)
```

```python
import functools

import jax
import jax.numpy as jnp
from jax import lax
from jax.experimental import pallas as pl
from jax.experimental.pallas import tpu as pltpu
from jax.sharding import PartitionSpec as P

MESH = pl.DeviceIdType.MESH
f32 = jnp.float32
bf16 = jnp.bfloat16
D = 768
F = 3072
C = 128
H = 64
RING = 3
K = 256
LAG = 6
TW = 512
SL = 3
NS = F // K
C0 = 0.7978845608028654
C1 = 0.044715

WORDS = (
    (0, 0, 26280016, 69280532, 69288721, 153174850, 18105121, 71406360, 17994514, 76780098, 143800609, 268432532, 268435455),
    (0, 83886080, 21037056, 43066177, 21173313, 71578148, 69473313, 20190353, 21119379, 71386148, 69485075, 35881748, 268435272),
    (5, 4194304, 67387392, 71385108, 35734337, 154353937, 17962002, 68294947, 19997714, 54674577, 37979186, 38020249, 268435442),
    (5, 0, 51384321, 34685185, 18952771, 26493970, 54673700, 19153939, 21250345, 37898545, 37962788, 54805540, 268432514),
    (5, 71303172, 67191809, 9520129, 9703696, 17892401, 20193602, 18039076, 43272513, 153232436, 36848275, 36839986, 268435442),
    (5, 16842768, 18022416, 16843009, 20058132, 26362898, 36802884, 138691396, 38024228, 69419588, 69420068, 76690498, 268435272),
    (66565, 1638724, 26251284, 68194561, 16859152, 1311040, 18088724, 154420244, 35857044, 76059700, 58925619, 268431912, 268435455),
    (16843013, 1052688, 16843009, 1052688, 16843009, 54675747, 71902024, 71533108, 71447620, 53027890, 38019657, 71582786, 268435444),
)
STEPS = 7


def _dot(a, b):
    return jnp.dot(a, b, preferred_element_type=f32)


def _dot_t(a, b):
    return lax.dot_general(a, b, (((0,), (0,)), ((), ())), preferred_element_type=f32)


def _gelu(z):
    q = (C0 * C1) * (z * z)
    p = 0.5 * jnp.tanh(z * (C0 + q)) + 0.5
    u = z * p
    return u.astype(bf16), p + (u * (1.0 - p)) * (2.0 * C0 + 6.0 * q)


def _pipeline(n_st, n_ch, *refs):
    dma = pltpu.SemaphoreType.DMA
    pl.run_scoped(functools.partial(_work, n_st, n_ch, *refs), dma((2, SL)), dma((n_st // 2 - 1,)), dma((RING,)), dma((RING,)), dma((RING,)),
                  dma((2,)), dma((2,)), dma((2,)), dma((2,)), dma((2,)), dma((2,)), dma((2,)))


def _work(n_st, n_ch, x, g, w1h, w2h, lf, rb, a1, a2, zh, uh, dh,
          w1, w2, w1t, w2t, hb, gb, uw, dw, zb, ub, db, fo, bo,
          hsem, gsem, psem, lsem, wsem, esem, fsem, bsem, osem, rsem, zwsem, zrsem, uwsem, dwsem, ursem, drsem):
    d = lax.axis_index("data")
    s = lax.axis_index("stage")
    last = n_st - 1
    end = n_ch - 1
    pieces = 2 * end
    spill = s < n_st - 2
    even = s % 2 == 0
    top, low = pl.ds(0, H), pl.ds(H, H)

    def peer(k):
        return (d, k)

    def sized(i, small, full):
        short = (i == 0) | (i == end)
        pl.when(short)(small)
        pl.when(jnp.logical_not(short))(full)

    def row(i):
        return jnp.maximum(i * C - H, 0)

    def cols(k):
        return pl.ds(k * K, K)

    def load(src, dst, sem, i):
        at = pl.ds(pl.multiple_of(row(i), H), C)
        return pltpu.make_async_copy(src.at[at], dst.at[i], sem.at[i])

    def load_end(src, dst, sem, i):
        at = pl.ds(0 if i == 0 else (2 * end - 1) * H, H)
        return pltpu.make_async_copy(src.at[at], dst.at[i, top], sem.at[i])

    def landed(buf, sem, i, rows):
        part = buf.at[i, pl.ds(0, rows)]
        pltpu.make_async_copy(part, part, sem.at[i]).wait()

    part_of = F // SL

    def piece(n):
        at = n * part_of
        return pl.ds(at if isinstance(n, int) else pl.multiple_of(at, part_of), part_of)

    def get_w1(n):
        return pltpu.make_async_copy(w1h.at[0, :, piece(n)], w1.at[:, piece(n)], wsem.at[0, n])

    def get_w2(n):
        return pltpu.make_async_copy(w2h.at[0, piece(n)], w2.at[piece(n)], wsem.at[1, n])

    def have_weights():
        for n in range(SL):
            get_w1(n).wait()
        for n in range(SL):
            get_w2(n).wait()

    def load_all(src, dst, sem):
        load_end(src, dst, sem, end).start()

        def f(i, _):
            load(src, dst, sem, i).start()
            return 0
        lax.fori_loop(1, end, f, 0)

    @pl.when(s == 0)
    def _():
        load_end(x, hb, hsem, 0).start()

    for n in range(SL):
        get_w1(n).start()
    for n in range(SL):
        get_w2(n).start()

    @pl.when(s == 0)
    def _():
        load_all(x, hb, hsem)

    @pl.when(s == last)
    def _():
        load_end(g, gb, gsem, 0).start()
        load_all(g, gb, gsem)

    bar = pltpu.get_barrier_semaphore()
    near = (-2, -1, 1, 2)
    for off in near:
        @pl.when((s + off >= 0) & (s + off < n_st))
        def _(off=off):
            pl.semaphore_signal(bar, inc=1, device_id=peer(s + off), device_id_type=MESH)
    for k in range(3, n_st, 2):
        @pl.when(s == 0)
        def _(k=k):
            pl.semaphore_signal(bar, inc=1, device_id=peer(k), device_id_type=MESH)

        @pl.when(s == k)
        def _(k=k):
            pl.semaphore_signal(bar, inc=1, device_id=peer(0), device_id_type=MESH)
    far = jnp.where(s == 0, (n_st - 2) // 2, jnp.where((s % 2 == 1) & (s >= 3), 1, 0))
    peers = jnp.minimum(s, 2) + jnp.minimum(last - s, 2) + far

    def send(src, r, dst, i, ssem, to, dev, rows):
        part = pl.ds(0, rows)
        return pltpu.make_async_remote_copy(src_ref=src.at[r, part], dst_ref=dst.at[i, part], send_sem=ssem.at[r],
                                            recv_sem=to.at[i], device_id=peer(dev), device_id_type=MESH)

    def send_f(i, r, rows):
        return send(fo, r, hb, i, fsem, hsem, s + 1, rows)

    def send_b(i, r, rows):
        return send(bo, r, gb, i, bsem, gsem, s - 1, rows)

    def sent_f(i, r):
        sized(i, lambda: send_f(i, r, H).wait_send(), lambda: send_f(i, r, C).wait_send())

    def sent_b(i, r):
        sized(i, lambda: send_b(i, r, H).wait_send(), lambda: send_b(i, r, C).wait_send())

    def first_piece(i):
        return jnp.maximum(2 * i - 1, 0)

    def hand(src, r, k, p, ssem, dev):
        return pltpu.make_async_remote_copy(src_ref=src.at[r, pl.ds(k * H, H)], dst_ref=rb.at[p], send_sem=ssem.at[r],
                                            recv_sem=psem.at[p], device_id=peer(dev), device_id_type=MESH)

    def keep(src, r, k, p):
        return pltpu.make_async_copy(src.at[r, pl.ds(k * H, H)], lf.at[p], osem.at[r])

    def out_start(src, r, i, ssem, dev):
        p = first_piece(i)
        hand(src, r, 0, p, ssem, dev).start()
        keep(src, r, 0, p).start()

        def more():
            hand(src, r, 1, p + 1, ssem, dev).start()
            keep(src, r, 1, p + 1).start()
        sized(i, lambda: None, more)

    def out_wait(src, r, i, ssem):
        def both(rows):
            part = src.at[r, pl.ds(0, rows)]
            pltpu.make_async_copy(part, part, ssem.at[r]).wait()
            pltpu.make_async_copy(part, part, osem.at[r]).wait()
        sized(i, lambda: both(H), lambda: both(C))

    def direct(r, k):
        return pltpu.make_async_remote_copy(src_ref=bo.at[r, top], dst_ref=rb.at[pieces - 1], send_sem=esem.at[k // 2 - 1],
                                            recv_sem=psem.at[pieces - 1], device_id=peer(k), device_id_type=MESH)

    def onward(p, dev):
        return pltpu.make_async_remote_copy(src_ref=rb.at[p], dst_ref=rb.at[p], send_sem=rsem.at[0], recv_sem=psem.at[p],
                                            device_id=peer(dev), device_id_type=MESH)

    def across(p, dev):
        return pltpu.make_async_remote_copy(src_ref=rb.at[p], dst_ref=lf.at[p], send_sem=rsem.at[1], recv_sem=lsem,
                                            device_id=peer(dev), device_id_type=MESH)

    def write_z(i):
        q = lax.rem(i, 2)
        return pltpu.make_async_copy(zb.at[q], zh.at[i], zwsem.at[q])

    def read_z(i):
        q = lax.rem(i, 2)
        return pltpu.make_async_copy(zh.at[i], zb.at[2 + q], zrsem.at[q])

    def rows_of(i, rows):
        first = i == 0
        k = jnp.where(first, end // 2 - 1, lax.div(i - 1, 2))
        at = jnp.where(first, C + H, lax.rem(i - 1, 2) * C)
        return k, pl.ds(pl.multiple_of(at, H), rows)

    def write_ud(src, dst, sem, i, rows):
        k, at = rows_of(i, rows)
        q = lax.rem(i, 2)
        return pltpu.make_async_copy(src.at[q, pl.ds(0, rows)], dst.at[k, at], sem.at[q])

    def done_u(i):
        sized(i, lambda: write_ud(ub, uh, uwsem, i, H).wait(), lambda: write_ud(ub, uh, uwsem, i, C).wait())

    def done_d(i):
        sized(i, lambda: write_ud(db, dh, dwsem, i, H).wait(), lambda: write_ud(db, dh, dwsem, i, C).wait())

    def read_u(k):
        q = lax.rem(k, 2)
        return pltpu.make_async_copy(uh.at[k], uw.at[q], ursem.at[q])

    def read_d(k):
        q = lax.rem(k, 2)
        return pltpu.make_async_copy(dh.at[k], dw.at[q], drsem.at[q])

    def ensure(wait, done, want):
        for j in range(2):
            @pl.when(done + j < want)
            def _(j=j):
                wait(done + j)

    def f_slots(i):
        q = lax.rem(i, 2)
        return lax.rem(i, RING), jnp.where(spill, q, lax.rem(i, 4)), q

    def b_slots(i):
        q = lax.rem(i, 2)
        return lax.rem(i, RING), jnp.where(spill, 2 + q, lax.rem(i, 4)), q

    def f_ready(i, r, zw, uc):
        @pl.when(spill)
        def _():
            ensure(lambda j: write_z(j).wait(), zw, i - 1)

        ensure(done_u, uc, i - 1)

        @pl.when(i >= RING)
        def _():
            @pl.when(s < last)
            def _():
                sent_f(i - RING, r)

            @pl.when(s == last)
            def _():
                out_wait(fo, r, i - RING, fsem)

    def f_body(i, rows, slots):
        r, zs, q = slots
        part = pl.ds(0, rows)
        h = hb[i, part, :]
        tot = None
        for n in range(NS + LAG):
            if n < NS:
                z = _dot(h, w1[:, cols(n)])
            if n >= LAG:
                m = n - LAG
                y = _dot(ub[q, part, cols(m)], w2[cols(m), :])
                tot = y if m == 0 else tot + y
            if n < NS:
                u, gp = _gelu(z)
                zb[zs, part, cols(n)] = gp
                ub[q, part, cols(n)] = u
        fo[r, part, :] = (h.astype(f32) + tot).astype(bf16)

    def f_first(i, slots):
        r, zs, q = slots
        landed(hb, hsem, i, H)
        tot = pl.ds(0, D)

        def one(n, _):
            get_w1(n).wait()
            h = hb[i, top, :]
            for m in range(NS // SL):
                sl = pl.ds(pl.multiple_of(n * part_of + m * K, K), K)
                u, gp = _gelu(_dot(h, w1[:, sl]))
                zb[zs, top, sl] = gp
                ub[q, top, sl] = u
            return 0
        lax.fori_loop(0, SL, one, 0)
        zb[zs, low, tot] = hb[i, top, :].astype(f32)

        def two(n, _):
            get_w2(n).wait()
            zb[zs, low, tot] += _dot(ub[q, top, piece(n)], w2[piece(n), :])
            return 0
        lax.fori_loop(0, SL, two, 0)
        fo[r, top, :] = zb[zs, low, tot].astype(bf16)

    def f_send(i, rows, r):
        @pl.when(s < last)
        def _():
            send_f(i, r, rows).start()

        @pl.when(s == last)
        def _():
            out_start(fo, r, i, fsem, s - 1)

        write_ud(ub, uh, uwsem, i, rows).start()

        @pl.when(spill)
        def _():
            write_z(i).start()

    def forward(i, zw, uc, fresh):
        slots = f_slots(i)
        r = slots[0]
        f_ready(i, r, zw, uc)

        def small():
            @pl.when(fresh)
            def _():
                f_first(i, slots)

            @pl.when(jnp.logical_not(fresh))
            def _():
                landed(hb, hsem, i, H)
                f_body(i, H, slots)

            @pl.when(i == 0)
            def _():
                pl.semaphore_wait(bar, peers)
                hb[end, low, :] = hb[0, top, :]
            f_send(i, H, r)

        def full():
            landed(hb, hsem, i, C)
            f_body(i, C, slots)
            f_send(i, C, r)

            @pl.when(spill & (i == 4))
            def _():
                read_z(0).start()
        sized(i, small, full)

    def b_ready(i, r, zw, dc):
        @pl.when(spill)
        def _():
            read_z(i).wait()
            ensure(lambda j: write_z(j).wait(), zw, jnp.minimum(i + 2, n_ch))

            @pl.when(i + 1 < n_ch)
            def _():
                read_z(i + 1).start()

        ensure(done_d, dc, i - 1)

        @pl.when(i >= RING)
        def _():
            @pl.when(s > 0)
            def _():
                sent_b(i - RING, r)

            @pl.when(s == 0)
            def _():
                out_wait(bo, r, i - RING, bsem)

    def b_body(i, slots):
        r, zs, q = slots
        gg = gb[i]
        tot = None
        for n in range(NS + LAG):
            if n < NS:
                du = _dot(gg, w2t[:, cols(n)])
            if n >= LAG:
                m = n - LAG
                y = _dot(db[q, :, cols(m)], w1t[cols(m), :])
                tot = y if m == 0 else tot + y
            if n < NS:
                db[q, :, cols(n)] = (zb[zs, :, cols(n)] * du).astype(bf16)
        bo[r] = (gg.astype(f32) + tot).astype(bf16)

    def b_send(i, rows, r):
        @pl.when(s > 0)
        def _():
            send_b(i, r, rows).start()

        @pl.when(s == 0)
        def _():
            if rows == H:
                @pl.when(i == end)
                def _():
                    for k in range(last, 2, -2):
                        direct(r, k).start()
            out_start(bo, r, i, bsem, s + 1)

        write_ud(db, dh, dwsem, i, rows).start()

    def backward(i, zw, dc):
        slots = b_slots(i)
        r = slots[0]
        b_ready(i, r, zw, dc)

        def small():
            landed(gb, gsem, i, H)
            b_body(i, slots)

            @pl.when(i == 0)
            def _():
                gb[end, low, :] = gb[0, top, :]
            b_send(i, H, r)

        def full():
            landed(gb, gsem, i, C)
            b_body(i, slots)
            b_send(i, C, r)
        sized(i, small, full)

    def prefetch(k, uc, dc):
        ensure(done_u, uc, 2 * k + 3)
        ensure(done_d, dc, 2 * k + 3)
        read_d(k).start()
        read_u(k).start()

    def grad1(k):
        q = lax.rem(k, 2)
        h = hb[pl.ds(2 * k + 1, 2)].reshape(2 * C, D)
        for n in range(F // TW):
            sl = pl.ds(n * TW, TW)
            a1[:, sl] += _dot_t(h, dw[q, :, sl])

    def grad2(k):
        q = lax.rem(k, 2)
        gg = gb[pl.ds(2 * k + 1, 2)].reshape(2 * C, D)
        for n in range(F // TW):
            sl = pl.ds(n * TW, TW)
            a2[sl, :] += _dot_t(uw[q, :, sl], gg)

    def weights(w):
        k = lax.div(w, 2)
        odd = lax.rem(w, 2)

        @pl.when(odd == 0)
        def _():
            read_d(k).wait()
            grad1(k)

        @pl.when(odd == 1)
        def _():
            read_u(k).wait()
            grad2(k)

    def weights_both(w):
        k = lax.div(w, 2)
        read_d(k).wait()
        read_u(k).wait()
        grad1(k)
        grad2(k)

    def relay_step(p):
        piece = rb.at[p]
        pltpu.make_async_copy(piece, piece, psem.at[p]).wait()

        @pl.when(even)
        def _():
            @pl.when(s >= 2)
            def _():
                onward(p, s - 2).start()

            @pl.when(s < n_st - 2)
            def _():
                across(p, s + 1).start()

        @pl.when(jnp.logical_not(even))
        def _():
            @pl.when((s < last) & (p < pieces - 1))
            def _():
                onward(p, s + 2).start()

            @pl.when(s > 1)
            def _():
                across(p, s - 1).start()

    def transposes(fresh):
        pl.when(fresh)(have_weights)

        def f(n, _):
            sl = pl.ds(pl.multiple_of(n * 256, 256), 256)
            w1t[sl, :] = w1[:, sl].T
            w2t[:, sl] = w2[sl, :].T
            a1[:, sl] = jnp.zeros((D, 256), f32)
            a2[sl, :] = jnp.zeros((256, D), f32)
            return 0
        lax.fori_loop(0, F // 256, f, 0)

    def step(j, carry):
        word, nf, nb, nw, npf, nr, nt, zw, uc, dc = carry
        op = lax.rem(word, 16)
        is_f, is_b, is_p = op == 0, op == 1, op == 3

        @pl.when(op < 2)
        def _():
            @pl.when(is_f)
            def _():
                forward(nf, zw, uc, (nf == 0) & (nt == 0))

            @pl.when(is_b)
            def _():
                backward(nb, zw, dc)

        @pl.when((op >= 2) & (op < 6))
        def _():
            @pl.when(op == 2)
            def _():
                weights(nw)

            @pl.when(op == 4)
            def _():
                relay_step(nr)

            @pl.when(is_p)
            def _():
                prefetch(npf, uc, dc)

            @pl.when(op == 5)
            def _():
                transposes(nf == 0)

        @pl.when(op >= 6)
        def _():
            @pl.when(op == 8)
            def _():
                weights_both(nw)

            @pl.when(op == 9)
            def _():
                relay_step(nr)
                relay_step(nr + 1)

        zw = jnp.where(is_f, jnp.maximum(zw, nf - 1), zw)
        zw = jnp.where(is_b, jnp.maximum(zw, jnp.minimum(nb + 2, n_ch)), zw)
        uc = jnp.where(is_f, jnp.maximum(uc, nf - 1), uc)
        uc = jnp.where(is_p, jnp.maximum(uc, 2 * npf + 3), uc)
        dc = jnp.where(is_b, jnp.maximum(dc, nb - 1), dc)
        dc = jnp.where(is_p, jnp.maximum(dc, 2 * npf + 3), dc)
        one = lambda k: jnp.where(k, 1, 0)
        two = lambda k, m: jnp.where(op == k, 1, jnp.where(op == m, 2, 0))
        return (lax.div(word, 16), nf + one(is_f), nb + one(is_b), nw + two(2, 8), npf + one(is_p), nr + two(4, 9), nt + one(op == 5),
                zw, uc, dc)

    zero = s * 0
    words = []
    for k in range(len(WORDS[0])):
        word = zero
        for q in range(n_st):
            word = jnp.where(s == q, WORDS[q][k], word)
        words.append(word)

    def work(k, carry):
        word = words[0]
        for q in range(1, len(words)):
            word = jnp.where(k == q, words[q], word)
        out = lax.fori_loop(0, STEPS, step, (word, *carry))
        return out[1:]

    lax.fori_loop(0, len(words), work, (zero,) * 9)

    for j in range(RING):
        i = zero + (n_ch - RING + j)
        r = (n_ch - RING + j) % RING

        @pl.when(s < last)
        def _(i=i, r=r):
            sent_f(i, r)

        @pl.when(s == last)
        def _(i=i, r=r):
            out_wait(fo, r, i, fsem)

        @pl.when(s > 0)
        def _(i=i, r=r):
            sent_b(i, r)

        @pl.when(s == 0)
        def _(i=i, r=r):
            out_wait(bo, r, i, bsem)

    @pl.when(s == 0)
    def _():
        for k in range(last, 2, -2):
            direct(end % RING, k).wait_send()

    def all_of(ref, sem, count):
        part = ref.at[pl.ds(0, count)]
        pltpu.make_async_copy(part, part, sem).wait()

    @pl.when(even)
    def _():
        @pl.when(s >= 2)
        def _():
            all_of(rb, rsem.at[0], pieces)

        @pl.when(s < n_st - 2)
        def _():
            all_of(rb, rsem.at[1], pieces)

        @pl.when(s > 0)
        def _():
            all_of(lf, lsem, pieces)

    @pl.when(jnp.logical_not(even))
    def _():
        @pl.when(s < last)
        def _():
            all_of(rb, rsem.at[0], pieces - 1)
            all_of(lf, lsem, pieces)

        @pl.when(s > 1)
        def _():
            all_of(rb, rsem.at[1], pieces)


def _write_out(lf, rb, a1, a2, y, dx, d1, d2, lb, sem_w, sem_r, sem_o):
    s = lax.axis_index("stage")
    parts = 4
    big = []
    for p in range(parts):
        r1 = pl.ds(p * (D // parts), D // parts)
        r2 = pl.ds(p * (F // parts), F // parts)
        big.append(pltpu.make_async_copy(a1.at[r1], d1.at[0, r1], sem_w.at[0, p]))
        big.append(pltpu.make_async_copy(a2.at[r2], d2.at[0, r2], sem_w.at[1, p]))
    back = pltpu.make_async_copy(lf, lb, sem_r)
    back.start()
    for c in big:
        c.start()

    def rest(mine, other):
        near = pltpu.make_async_copy(rb, mine, sem_o.at[0])
        near.start()
        back.wait()
        far = pltpu.make_async_copy(lb, other, sem_o.at[1])
        far.start()
        near.wait()
        far.wait()

    @pl.when(s % 2 == 0)
    def _():
        rest(y, dx)

    @pl.when(s % 2 == 1)
    def _():
        rest(dx, y)

    for c in big:
        c.wait()


def solution(mesh):
    n_st = mesh.shape["stage"]

    def body(x, g, w1, w2):
        tokens = x.shape[0] * x.shape[1]
        n_ch = tokens // C + 1
        hbm = pl.BlockSpec(memory_space=pltpu.HBM)
        vmem = pl.BlockSpec(memory_space=pltpu.VMEM)
        dma = pltpu.SemaphoreType.DMA
        pieces = (tokens // H, H, D)
        groups = (tokens // (2 * C), 2 * C, F)
        params = dict(has_side_effects=True)
        rows = (n_ch, C, D)
        slabs = (2, 2 * C, F)
        lf, rb, a1, a2, _, _, _ = pl.pallas_call(
            functools.partial(_pipeline, n_st, n_ch),
            out_shape=[pltpu.HBM(pieces, bf16), pltpu.VMEM(pieces, bf16), pltpu.VMEM((D, F), f32), pltpu.VMEM((F, D), f32),
                       pltpu.HBM((n_ch, C, F), f32), pltpu.HBM(groups, bf16), pltpu.HBM(groups, bf16)],
            in_specs=[hbm] * 4,
            out_specs=[hbm] + [vmem] * 3 + [hbm] * 3,
            scratch_shapes=[
                pltpu.VMEM((D, F), bf16), pltpu.VMEM((F, D), bf16), pltpu.VMEM((F, D), bf16), pltpu.VMEM((D, F), bf16),
                pltpu.VMEM(rows, bf16), pltpu.VMEM(rows, bf16), pltpu.VMEM(slabs, bf16), pltpu.VMEM(slabs, bf16),
                pltpu.VMEM((4, C, F), f32), pltpu.VMEM((2, C, F), bf16), pltpu.VMEM((2, C, F), bf16),
                pltpu.VMEM((RING, C, D), bf16), pltpu.VMEM((RING, C, D), bf16),
                dma((n_ch,)), dma((n_ch,)), dma((pieces[0],)), dma,
            ],
            compiler_params=pltpu.CompilerParams(collective_id=0, vmem_limit_bytes=45_000_000, **params),
            name="pipeline",
        )(x.reshape(tokens, D), g.reshape(tokens, D), w1, w2)
        y, dx, d1, d2 = pl.pallas_call(
            _write_out,
            out_shape=[pltpu.HBM(pieces, bf16), pltpu.HBM(pieces, bf16), pltpu.HBM((1, D, F), f32), pltpu.HBM((1, F, D), f32)],
            in_specs=[hbm, vmem, vmem, vmem],
            out_specs=[hbm] * 4,
            scratch_shapes=[pltpu.VMEM(pieces, bf16), dma((2, 4)), dma, dma((2,))],
            compiler_params=pltpu.CompilerParams(vmem_limit_bytes=4_000_000, **params),
            name="write_out",
        )(pltpu.with_memory_space_constraint(lf, pltpu.HBM), rb, a1, a2)
        return y.reshape(x.shape), dx.reshape(x.shape), d1, d2

    return jax.shard_map(body, mesh=mesh,
                         in_specs=(P("data"), P("data"), P("stage"), P("stage")),
                         out_specs=(P("data"), P("data"), P(("data", "stage")), P(("data", "stage"))),
                         check_vma=False)
```

```python
import functools

import jax
import jax.numpy as jnp
from jax import lax
from jax.experimental import pallas as pl
from jax.experimental.pallas import tpu as pltpu
from jax.sharding import PartitionSpec as P

MESH = pl.DeviceIdType.MESH
f32 = jnp.float32
bf16 = jnp.bfloat16
D = 768
F = 3072
C = 128
H = 64
RING = 3
K = 256
LAG = 6
TW = 512
SL = 3
NS = F // K
C0 = 0.7978845608028654
C1 = 0.044715

WORDS = (
    (0, 0, 26280016, 69280532, 69288721, 153174850, 18105121, 71406360, 17994514, 76780098, 143800609, 268432532, 268435455),
    (0, 83886080, 21037056, 43066177, 21173313, 71578148, 69473313, 20190353, 21119379, 71386148, 69485075, 35881748, 268435272),
    (5, 4194304, 67387392, 71385108, 35734337, 154353937, 17962002, 68294947, 19997714, 54674577, 37979186, 38020249, 268435442),
    (5, 0, 51384321, 34685185, 18952771, 26493970, 54673700, 19153939, 21250345, 37898545, 37962788, 54805540, 268432514),
    (5, 71303172, 67191809, 9520129, 9703696, 17892401, 20193602, 18039076, 43272513, 153232436, 36848275, 36839986, 268435442),
    (5, 16842768, 18022416, 16843009, 20058132, 26362898, 36802884, 138691396, 38024228, 69419588, 69420068, 76690498, 268435272),
    (66565, 1638724, 26251284, 68194561, 16859152, 1311040, 18088724, 154420244, 35857044, 76059700, 58925619, 268431912, 268435455),
    (16843013, 1052688, 16843009, 1052688, 16843009, 54675747, 71902024, 71533108, 71447620, 53027890, 38019657, 71582786, 268435444),
)
STEPS = 7


def _dot(a, b):
    return jnp.dot(a, b, preferred_element_type=f32)


def _dot_t(a, b):
    return lax.dot_general(a, b, (((0,), (0,)), ((), ())), preferred_element_type=f32)


def _gelu(z):
    q = (C0 * C1) * (z * z)
    p = 0.5 * jnp.tanh(z * (C0 + q)) + 0.5
    u = z * p
    return u.astype(bf16), p + (u * (1.0 - p)) * (2.0 * C0 + 6.0 * q)


def _pipeline(n_st, n_ch, *refs):
    dma = pltpu.SemaphoreType.DMA
    pl.run_scoped(functools.partial(_work, n_st, n_ch, *refs), dma((2, SL)), dma((n_st // 2 - 1,)), dma((RING,)), dma((RING,)), dma((RING,)),
                  dma((2,)), dma((2,)), dma((2,)), dma((2,)), dma((2,)), dma((2,)), dma((2,)))


def _work(n_st, n_ch, x, g, w1h, w2h, lf, rb, a1, a2, zh, uh, dh,
          w1, w2, w1t, w2t, hb, gb, uw, dw, zb, ub, db, fo, bo,
          hsem, gsem, psem, lsem, wsem, esem, fsem, bsem, osem, rsem, zwsem, zrsem, uwsem, dwsem, ursem, drsem):
    d = lax.axis_index("data")
    s = lax.axis_index("stage")
    last = n_st - 1
    end = n_ch - 1
    pieces = 2 * end
    spill = s < n_st - 2
    even = s % 2 == 0
    top, low = pl.ds(0, H), pl.ds(H, H)

    def peer(k):
        return (d, k)

    def sized(i, small, full):
        short = (i == 0) | (i == end)
        pl.when(short)(small)
        pl.when(jnp.logical_not(short))(full)

    def row(i):
        return jnp.maximum(i * C - H, 0)

    def cols(k):
        return pl.ds(k * K, K)

    def load(src, dst, sem, i):
        at = pl.ds(pl.multiple_of(row(i), H), C)
        return pltpu.make_async_copy(src.at[at], dst.at[i], sem.at[i])

    def load_end(src, dst, sem, i):
        at = pl.ds(0 if i == 0 else (2 * end - 1) * H, H)
        return pltpu.make_async_copy(src.at[at], dst.at[i, top], sem.at[i])

    def landed(buf, sem, i, rows):
        part = buf.at[i, pl.ds(0, rows)]
        pltpu.make_async_copy(part, part, sem.at[i]).wait()

    part_of = F // SL

    def piece(n):
        at = n * part_of
        return pl.ds(at if isinstance(n, int) else pl.multiple_of(at, part_of), part_of)

    def get_w1(n):
        return pltpu.make_async_copy(w1h.at[0, :, piece(n)], w1.at[:, piece(n)], wsem.at[0, n])

    def get_w2(n):
        return pltpu.make_async_copy(w2h.at[0, piece(n)], w2.at[piece(n)], wsem.at[1, n])

    def have_weights():
        for n in range(SL):
            get_w1(n).wait()
        for n in range(SL):
            get_w2(n).wait()

    def load_all(src, dst, sem):
        load_end(src, dst, sem, end).start()

        def f(i, _):
            load(src, dst, sem, i).start()
            return 0
        lax.fori_loop(1, end, f, 0)

    @pl.when(s == 0)
    def _():
        load_end(x, hb, hsem, 0).start()

    for n in range(SL):
        get_w1(n).start()
    for n in range(SL):
        get_w2(n).start()

    @pl.when(s == 0)
    def _():
        load_all(x, hb, hsem)

    @pl.when(s == last)
    def _():
        load_end(g, gb, gsem, 0).start()
        load_all(g, gb, gsem)

    bar = pltpu.get_barrier_semaphore()
    near = (-2, -1, 1, 2)
    for off in near:
        @pl.when((s + off >= 0) & (s + off < n_st))
        def _(off=off):
            pl.semaphore_signal(bar, inc=1, device_id=peer(s + off), device_id_type=MESH)
    peers = jnp.minimum(s, 2) + jnp.minimum(last - s, 2)

    def send(src, r, dst, i, ssem, to, dev, rows):
        part = pl.ds(0, rows)
        return pltpu.make_async_remote_copy(src_ref=src.at[r, part], dst_ref=dst.at[i, part], send_sem=ssem.at[r],
                                            recv_sem=to.at[i], device_id=peer(dev), device_id_type=MESH)

    def send_f(i, r, rows):
        return send(fo, r, hb, i, fsem, hsem, s + 1, rows)

    def send_b(i, r, rows):
        return send(bo, r, gb, i, bsem, gsem, s - 1, rows)

    def sent_f(i, r):
        sized(i, lambda: send_f(i, r, H).wait_send(), lambda: send_f(i, r, C).wait_send())

    def sent_b(i, r):
        sized(i, lambda: send_b(i, r, H).wait_send(), lambda: send_b(i, r, C).wait_send())

    def first_piece(i):
        return jnp.maximum(2 * i - 1, 0)

    def hand(src, r, k, p, ssem, dev):
        return pltpu.make_async_remote_copy(src_ref=src.at[r, pl.ds(k * H, H)], dst_ref=rb.at[p], send_sem=ssem.at[r],
                                            recv_sem=psem.at[p], device_id=peer(dev), device_id_type=MESH)

    def keep(src, r, k, p):
        return pltpu.make_async_copy(src.at[r, pl.ds(k * H, H)], lf.at[p], osem.at[r])

    def out_start(src, r, i, ssem, dev):
        p = first_piece(i)
        hand(src, r, 0, p, ssem, dev).start()
        keep(src, r, 0, p).start()

        def more():
            hand(src, r, 1, p + 1, ssem, dev).start()
            keep(src, r, 1, p + 1).start()
        sized(i, lambda: None, more)

    def out_wait(src, r, i, ssem):
        def both(rows):
            part = src.at[r, pl.ds(0, rows)]
            pltpu.make_async_copy(part, part, ssem.at[r]).wait()
            pltpu.make_async_copy(part, part, osem.at[r]).wait()
        sized(i, lambda: both(H), lambda: both(C))

    def direct(r, k):
        return pltpu.make_async_remote_copy(src_ref=bo.at[r, top], dst_ref=rb.at[pieces - 1], send_sem=esem.at[k // 2 - 1],
                                            recv_sem=psem.at[pieces - 1], device_id=peer(k), device_id_type=MESH)

    def onward(p, dev):
        return pltpu.make_async_remote_copy(src_ref=rb.at[p], dst_ref=rb.at[p], send_sem=rsem.at[0], recv_sem=psem.at[p],
                                            device_id=peer(dev), device_id_type=MESH)

    def across(p, dev):
        return pltpu.make_async_remote_copy(src_ref=rb.at[p], dst_ref=lf.at[p], send_sem=rsem.at[1], recv_sem=lsem,
                                            device_id=peer(dev), device_id_type=MESH)

    def write_z(i):
        q = lax.rem(i, 2)
        return pltpu.make_async_copy(zb.at[q], zh.at[i], zwsem.at[q])

    def read_z(i):
        q = lax.rem(i, 2)
        return pltpu.make_async_copy(zh.at[i], zb.at[2 + q], zrsem.at[q])

    def rows_of(i, rows):
        first = i == 0
        k = jnp.where(first, end // 2 - 1, lax.div(i - 1, 2))
        at = jnp.where(first, C + H, lax.rem(i - 1, 2) * C)
        return k, pl.ds(pl.multiple_of(at, H), rows)

    def write_ud(src, dst, sem, i, rows):
        k, at = rows_of(i, rows)
        q = lax.rem(i, 2)
        return pltpu.make_async_copy(src.at[q, pl.ds(0, rows)], dst.at[k, at], sem.at[q])

    def done_u(i):
        sized(i, lambda: write_ud(ub, uh, uwsem, i, H).wait(), lambda: write_ud(ub, uh, uwsem, i, C).wait())

    def done_d(i):
        sized(i, lambda: write_ud(db, dh, dwsem, i, H).wait(), lambda: write_ud(db, dh, dwsem, i, C).wait())

    def read_u(k):
        q = lax.rem(k, 2)
        return pltpu.make_async_copy(uh.at[k], uw.at[q], ursem.at[q])

    def read_d(k):
        q = lax.rem(k, 2)
        return pltpu.make_async_copy(dh.at[k], dw.at[q], drsem.at[q])

    def ensure(wait, done, want):
        for j in range(2):
            @pl.when(done + j < want)
            def _(j=j):
                wait(done + j)

    def f_slots(i):
        q = lax.rem(i, 2)
        return lax.rem(i, RING), jnp.where(spill, q, lax.rem(i, 4)), q

    def b_slots(i):
        q = lax.rem(i, 2)
        return lax.rem(i, RING), jnp.where(spill, 2 + q, lax.rem(i, 4)), q

    def f_ready(i, r, zw, uc):
        @pl.when(spill)
        def _():
            ensure(lambda j: write_z(j).wait(), zw, i - 1)

        ensure(done_u, uc, i - 1)

        @pl.when(i >= RING)
        def _():
            @pl.when(s < last)
            def _():
                sent_f(i - RING, r)

            @pl.when(s == last)
            def _():
                out_wait(fo, r, i - RING, fsem)

    def f_body(i, rows, slots):
        r, zs, q = slots
        part = pl.ds(0, rows)
        h = hb[i, part, :]
        tot = None
        for n in range(NS + LAG):
            if n < NS:
                z = _dot(h, w1[:, cols(n)])
            if n >= LAG:
                m = n - LAG
                y = _dot(ub[q, part, cols(m)], w2[cols(m), :])
                tot = y if m == 0 else tot + y
            if n < NS:
                u, gp = _gelu(z)
                zb[zs, part, cols(n)] = gp
                ub[q, part, cols(n)] = u
        fo[r, part, :] = (h.astype(f32) + tot).astype(bf16)

    def f_first(i, slots):
        r, zs, q = slots
        landed(hb, hsem, i, H)
        tot = pl.ds(0, D)

        def one(n, _):
            get_w1(n).wait()
            h = hb[i, top, :]
            for m in range(NS // SL):
                sl = pl.ds(pl.multiple_of(n * part_of + m * K, K), K)
                u, gp = _gelu(_dot(h, w1[:, sl]))
                zb[zs, top, sl] = gp
                ub[q, top, sl] = u
            return 0
        lax.fori_loop(0, SL, one, 0)
        zb[zs, low, tot] = hb[i, top, :].astype(f32)

        def two(n, _):
            get_w2(n).wait()
            zb[zs, low, tot] += _dot(ub[q, top, piece(n)], w2[piece(n), :])
            return 0
        lax.fori_loop(0, SL, two, 0)
        fo[r, top, :] = zb[zs, low, tot].astype(bf16)

    def f_send(i, rows, r):
        @pl.when(s < last)
        def _():
            send_f(i, r, rows).start()

        @pl.when(s == last)
        def _():
            out_start(fo, r, i, fsem, s - 1)

        write_ud(ub, uh, uwsem, i, rows).start()

        @pl.when(spill)
        def _():
            write_z(i).start()

    def forward(i, zw, uc, fresh):
        slots = f_slots(i)
        r = slots[0]
        f_ready(i, r, zw, uc)

        def small():
            @pl.when(fresh)
            def _():
                f_first(i, slots)

            @pl.when(jnp.logical_not(fresh))
            def _():
                landed(hb, hsem, i, H)
                f_body(i, H, slots)

            @pl.when(i == 0)
            def _():
                pl.semaphore_wait(bar, peers)
                hb[end, low, :] = hb[0, top, :]
            f_send(i, H, r)

        def full():
            landed(hb, hsem, i, C)
            f_body(i, C, slots)
            f_send(i, C, r)

            @pl.when(spill & (i == 4))
            def _():
                read_z(0).start()
        sized(i, small, full)

    def b_ready(i, r, zw, dc):
        @pl.when(spill)
        def _():
            read_z(i).wait()
            ensure(lambda j: write_z(j).wait(), zw, jnp.minimum(i + 2, n_ch))

            @pl.when(i + 1 < n_ch)
            def _():
                read_z(i + 1).start()

        ensure(done_d, dc, i - 1)

        @pl.when(i >= RING)
        def _():
            @pl.when(s > 0)
            def _():
                sent_b(i - RING, r)

            @pl.when(s == 0)
            def _():
                out_wait(bo, r, i - RING, bsem)

    def b_body(i, slots):
        r, zs, q = slots
        gg = gb[i]
        tot = None
        for n in range(NS + LAG):
            if n < NS:
                du = _dot(gg, w2t[:, cols(n)])
            if n >= LAG:
                m = n - LAG
                y = _dot(db[q, :, cols(m)], w1t[cols(m), :])
                tot = y if m == 0 else tot + y
            if n < NS:
                db[q, :, cols(n)] = (zb[zs, :, cols(n)] * du).astype(bf16)
        bo[r] = (gg.astype(f32) + tot).astype(bf16)

    def b_send(i, rows, r):
        @pl.when(s > 0)
        def _():
            send_b(i, r, rows).start()

        @pl.when(s == 0)
        def _():
            if rows == H:
                @pl.when(i == end)
                def _():
                    for k in range(last, 2, -2):
                        direct(r, k).start()
            out_start(bo, r, i, bsem, s + 1)

        write_ud(db, dh, dwsem, i, rows).start()

    def backward(i, zw, dc):
        slots = b_slots(i)
        r = slots[0]
        b_ready(i, r, zw, dc)

        def small():
            landed(gb, gsem, i, H)
            b_body(i, slots)

            @pl.when(i == 0)
            def _():
                gb[end, low, :] = gb[0, top, :]
            b_send(i, H, r)

        def full():
            landed(gb, gsem, i, C)
            b_body(i, slots)
            b_send(i, C, r)
        sized(i, small, full)

    def prefetch(k, uc, dc):
        ensure(done_u, uc, 2 * k + 3)
        ensure(done_d, dc, 2 * k + 3)
        read_d(k).start()
        read_u(k).start()

    def grad1(k):
        q = lax.rem(k, 2)
        h = hb[pl.ds(2 * k + 1, 2)].reshape(2 * C, D)
        for n in range(F // TW):
            sl = pl.ds(n * TW, TW)
            a1[:, sl] += _dot_t(h, dw[q, :, sl])

    def grad2(k):
        q = lax.rem(k, 2)
        gg = gb[pl.ds(2 * k + 1, 2)].reshape(2 * C, D)
        for n in range(F // TW):
            sl = pl.ds(n * TW, TW)
            a2[sl, :] += _dot_t(uw[q, :, sl], gg)

    def weights(w):
        k = lax.div(w, 2)
        odd = lax.rem(w, 2)

        @pl.when(odd == 0)
        def _():
            read_d(k).wait()
            grad1(k)

        @pl.when(odd == 1)
        def _():
            read_u(k).wait()
            grad2(k)

    def weights_both(w):
        k = lax.div(w, 2)
        read_d(k).wait()
        read_u(k).wait()
        grad1(k)
        grad2(k)

    def relay_step(p):
        piece = rb.at[p]
        pltpu.make_async_copy(piece, piece, psem.at[p]).wait()

        @pl.when(even)
        def _():
            @pl.when(s >= 2)
            def _():
                onward(p, s - 2).start()

            @pl.when(s < n_st - 2)
            def _():
                across(p, s + 1).start()

        @pl.when(jnp.logical_not(even))
        def _():
            @pl.when((s < last) & (p < pieces - 1))
            def _():
                onward(p, s + 2).start()

            @pl.when(s > 1)
            def _():
                across(p, s - 1).start()

    def transposes(fresh):
        pl.when(fresh)(have_weights)

        def f(n, _):
            sl = pl.ds(pl.multiple_of(n * 256, 256), 256)
            w1t[sl, :] = w1[:, sl].T
            w2t[:, sl] = w2[sl, :].T
            a1[:, sl] = jnp.zeros((D, 256), f32)
            a2[sl, :] = jnp.zeros((256, D), f32)
            return 0
        lax.fori_loop(0, F // 256, f, 0)

    def step(j, carry):
        word, nf, nb, nw, npf, nr, nt, zw, uc, dc = carry
        op = lax.rem(word, 16)
        is_f, is_b, is_p = op == 0, op == 1, op == 3

        @pl.when(op < 2)
        def _():
            @pl.when(is_f)
            def _():
                forward(nf, zw, uc, (nf == 0) & (nt == 0))

            @pl.when(is_b)
            def _():
                backward(nb, zw, dc)

        @pl.when((op >= 2) & (op < 6))
        def _():
            @pl.when(op == 2)
            def _():
                weights(nw)

            @pl.when(op == 4)
            def _():
                relay_step(nr)

            @pl.when(is_p)
            def _():
                prefetch(npf, uc, dc)

            @pl.when(op == 5)
            def _():
                transposes(nf == 0)

        @pl.when(op >= 6)
        def _():
            @pl.when(op == 8)
            def _():
                weights_both(nw)

            @pl.when(op == 9)
            def _():
                relay_step(nr)
                relay_step(nr + 1)

        zw = jnp.where(is_f, jnp.maximum(zw, nf - 1), zw)
        zw = jnp.where(is_b, jnp.maximum(zw, jnp.minimum(nb + 2, n_ch)), zw)
        uc = jnp.where(is_f, jnp.maximum(uc, nf - 1), uc)
        uc = jnp.where(is_p, jnp.maximum(uc, 2 * npf + 3), uc)
        dc = jnp.where(is_b, jnp.maximum(dc, nb - 1), dc)
        dc = jnp.where(is_p, jnp.maximum(dc, 2 * npf + 3), dc)
        one = lambda k: jnp.where(k, 1, 0)
        two = lambda k, m: jnp.where(op == k, 1, jnp.where(op == m, 2, 0))
        return (lax.div(word, 16), nf + one(is_f), nb + one(is_b), nw + two(2, 8), npf + one(is_p), nr + two(4, 9), nt + one(op == 5),
                zw, uc, dc)

    zero = s * 0
    words = []
    for k in range(len(WORDS[0])):
        word = zero
        for q in range(n_st):
            word = jnp.where(s == q, WORDS[q][k], word)
        words.append(word)

    def work(k, carry):
        word = words[0]
        for q in range(1, len(words)):
            word = jnp.where(k == q, words[q], word)
        out = lax.fori_loop(0, STEPS, step, (word, *carry))
        return out[1:]

    lax.fori_loop(0, len(words), work, (zero,) * 9)

    for j in range(RING):
        i = zero + (n_ch - RING + j)
        r = (n_ch - RING + j) % RING

        @pl.when(s < last)
        def _(i=i, r=r):
            sent_f(i, r)

        @pl.when(s == last)
        def _(i=i, r=r):
            out_wait(fo, r, i, fsem)

        @pl.when(s > 0)
        def _(i=i, r=r):
            sent_b(i, r)

        @pl.when(s == 0)
        def _(i=i, r=r):
            out_wait(bo, r, i, bsem)

    @pl.when(s == 0)
    def _():
        for k in range(last, 2, -2):
            direct(end % RING, k).wait_send()

    def all_of(ref, sem, count):
        part = ref.at[pl.ds(0, count)]
        pltpu.make_async_copy(part, part, sem).wait()

    @pl.when(even)
    def _():
        @pl.when(s >= 2)
        def _():
            all_of(rb, rsem.at[0], pieces)

        @pl.when(s < n_st - 2)
        def _():
            all_of(rb, rsem.at[1], pieces)

        @pl.when(s > 0)
        def _():
            all_of(lf, lsem, pieces)

    @pl.when(jnp.logical_not(even))
    def _():
        @pl.when(s < last)
        def _():
            all_of(rb, rsem.at[0], pieces - 1)
            all_of(lf, lsem, pieces)

        @pl.when(s > 1)
        def _():
            all_of(rb, rsem.at[1], pieces)


def _write_out(lf, rb, a1, a2, y, dx, d1, d2, lb, sem_w, sem_r, sem_o):
    s = lax.axis_index("stage")
    parts = 4
    big = []
    for p in range(parts):
        r1 = pl.ds(p * (D // parts), D // parts)
        r2 = pl.ds(p * (F // parts), F // parts)
        big.append(pltpu.make_async_copy(a1.at[r1], d1.at[0, r1], sem_w.at[0, p]))
        big.append(pltpu.make_async_copy(a2.at[r2], d2.at[0, r2], sem_w.at[1, p]))
    back = pltpu.make_async_copy(lf, lb, sem_r)
    back.start()
    for c in big:
        c.start()

    def rest(mine, other):
        near = pltpu.make_async_copy(rb, mine, sem_o.at[0])
        near.start()
        back.wait()
        far = pltpu.make_async_copy(lb, other, sem_o.at[1])
        far.start()
        near.wait()
        far.wait()

    @pl.when(s % 2 == 0)
    def _():
        rest(y, dx)

    @pl.when(s % 2 == 1)
    def _():
        rest(dx, y)

    for c in big:
        c.wait()


def solution(mesh):
    n_st = mesh.shape["stage"]

    def body(x, g, w1, w2):
        tokens = x.shape[0] * x.shape[1]
        n_ch = tokens // C + 1
        hbm = pl.BlockSpec(memory_space=pltpu.HBM)
        vmem = pl.BlockSpec(memory_space=pltpu.VMEM)
        dma = pltpu.SemaphoreType.DMA
        pieces = (tokens // H, H, D)
        groups = (tokens // (2 * C), 2 * C, F)
        params = dict(has_side_effects=True)
        rows = (n_ch, C, D)
        slabs = (2, 2 * C, F)
        lf, rb, a1, a2, _, _, _ = pl.pallas_call(
            functools.partial(_pipeline, n_st, n_ch),
            out_shape=[pltpu.HBM(pieces, bf16), pltpu.VMEM(pieces, bf16), pltpu.VMEM((D, F), f32), pltpu.VMEM((F, D), f32),
                       pltpu.HBM((n_ch, C, F), f32), pltpu.HBM(groups, bf16), pltpu.HBM(groups, bf16)],
            in_specs=[hbm] * 4,
            out_specs=[hbm] + [vmem] * 3 + [hbm] * 3,
            scratch_shapes=[
                pltpu.VMEM((D, F), bf16), pltpu.VMEM((F, D), bf16), pltpu.VMEM((F, D), bf16), pltpu.VMEM((D, F), bf16),
                pltpu.VMEM(rows, bf16), pltpu.VMEM(rows, bf16), pltpu.VMEM(slabs, bf16), pltpu.VMEM(slabs, bf16),
                pltpu.VMEM((4, C, F), f32), pltpu.VMEM((2, C, F), bf16), pltpu.VMEM((2, C, F), bf16),
                pltpu.VMEM((RING, C, D), bf16), pltpu.VMEM((RING, C, D), bf16),
                dma((n_ch,)), dma((n_ch,)), dma((pieces[0],)), dma,
            ],
            compiler_params=pltpu.CompilerParams(collective_id=0, vmem_limit_bytes=45_000_000, **params),
            name="pipeline",
        )(x.reshape(tokens, D), g.reshape(tokens, D), w1, w2)
        y, dx, d1, d2 = pl.pallas_call(
            _write_out,
            out_shape=[pltpu.HBM(pieces, bf16), pltpu.HBM(pieces, bf16), pltpu.HBM((1, D, F), f32), pltpu.HBM((1, F, D), f32)],
            in_specs=[hbm, vmem, vmem, vmem],
            out_specs=[hbm] * 4,
            scratch_shapes=[pltpu.VMEM(pieces, bf16), dma((2, 4)), dma, dma((2,))],
            compiler_params=pltpu.CompilerParams(vmem_limit_bytes=4_000_000, **params),
            name="write_out",
        )(pltpu.with_memory_space_constraint(lf, pltpu.HBM), rb, a1, a2)
        return y.reshape(x.shape), dx.reshape(x.shape), d1, d2

    return jax.shard_map(body, mesh=mesh,
                         in_specs=(P("data"), P("data"), P("stage"), P("stage")),
                         out_specs=(P("data"), P("data"), P(("data", "stage")), P(("data", "stage"))),
                         check_vma=False)
```

```python
import functools

import jax
import jax.numpy as jnp
from jax import lax
from jax.experimental import pallas as pl
from jax.experimental.pallas import tpu as pltpu
from jax.sharding import PartitionSpec as P

MESH = pl.DeviceIdType.MESH
f32 = jnp.float32
bf16 = jnp.bfloat16
D = 768
F = 3072
C = 128
H = 64
RING = 3
K = 256
LAG = 6
TW = 512
NS = F // K
C0 = 0.7978845608028654
C1 = 0.044715

WORDS = (
    (0, 5242880, 17891328, 75776308, 21184913, 138490434, 51659073, 34870145, 34837569, 154305585, 155339156, 268379202, 268435455),
    (0, 327680, 68222976, 69473089, 20191521, 69421348, 18421780, 70521668, 21119298, 68752452, 75776788, 267944835, 268435455),
    (0, 262144, 67388416, 68162629, 20190228, 54673682, 18040852, 52503569, 18096451, 69805121, 36848452, 36979268, 268378770),
    (0, 327680, 1114128, 68293139, 34816531, 76616260, 68293441, 71438996, 152122513, 69485378, 71451683, 37897251, 268432420),
    (5, 71303172, 67376132, 1638657, 51446804, 143855684, 20189457, 18096420, 38028353, 153297955, 55087940, 35856968, 268435455),
    (5, 1052672, 16843009, 51380481, 21242129, 154214691, 38015380, 37917476, 69485113, 37962307, 71578180, 69478690, 268435268),
    (66565, 151077897, 1085457, 17371161, 1114512, 20976641, 20189504, 70396233, 69486905, 42148642, 35881778, 268435234, 268435455),
    (65797, 1114129, 1052688, 1052689, 16843009, 52568979, 69477444, 59908900, 71574563, 154280777, 138560548, 71910473, 268435455),
)
STEPS = 7


def _dot(a, b):
    return jnp.dot(a, b, preferred_element_type=f32)


def _dot_t(a, b):
    return lax.dot_general(a, b, (((0,), (0,)), ((), ())), preferred_element_type=f32)


def _gelu(z):
    q = (C0 * C1) * (z * z)
    p = 0.5 * jnp.tanh(z * (C0 + q)) + 0.5
    u = z * p
    return u.astype(bf16), p + (u * (1.0 - p)) * (2.0 * C0 + 6.0 * q)


def _pipeline(n_st, n_ch, *refs):
    dma = pltpu.SemaphoreType.DMA
    pl.run_scoped(functools.partial(_work, n_st, n_ch, *refs), dma((2,)), dma((n_st // 2 - 1,)), dma((RING,)), dma((RING,)), dma((RING,)),
                  dma((2,)), dma((2,)), dma((2,)), dma((2,)), dma((2,)), dma((2,)), dma((2,)))


def _work(n_st, n_ch, x, g, w1h, w2h, lf, rb, a1, a2, zh, uh, dh,
          w1, w2, w1t, w2t, hb, gb, uw, dw, zb, ub, db, fo, bo,
          hsem, gsem, psem, lsem, wsem, esem, fsem, bsem, osem, rsem, zwsem, zrsem, uwsem, dwsem, ursem, drsem):
    d = lax.axis_index("data")
    s = lax.axis_index("stage")
    last = n_st - 1
    end = n_ch - 1
    pieces = 2 * end
    spill = s < n_st - 2
    even = s % 2 == 0
    top, low = pl.ds(0, H), pl.ds(H, H)

    def peer(k):
        return (d, k)

    def sized(i, small, full):
        short = (i == 0) | (i == end)
        pl.when(short)(small)
        pl.when(jnp.logical_not(short))(full)

    def row(i):
        return jnp.maximum(i * C - H, 0)

    def cols(k):
        return pl.ds(k * K, K)

    def load(src, dst, sem, i):
        at = pl.ds(pl.multiple_of(row(i), H), C)
        return pltpu.make_async_copy(src.at[at], dst.at[i], sem.at[i])

    def load_end(src, dst, sem, i):
        at = pl.ds(0 if i == 0 else (2 * end - 1) * H, H)
        return pltpu.make_async_copy(src.at[at], dst.at[i, top], sem.at[i])

    def landed(buf, sem, i, rows):
        part = buf.at[i, pl.ds(0, rows)]
        pltpu.make_async_copy(part, part, sem.at[i]).wait()

    get_w1 = pltpu.make_async_copy(w1h.at[0], w1, wsem.at[0])
    get_w2 = pltpu.make_async_copy(w2h.at[0], w2, wsem.at[1])

    def have_weights():
        get_w1.wait()
        get_w2.wait()

    def load_all(src, dst, sem):
        load_end(src, dst, sem, end).start()

        def f(i, _):
            load(src, dst, sem, i).start()
            return 0
        lax.fori_loop(1, end, f, 0)

    @pl.when(s == 0)
    def _():
        load_end(x, hb, hsem, 0).start()

    get_w1.start()
    get_w2.start()

    @pl.when(s == 0)
    def _():
        load_all(x, hb, hsem)

    @pl.when(s == last)
    def _():
        load_end(g, gb, gsem, 0).start()
        load_all(g, gb, gsem)

    bar = pltpu.get_barrier_semaphore()
    near = (-2, -1, 1, 2)
    for off in near:
        @pl.when((s + off >= 0) & (s + off < n_st))
        def _(off=off):
            pl.semaphore_signal(bar, inc=1, device_id=peer(s + off), device_id_type=MESH)
    peers = jnp.minimum(s, 2) + jnp.minimum(last - s, 2)

    def send(src, r, dst, i, ssem, to, dev, rows):
        part = pl.ds(0, rows)
        return pltpu.make_async_remote_copy(src_ref=src.at[r, part], dst_ref=dst.at[i, part], send_sem=ssem.at[r],
                                            recv_sem=to.at[i], device_id=peer(dev), device_id_type=MESH)

    def send_f(i, r, rows):
        return send(fo, r, hb, i, fsem, hsem, s + 1, rows)

    def send_b(i, r, rows):
        return send(bo, r, gb, i, bsem, gsem, s - 1, rows)

    def sent_f(i, r):
        sized(i, lambda: send_f(i, r, H).wait_send(), lambda: send_f(i, r, C).wait_send())

    def sent_b(i, r):
        sized(i, lambda: send_b(i, r, H).wait_send(), lambda: send_b(i, r, C).wait_send())

    def first_piece(i):
        return jnp.maximum(2 * i - 1, 0)

    def hand(src, r, k, p, ssem, dev):
        return pltpu.make_async_remote_copy(src_ref=src.at[r, pl.ds(k * H, H)], dst_ref=rb.at[p], send_sem=ssem.at[r],
                                            recv_sem=psem.at[p], device_id=peer(dev), device_id_type=MESH)

    def keep(src, r, k, p):
        return pltpu.make_async_copy(src.at[r, pl.ds(k * H, H)], lf.at[p], osem.at[r])

    def out_start(src, r, i, ssem, dev):
        p = first_piece(i)
        hand(src, r, 0, p, ssem, dev).start()
        keep(src, r, 0, p).start()

        def more():
            hand(src, r, 1, p + 1, ssem, dev).start()
            keep(src, r, 1, p + 1).start()
        sized(i, lambda: None, more)

    def out_wait(src, r, i, ssem):
        def both(rows):
            part = src.at[r, pl.ds(0, rows)]
            pltpu.make_async_copy(part, part, ssem.at[r]).wait()
            pltpu.make_async_copy(part, part, osem.at[r]).wait()
        sized(i, lambda: both(H), lambda: both(C))

    def direct(r, k):
        return pltpu.make_async_remote_copy(src_ref=bo.at[r, top], dst_ref=rb.at[pieces - 1], send_sem=esem.at[k // 2 - 1],
                                            recv_sem=psem.at[pieces - 1], device_id=peer(k), device_id_type=MESH)

    def onward(p, dev):
        return pltpu.make_async_remote_copy(src_ref=rb.at[p], dst_ref=rb.at[p], send_sem=rsem.at[0], recv_sem=psem.at[p],
                                            device_id=peer(dev), device_id_type=MESH)

    def across(p, dev):
        return pltpu.make_async_remote_copy(src_ref=rb.at[p], dst_ref=lf.at[p], send_sem=rsem.at[1], recv_sem=lsem,
                                            device_id=peer(dev), device_id_type=MESH)

    def write_z(i):
        q = lax.rem(i, 2)
        return pltpu.make_async_copy(zb.at[q], zh.at[i], zwsem.at[q])

    def read_z(i):
        q = lax.rem(i, 2)
        return pltpu.make_async_copy(zh.at[i], zb.at[2 + q], zrsem.at[q])

    def rows_of(i, rows):
        first = i == 0
        k = jnp.where(first, end // 2 - 1, lax.div(i - 1, 2))
        at = jnp.where(first, C + H, lax.rem(i - 1, 2) * C)
        return k, pl.ds(pl.multiple_of(at, H), rows)

    def write_ud(src, dst, sem, i, rows):
        k, at = rows_of(i, rows)
        q = lax.rem(i, 2)
        return pltpu.make_async_copy(src.at[q, pl.ds(0, rows)], dst.at[k, at], sem.at[q])

    def done_u(i):
        sized(i, lambda: write_ud(ub, uh, uwsem, i, H).wait(), lambda: write_ud(ub, uh, uwsem, i, C).wait())

    def done_d(i):
        sized(i, lambda: write_ud(db, dh, dwsem, i, H).wait(), lambda: write_ud(db, dh, dwsem, i, C).wait())

    def read_u(k):
        q = lax.rem(k, 2)
        return pltpu.make_async_copy(uh.at[k], uw.at[q], ursem.at[q])

    def read_d(k):
        q = lax.rem(k, 2)
        return pltpu.make_async_copy(dh.at[k], dw.at[q], drsem.at[q])

    def ensure(wait, done, want):
        for j in range(2):
            @pl.when(done + j < want)
            def _(j=j):
                wait(done + j)

    def f_slots(i):
        q = lax.rem(i, 2)
        return lax.rem(i, RING), jnp.where(spill, q, lax.rem(i, 4)), q

    def b_slots(i):
        q = lax.rem(i, 2)
        return lax.rem(i, RING), jnp.where(spill, 2 + q, lax.rem(i, 4)), q

    def f_ready(i, r, zw, uc):
        @pl.when(spill)
        def _():
            ensure(lambda j: write_z(j).wait(), zw, i - 1)

        ensure(done_u, uc, i - 1)

        @pl.when(i >= RING)
        def _():
            @pl.when(s < last)
            def _():
                sent_f(i - RING, r)

            @pl.when(s == last)
            def _():
                out_wait(fo, r, i - RING, fsem)

    def f_body(i, rows, slots):
        r, zs, q = slots
        part = pl.ds(0, rows)
        h = hb[i, part, :]
        tot = None
        for n in range(NS + LAG):
            if n < NS:
                z = _dot(h, w1[:, cols(n)])
            if n >= LAG:
                m = n - LAG
                y = _dot(ub[q, part, cols(m)], w2[cols(m), :])
                tot = y if m == 0 else tot + y
            if n < NS:
                u, gp = _gelu(z)
                zb[zs, part, cols(n)] = gp
                ub[q, part, cols(n)] = u
        fo[r, part, :] = (h.astype(f32) + tot).astype(bf16)

    def f_send(i, rows, r):
        @pl.when(s < last)
        def _():
            send_f(i, r, rows).start()

        @pl.when(s == last)
        def _():
            out_start(fo, r, i, fsem, s - 1)

        write_ud(ub, uh, uwsem, i, rows).start()

        @pl.when(spill)
        def _():
            write_z(i).start()

    def forward(i, zw, uc, fresh):
        slots = f_slots(i)
        r = slots[0]
        f_ready(i, r, zw, uc)

        def small():
            pl.when(fresh)(have_weights)
            landed(hb, hsem, i, H)
            f_body(i, H, slots)

            @pl.when(i == 0)
            def _():
                pl.semaphore_wait(bar, peers)
                hb[end, low, :] = hb[0, top, :]
            f_send(i, H, r)

        def full():
            landed(hb, hsem, i, C)
            f_body(i, C, slots)
            f_send(i, C, r)

            @pl.when(spill & (i == 4))
            def _():
                read_z(0).start()
        sized(i, small, full)

    def b_ready(i, r, zw, dc):
        @pl.when(spill)
        def _():
            read_z(i).wait()
            ensure(lambda j: write_z(j).wait(), zw, jnp.minimum(i + 2, n_ch))

            @pl.when(i + 1 < n_ch)
            def _():
                read_z(i + 1).start()

        ensure(done_d, dc, i - 1)

        @pl.when(i >= RING)
        def _():
            @pl.when(s > 0)
            def _():
                sent_b(i - RING, r)

            @pl.when(s == 0)
            def _():
                out_wait(bo, r, i - RING, bsem)

    def b_body(i, slots):
        r, zs, q = slots
        gg = gb[i]
        tot = None
        for n in range(NS + LAG):
            if n < NS:
                du = _dot(gg, w2t[:, cols(n)])
            if n >= LAG:
                m = n - LAG
                y = _dot(db[q, :, cols(m)], w1t[cols(m), :])
                tot = y if m == 0 else tot + y
            if n < NS:
                db[q, :, cols(n)] = (zb[zs, :, cols(n)] * du).astype(bf16)
        bo[r] = (gg.astype(f32) + tot).astype(bf16)

    def b_send(i, rows, r):
        @pl.when(s > 0)
        def _():
            send_b(i, r, rows).start()

        @pl.when(s == 0)
        def _():
            if rows == H:
                @pl.when(i == end)
                def _():
                    for k in range(last, 2, -2):
                        direct(r, k).start()
            out_start(bo, r, i, bsem, s + 1)

        write_ud(db, dh, dwsem, i, rows).start()

    def backward(i, zw, dc):
        slots = b_slots(i)
        r = slots[0]
        b_ready(i, r, zw, dc)

        def small():
            landed(gb, gsem, i, H)
            b_body(i, slots)

            @pl.when(i == 0)
            def _():
                gb[end, low, :] = gb[0, top, :]
            b_send(i, H, r)

        def full():
            landed(gb, gsem, i, C)
            b_body(i, slots)
            b_send(i, C, r)
        sized(i, small, full)

    def prefetch(k, uc, dc):
        ensure(done_u, uc, 2 * k + 3)
        ensure(done_d, dc, 2 * k + 3)
        read_d(k).start()
        read_u(k).start()

    def grad1(k):
        q = lax.rem(k, 2)
        h = hb[pl.ds(2 * k + 1, 2)].reshape(2 * C, D)
        for n in range(F // TW):
            sl = pl.ds(n * TW, TW)
            a1[:, sl] += _dot_t(h, dw[q, :, sl])

    def grad2(k):
        q = lax.rem(k, 2)
        gg = gb[pl.ds(2 * k + 1, 2)].reshape(2 * C, D)
        for n in range(F // TW):
            sl = pl.ds(n * TW, TW)
            a2[sl, :] += _dot_t(uw[q, :, sl], gg)

    def weights(w):
        k = lax.div(w, 2)
        odd = lax.rem(w, 2)

        @pl.when(odd == 0)
        def _():
            read_d(k).wait()
            grad1(k)

        @pl.when(odd == 1)
        def _():
            read_u(k).wait()
            grad2(k)

    def weights_both(w):
        k = lax.div(w, 2)
        read_d(k).wait()
        read_u(k).wait()
        grad1(k)
        grad2(k)

    def relay_step(p):
        piece = rb.at[p]
        pltpu.make_async_copy(piece, piece, psem.at[p]).wait()

        @pl.when(even)
        def _():
            @pl.when(s >= 2)
            def _():
                onward(p, s - 2).start()

            @pl.when(s < n_st - 2)
            def _():
                across(p, s + 1).start()

        @pl.when(jnp.logical_not(even))
        def _():
            @pl.when((s < last) & (p < pieces - 1))
            def _():
                onward(p, s + 2).start()

            @pl.when(s > 1)
            def _():
                across(p, s - 1).start()

    def transposes(fresh):
        pl.when(fresh)(have_weights)

        def f(n, _):
            sl = pl.ds(pl.multiple_of(n * 256, 256), 256)
            w1t[sl, :] = w1[:, sl].T
            w2t[:, sl] = w2[sl, :].T
            a1[:, sl] = jnp.zeros((D, 256), f32)
            a2[sl, :] = jnp.zeros((256, D), f32)
            return 0
        lax.fori_loop(0, F // 256, f, 0)

    def step(j, carry):
        word, nf, nb, nw, npf, nr, nt, zw, uc, dc = carry
        op = lax.rem(word, 16)
        is_f, is_b, is_p = op == 0, op == 1, op == 3

        @pl.when(op < 2)
        def _():
            @pl.when(is_f)
            def _():
                forward(nf, zw, uc, (nf == 0) & (nt == 0))

            @pl.when(is_b)
            def _():
                backward(nb, zw, dc)

        @pl.when((op >= 2) & (op < 6))
        def _():
            @pl.when(op == 2)
            def _():
                weights(nw)

            @pl.when(op == 4)
            def _():
                relay_step(nr)

            @pl.when(is_p)
            def _():
                prefetch(npf, uc, dc)

            @pl.when(op == 5)
            def _():
                transposes(nf == 0)

        @pl.when(op >= 6)
        def _():
            @pl.when(op == 8)
            def _():
                weights_both(nw)

            @pl.when(op == 9)
            def _():
                relay_step(nr)
                relay_step(nr + 1)

        zw = jnp.where(is_f, jnp.maximum(zw, nf - 1), zw)
        zw = jnp.where(is_b, jnp.maximum(zw, jnp.minimum(nb + 2, n_ch)), zw)
        uc = jnp.where(is_f, jnp.maximum(uc, nf - 1), uc)
        uc = jnp.where(is_p, jnp.maximum(uc, 2 * npf + 3), uc)
        dc = jnp.where(is_b, jnp.maximum(dc, nb - 1), dc)
        dc = jnp.where(is_p, jnp.maximum(dc, 2 * npf + 3), dc)
        one = lambda k: jnp.where(k, 1, 0)
        two = lambda k, m: jnp.where(op == k, 1, jnp.where(op == m, 2, 0))
        return (lax.div(word, 16), nf + one(is_f), nb + one(is_b), nw + two(2, 8), npf + one(is_p), nr + two(4, 9), nt + one(op == 5),
                zw, uc, dc)

    zero = s * 0
    words = []
    for k in range(len(WORDS[0])):
        word = zero
        for q in range(n_st):
            word = jnp.where(s == q, WORDS[q][k], word)
        words.append(word)

    def work(k, carry):
        word = words[0]
        for q in range(1, len(words)):
            word = jnp.where(k == q, words[q], word)
        out = lax.fori_loop(0, STEPS, step, (word, *carry))
        return out[1:]

    lax.fori_loop(0, len(words), work, (zero,) * 9)

    for j in range(RING):
        i = zero + (n_ch - RING + j)
        r = (n_ch - RING + j) % RING

        @pl.when(s < last)
        def _(i=i, r=r):
            sent_f(i, r)

        @pl.when(s == last)
        def _(i=i, r=r):
            out_wait(fo, r, i, fsem)

        @pl.when(s > 0)
        def _(i=i, r=r):
            sent_b(i, r)

        @pl.when(s == 0)
        def _(i=i, r=r):
            out_wait(bo, r, i, bsem)

    @pl.when(s == 0)
    def _():
        for k in range(last, 2, -2):
            direct(end % RING, k).wait_send()

    def all_of(ref, sem, count):
        part = ref.at[pl.ds(0, count)]
        pltpu.make_async_copy(part, part, sem).wait()

    @pl.when(even)
    def _():
        @pl.when(s >= 2)
        def _():
            all_of(rb, rsem.at[0], pieces)

        @pl.when(s < n_st - 2)
        def _():
            all_of(rb, rsem.at[1], pieces)

        @pl.when(s > 0)
        def _():
            all_of(lf, lsem, pieces)

    @pl.when(jnp.logical_not(even))
    def _():
        @pl.when(s < last)
        def _():
            all_of(rb, rsem.at[0], pieces - 1)
            all_of(lf, lsem, pieces)

        @pl.when(s > 1)
        def _():
            all_of(rb, rsem.at[1], pieces)


def _write_out(lf, rb, a1, a2, y, dx, d1, d2, lb, sem_w, sem_r, sem_o):
    s = lax.axis_index("stage")
    parts = 4
    big = []
    for p in range(parts):
        r1 = pl.ds(p * (D // parts), D // parts)
        r2 = pl.ds(p * (F // parts), F // parts)
        big.append(pltpu.make_async_copy(a1.at[r1], d1.at[0, r1], sem_w.at[0, p]))
        big.append(pltpu.make_async_copy(a2.at[r2], d2.at[0, r2], sem_w.at[1, p]))
    back = pltpu.make_async_copy(lf, lb, sem_r)
    back.start()
    for c in big:
        c.start()

    def rest(mine, other):
        near = pltpu.make_async_copy(rb, mine, sem_o.at[0])
        near.start()
        back.wait()
        far = pltpu.make_async_copy(lb, other, sem_o.at[1])
        far.start()
        near.wait()
        far.wait()

    @pl.when(s % 2 == 0)
    def _():
        rest(y, dx)

    @pl.when(s % 2 == 1)
    def _():
        rest(dx, y)

    for c in big:
        c.wait()


def solution(mesh):
    n_st = mesh.shape["stage"]

    def body(x, g, w1, w2):
        tokens = x.shape[0] * x.shape[1]
        n_ch = tokens // C + 1
        hbm = pl.BlockSpec(memory_space=pltpu.HBM)
        vmem = pl.BlockSpec(memory_space=pltpu.VMEM)
        dma = pltpu.SemaphoreType.DMA
        pieces = (tokens // H, H, D)
        groups = (tokens // (2 * C), 2 * C, F)
        params = dict(has_side_effects=True)
        rows = (n_ch, C, D)
        slabs = (2, 2 * C, F)
        lf, rb, a1, a2, _, _, _ = pl.pallas_call(
            functools.partial(_pipeline, n_st, n_ch),
            out_shape=[pltpu.HBM(pieces, bf16), pltpu.VMEM(pieces, bf16), pltpu.VMEM((D, F), f32), pltpu.VMEM((F, D), f32),
                       pltpu.HBM((n_ch, C, F), f32), pltpu.HBM(groups, bf16), pltpu.HBM(groups, bf16)],
            in_specs=[hbm] * 4,
            out_specs=[hbm] + [vmem] * 3 + [hbm] * 3,
            scratch_shapes=[
                pltpu.VMEM((D, F), bf16), pltpu.VMEM((F, D), bf16), pltpu.VMEM((F, D), bf16), pltpu.VMEM((D, F), bf16),
                pltpu.VMEM(rows, bf16), pltpu.VMEM(rows, bf16), pltpu.VMEM(slabs, bf16), pltpu.VMEM(slabs, bf16),
                pltpu.VMEM((4, C, F), f32), pltpu.VMEM((2, C, F), bf16), pltpu.VMEM((2, C, F), bf16),
                pltpu.VMEM((RING, C, D), bf16), pltpu.VMEM((RING, C, D), bf16),
                dma((n_ch,)), dma((n_ch,)), dma((pieces[0],)), dma,
            ],
            compiler_params=pltpu.CompilerParams(collective_id=0, vmem_limit_bytes=45_000_000, **params),
            name="pipeline",
        )(x.reshape(tokens, D), g.reshape(tokens, D), w1, w2)
        y, dx, d1, d2 = pl.pallas_call(
            _write_out,
            out_shape=[pltpu.HBM(pieces, bf16), pltpu.HBM(pieces, bf16), pltpu.HBM((1, D, F), f32), pltpu.HBM((1, F, D), f32)],
            in_specs=[hbm, vmem, vmem, vmem],
            out_specs=[hbm] * 4,
            scratch_shapes=[pltpu.VMEM(pieces, bf16), dma((2, 4)), dma, dma((2,))],
            compiler_params=pltpu.CompilerParams(vmem_limit_bytes=4_000_000, **params),
            name="write_out",
        )(pltpu.with_memory_space_constraint(lf, pltpu.HBM), rb, a1, a2)
        return y.reshape(x.shape), dx.reshape(x.shape), d1, d2

    return jax.shard_map(body, mesh=mesh,
                         in_specs=(P("data"), P("data"), P("stage"), P("stage")),
                         out_specs=(P("data"), P("data"), P(("data", "stage")), P(("data", "stage"))),
                         check_vma=False)
```

```python
import functools

import jax
import jax.numpy as jnp
from jax import lax
from jax.experimental import pallas as pl
from jax.experimental.pallas import tpu as pltpu
from jax.sharding import PartitionSpec as P

MESH = pl.DeviceIdType.MESH
f32 = jnp.float32
bf16 = jnp.bfloat16
D = 768
F = 3072
C = 128
H = 64
RING = 3
K = 256
LAG = 6
TW = 512
NS = F // K
C0 = 0.7978845608028654
C1 = 0.044715

WORDS = (
    (0, 83886080, 17891328, 54661908, 155263524, 37826881, 21107522, 71516452, 68240017, 20201778, 43161912, 71583812, 268435455),
    (0, 0, 17891333, 68436756, 38021426, 71385377, 69420081, 69280793, 153359425, 34878513, 71405892, 138617634, 268435234),
    (0, 67108864, 4457477, 17842500, 71516465, 19141666, 52642833, 37823506, 68239889, 70849555, 76100242, 43590466, 268435442),
    (0, 83886080, 16842768, 34832689, 21184833, 19108420, 152314178, 154407569, 71385619, 37954625, 71451204, 36250691, 268435444),
    (5, 4194368, 4211012, 152113172, 1061892, 60035348, 17961537, 19087636, 153687090, 71574308, 69477266, 52568628, 268435234),
    (5, 16777472, 78096, 1126657, 21107216, 51650884, 155263300, 38343460, 37299090, 76694564, 38028067, 71844900, 268435444),
    (66565, 1327172, 151060761, 18415876, 68748304, 16843792, 20976400, 71570564, 137577540, 60040082, 35856930, 268403587, 268435455),
    (65797, 1052689, 16843009, 1052688, 3211521, 36934785, 59974185, 43197586, 153371177, 70525764, 69485714, 268387474, 268435455),
)
STEPS = 7


def _dot(a, b):
    return jnp.dot(a, b, preferred_element_type=f32)


def _dot_t(a, b):
    return lax.dot_general(a, b, (((0,), (0,)), ((), ())), preferred_element_type=f32)


def _gelu(z):
    q = (C0 * C1) * (z * z)
    p = 0.5 * jnp.tanh(z * (C0 + q)) + 0.5
    u = z * p
    return u.astype(bf16), p + (u * (1.0 - p)) * (2.0 * C0 + 6.0 * q)


def _pipeline(n_st, n_ch, *refs):
    dma = pltpu.SemaphoreType.DMA
    pl.run_scoped(functools.partial(_work, n_st, n_ch, *refs), dma((n_ch,)), dma((n_ch,)), dma((2 * (n_ch - 1),)), dma, dma((2,)), dma((n_st // 2 - 1,)), dma((RING,)), dma((RING,)), dma((RING,)),
                  dma((2,)), dma((2,)), dma((2,)), dma((2,)), dma((2,)), dma((2,)), dma((2,)))


def _work(n_st, n_ch, x, g, w1h, w2h, lf, rb, a1, a2, zh, uh, dh,
          w1, w2, w1t, w2t, hb, gb, uw, dw, zb, ub, db, fo, bo,
          hsem, gsem, psem, lsem, wsem, esem, fsem, bsem, osem, rsem, zwsem, zrsem, uwsem, dwsem, ursem, drsem):
    d = lax.axis_index("data")
    s = lax.axis_index("stage")
    last = n_st - 1
    end = n_ch - 1
    pieces = 2 * end
    spill = s < n_st - 2
    even = s % 2 == 0
    top, low = pl.ds(0, H), pl.ds(H, H)

    def peer(k):
        return (d, k)

    def sized(i, small, full):
        short = (i == 0) | (i == end)
        pl.when(short)(small)
        pl.when(jnp.logical_not(short))(full)

    def row(i):
        return jnp.maximum(i * C - H, 0)

    def cols(k):
        return pl.ds(k * K, K)

    def load(src, dst, sem, i):
        at = pl.ds(pl.multiple_of(row(i), H), C)
        return pltpu.make_async_copy(src.at[at], dst.at[i], sem.at[i])

    def load_end(src, dst, sem, i):
        at = pl.ds(0 if i == 0 else (2 * end - 1) * H, H)
        return pltpu.make_async_copy(src.at[at], dst.at[i, top], sem.at[i])

    def landed(buf, sem, i, rows):
        part = buf.at[i, pl.ds(0, rows)]
        pltpu.make_async_copy(part, part, sem.at[i]).wait()

    get_w1 = pltpu.make_async_copy(w1h.at[0], w1, wsem.at[0])
    get_w2 = pltpu.make_async_copy(w2h.at[0], w2, wsem.at[1])

    def have_weights():
        get_w1.wait()
        get_w2.wait()

    def load_all(src, dst, sem):
        load_end(src, dst, sem, end).start()

        def f(i, _):
            load(src, dst, sem, i).start()
            return 0
        lax.fori_loop(1, end, f, 0)

    @pl.when(s == 0)
    def _():
        load_end(x, hb, hsem, 0).start()

    get_w1.start()
    get_w2.start()

    @pl.when(s == 0)
    def _():
        load_all(x, hb, hsem)

    @pl.when(s == last)
    def _():
        load_end(g, gb, gsem, 0).start()
        load_all(g, gb, gsem)

    bar = pltpu.get_barrier_semaphore()
    near = (-2, -1, 1, 2)
    for off in near:
        @pl.when((s + off >= 0) & (s + off < n_st))
        def _(off=off):
            pl.semaphore_signal(bar, inc=1, device_id=peer(s + off), device_id_type=MESH)
    peers = jnp.minimum(s, 2) + jnp.minimum(last - s, 2)

    def send(src, r, dst, i, ssem, to, dev, rows):
        part = pl.ds(0, rows)
        return pltpu.make_async_remote_copy(src_ref=src.at[r, part], dst_ref=dst.at[i, part], send_sem=ssem.at[r],
                                            recv_sem=to.at[i], device_id=peer(dev), device_id_type=MESH)

    def send_f(i, r, rows):
        return send(fo, r, hb, i, fsem, hsem, s + 1, rows)

    def send_b(i, r, rows):
        return send(bo, r, gb, i, bsem, gsem, s - 1, rows)

    def sent_f(i, r):
        sized(i, lambda: send_f(i, r, H).wait_send(), lambda: send_f(i, r, C).wait_send())

    def sent_b(i, r):
        sized(i, lambda: send_b(i, r, H).wait_send(), lambda: send_b(i, r, C).wait_send())

    def first_piece(i):
        return jnp.maximum(2 * i - 1, 0)

    def hand(src, r, k, p, ssem, dev):
        return pltpu.make_async_remote_copy(src_ref=src.at[r, pl.ds(k * H, H)], dst_ref=rb.at[p], send_sem=ssem.at[r],
                                            recv_sem=psem.at[p], device_id=peer(dev), device_id_type=MESH)

    def keep(src, r, k, p):
        return pltpu.make_async_copy(src.at[r, pl.ds(k * H, H)], lf.at[p], osem.at[r])

    def out_start(src, r, i, ssem, dev):
        p = first_piece(i)
        hand(src, r, 0, p, ssem, dev).start()
        keep(src, r, 0, p).start()

        def more():
            hand(src, r, 1, p + 1, ssem, dev).start()
            keep(src, r, 1, p + 1).start()
        sized(i, lambda: None, more)

    def out_wait(src, r, i, ssem):
        def both(rows):
            part = src.at[r, pl.ds(0, rows)]
            pltpu.make_async_copy(part, part, ssem.at[r]).wait()
            pltpu.make_async_copy(part, part, osem.at[r]).wait()
        sized(i, lambda: both(H), lambda: both(C))

    def direct(r, k):
        return pltpu.make_async_remote_copy(src_ref=bo.at[r, top], dst_ref=rb.at[pieces - 1], send_sem=esem.at[k // 2 - 1],
                                            recv_sem=psem.at[pieces - 1], device_id=peer(k), device_id_type=MESH)

    def onward(p, dev):
        return pltpu.make_async_remote_copy(src_ref=rb.at[p], dst_ref=rb.at[p], send_sem=rsem.at[0], recv_sem=psem.at[p],
                                            device_id=peer(dev), device_id_type=MESH)

    def across(p, dev):
        return pltpu.make_async_remote_copy(src_ref=rb.at[p], dst_ref=lf.at[p], send_sem=rsem.at[1], recv_sem=lsem,
                                            device_id=peer(dev), device_id_type=MESH)

    def write_z(i):
        q = lax.rem(i, 2)
        return pltpu.make_async_copy(zb.at[q], zh.at[i], zwsem.at[q])

    def read_z(i):
        q = lax.rem(i, 2)
        return pltpu.make_async_copy(zh.at[i], zb.at[2 + q], zrsem.at[q])

    def rows_of(i, rows):
        first = i == 0
        k = jnp.where(first, end // 2 - 1, lax.div(i - 1, 2))
        at = jnp.where(first, C + H, lax.rem(i - 1, 2) * C)
        return k, pl.ds(pl.multiple_of(at, H), rows)

    def write_ud(src, dst, sem, i, rows):
        k, at = rows_of(i, rows)
        q = lax.rem(i, 2)
        return pltpu.make_async_copy(src.at[q, pl.ds(0, rows)], dst.at[k, at], sem.at[q])

    def done_u(i):
        sized(i, lambda: write_ud(ub, uh, uwsem, i, H).wait(), lambda: write_ud(ub, uh, uwsem, i, C).wait())

    def done_d(i):
        sized(i, lambda: write_ud(db, dh, dwsem, i, H).wait(), lambda: write_ud(db, dh, dwsem, i, C).wait())

    def read_u(k):
        q = lax.rem(k, 2)
        return pltpu.make_async_copy(uh.at[k], uw.at[q], ursem.at[q])

    def read_d(k):
        q = lax.rem(k, 2)
        return pltpu.make_async_copy(dh.at[k], dw.at[q], drsem.at[q])

    def ensure(wait, done, want):
        for j in range(2):
            @pl.when(done + j < want)
            def _(j=j):
                wait(done + j)

    def f_slots(i):
        q = lax.rem(i, 2)
        return lax.rem(i, RING), jnp.where(spill, q, lax.rem(i, 4)), q

    def b_slots(i):
        q = lax.rem(i, 2)
        return lax.rem(i, RING), jnp.where(spill, 2 + q, lax.rem(i, 4)), q

    def f_ready(i, r, zw, uc):
        @pl.when(spill)
        def _():
            ensure(lambda j: write_z(j).wait(), zw, i - 1)

        ensure(done_u, uc, i - 1)

        @pl.when(i >= RING)
        def _():
            @pl.when(s < last)
            def _():
                sent_f(i - RING, r)

            @pl.when(s == last)
            def _():
                out_wait(fo, r, i - RING, fsem)

    def f_body(i, rows, slots):
        r, zs, q = slots
        part = pl.ds(0, rows)
        h = hb[i, part, :]
        tot = None
        for n in range(NS + LAG):
            if n < NS:
                z = _dot(h, w1[:, cols(n)])
            if n >= LAG:
                m = n - LAG
                y = _dot(ub[q, part, cols(m)], w2[cols(m), :])
                tot = y if m == 0 else tot + y
            if n < NS:
                u, gp = _gelu(z)
                zb[zs, part, cols(n)] = gp
                ub[q, part, cols(n)] = u
        fo[r, part, :] = (h.astype(f32) + tot).astype(bf16)

    def f_send(i, rows, r):
        @pl.when(s < last)
        def _():
            send_f(i, r, rows).start()

        @pl.when(s == last)
        def _():
            out_start(fo, r, i, fsem, s - 1)

        write_ud(ub, uh, uwsem, i, rows).start()

        @pl.when(spill)
        def _():
            write_z(i).start()

    def forward(i, zw, uc, fresh):
        slots = f_slots(i)
        r = slots[0]
        f_ready(i, r, zw, uc)

        def small():
            pl.when(fresh)(have_weights)
            landed(hb, hsem, i, H)
            f_body(i, H, slots)

            @pl.when(i == 0)
            def _():
                pl.semaphore_wait(bar, peers)
                hb[end, low, :] = hb[0, top, :]
            f_send(i, H, r)

        def full():
            landed(hb, hsem, i, C)
            f_body(i, C, slots)
            f_send(i, C, r)

            @pl.when(spill & (i == 4))
            def _():
                read_z(0).start()
        sized(i, small, full)

    def b_ready(i, r, zw, dc):
        @pl.when(spill)
        def _():
            read_z(i).wait()
            ensure(lambda j: write_z(j).wait(), zw, jnp.minimum(i + 2, n_ch))

            @pl.when(i + 1 < n_ch)
            def _():
                read_z(i + 1).start()

        ensure(done_d, dc, i - 1)

        @pl.when(i >= RING)
        def _():
            @pl.when(s > 0)
            def _():
                sent_b(i - RING, r)

            @pl.when(s == 0)
            def _():
                out_wait(bo, r, i - RING, bsem)

    def b_body(i, slots):
        r, zs, q = slots
        gg = gb[i]
        tot = None
        for n in range(NS + LAG):
            if n < NS:
                du = _dot(gg, w2t[:, cols(n)])
            if n >= LAG:
                m = n - LAG
                y = _dot(db[q, :, cols(m)], w1t[cols(m), :])
                tot = y if m == 0 else tot + y
            if n < NS:
                db[q, :, cols(n)] = (zb[zs, :, cols(n)] * du).astype(bf16)
        bo[r] = (gg.astype(f32) + tot).astype(bf16)

    def b_send(i, rows, r):
        @pl.when(s > 0)
        def _():
            send_b(i, r, rows).start()

        @pl.when(s == 0)
        def _():
            if rows == H:
                @pl.when(i == end)
                def _():
                    for k in range(last, 2, -2):
                        direct(r, k).start()
            out_start(bo, r, i, bsem, s + 1)

        write_ud(db, dh, dwsem, i, rows).start()

    def backward(i, zw, dc):
        slots = b_slots(i)
        r = slots[0]
        b_ready(i, r, zw, dc)

        def small():
            landed(gb, gsem, i, H)
            b_body(i, slots)

            @pl.when(i == 0)
            def _():
                gb[end, low, :] = gb[0, top, :]
            b_send(i, H, r)

        def full():
            landed(gb, gsem, i, C)
            b_body(i, slots)
            b_send(i, C, r)
        sized(i, small, full)

    def prefetch(k, uc, dc):
        ensure(done_u, uc, 2 * k + 3)
        ensure(done_d, dc, 2 * k + 3)
        read_d(k).start()
        read_u(k).start()

    def grad1(k):
        q = lax.rem(k, 2)
        h = hb[pl.ds(2 * k + 1, 2)].reshape(2 * C, D)
        for n in range(F // TW):
            sl = pl.ds(n * TW, TW)
            a1[:, sl] += _dot_t(h, dw[q, :, sl])

    def grad2(k):
        q = lax.rem(k, 2)
        gg = gb[pl.ds(2 * k + 1, 2)].reshape(2 * C, D)
        for n in range(F // TW):
            sl = pl.ds(n * TW, TW)
            a2[sl, :] += _dot_t(uw[q, :, sl], gg)

    def weights(w):
        k = lax.div(w, 2)
        odd = lax.rem(w, 2)

        @pl.when(odd == 0)
        def _():
            read_d(k).wait()
            grad1(k)

        @pl.when(odd == 1)
        def _():
            read_u(k).wait()
            grad2(k)

    def weights_both(w):
        k = lax.div(w, 2)
        read_d(k).wait()
        read_u(k).wait()
        grad1(k)
        grad2(k)

    def relay_step(p):
        piece = rb.at[p]
        pltpu.make_async_copy(piece, piece, psem.at[p]).wait()

        @pl.when(even)
        def _():
            @pl.when(s >= 2)
            def _():
                onward(p, s - 2).start()

            @pl.when(s < n_st - 2)
            def _():
                across(p, s + 1).start()

        @pl.when(jnp.logical_not(even))
        def _():
            @pl.when((s < last) & (p < pieces - 1))
            def _():
                onward(p, s + 2).start()

            @pl.when(s > 1)
            def _():
                across(p, s - 1).start()

    def transposes(fresh):
        pl.when(fresh)(have_weights)

        def f(n, _):
            sl = pl.ds(pl.multiple_of(n * 256, 256), 256)
            w1t[sl, :] = w1[:, sl].T
            w2t[:, sl] = w2[sl, :].T
            a1[:, sl] = jnp.zeros((D, 256), f32)
            a2[sl, :] = jnp.zeros((256, D), f32)
            return 0
        lax.fori_loop(0, F // 256, f, 0)

    def step(j, carry):
        word, nf, nb, nw, npf, nr, nt, zw, uc, dc = carry
        op = lax.rem(word, 16)
        is_f, is_b, is_p = op == 0, op == 1, op == 3

        @pl.when(op < 2)
        def _():
            @pl.when(is_f)
            def _():
                forward(nf, zw, uc, (nf == 0) & (nt == 0))

            @pl.when(is_b)
            def _():
                backward(nb, zw, dc)

        @pl.when((op >= 2) & (op < 6))
        def _():
            @pl.when(op == 2)
            def _():
                weights(nw)

            @pl.when(op == 4)
            def _():
                relay_step(nr)

            @pl.when(is_p)
            def _():
                prefetch(npf, uc, dc)

            @pl.when(op == 5)
            def _():
                transposes(nf == 0)

        @pl.when(op >= 6)
        def _():
            @pl.when(op == 8)
            def _():
                weights_both(nw)

            @pl.when(op == 9)
            def _():
                relay_step(nr)
                relay_step(nr + 1)

        zw = jnp.where(is_f, jnp.maximum(zw, nf - 1), zw)
        zw = jnp.where(is_b, jnp.maximum(zw, jnp.minimum(nb + 2, n_ch)), zw)
        uc = jnp.where(is_f, jnp.maximum(uc, nf - 1), uc)
        uc = jnp.where(is_p, jnp.maximum(uc, 2 * npf + 3), uc)
        dc = jnp.where(is_b, jnp.maximum(dc, nb - 1), dc)
        dc = jnp.where(is_p, jnp.maximum(dc, 2 * npf + 3), dc)
        one = lambda k: jnp.where(k, 1, 0)
        two = lambda k, m: jnp.where(op == k, 1, jnp.where(op == m, 2, 0))
        return (lax.div(word, 16), nf + one(is_f), nb + one(is_b), nw + two(2, 8), npf + one(is_p), nr + two(4, 9), nt + one(op == 5),
                zw, uc, dc)

    zero = s * 0
    words = []
    for k in range(len(WORDS[0])):
        word = zero
        for q in range(n_st):
            word = jnp.where(s == q, WORDS[q][k], word)
        words.append(word)

    def work(k, carry):
        word = words[0]
        for q in range(1, len(words)):
            word = jnp.where(k == q, words[q], word)
        out = lax.fori_loop(0, STEPS, step, (word, *carry))
        return out[1:]

    lax.fori_loop(0, len(words), work, (zero,) * 9)

    for j in range(RING):
        i = zero + (n_ch - RING + j)
        r = (n_ch - RING + j) % RING

        @pl.when(s < last)
        def _(i=i, r=r):
            sent_f(i, r)

        @pl.when(s == last)
        def _(i=i, r=r):
            out_wait(fo, r, i, fsem)

        @pl.when(s > 0)
        def _(i=i, r=r):
            sent_b(i, r)

        @pl.when(s == 0)
        def _(i=i, r=r):
            out_wait(bo, r, i, bsem)

    @pl.when(s == 0)
    def _():
        for k in range(last, 2, -2):
            direct(end % RING, k).wait_send()

    def all_of(ref, sem, count):
        part = ref.at[pl.ds(0, count)]
        pltpu.make_async_copy(part, part, sem).wait()

    @pl.when(even)
    def _():
        @pl.when(s >= 2)
        def _():
            all_of(rb, rsem.at[0], pieces)

        @pl.when(s < n_st - 2)
        def _():
            all_of(rb, rsem.at[1], pieces)

        @pl.when(s > 0)
        def _():
            all_of(lf, lsem, pieces)

    @pl.when(jnp.logical_not(even))
    def _():
        @pl.when(s < last)
        def _():
            all_of(rb, rsem.at[0], pieces - 1)
            all_of(lf, lsem, pieces)

        @pl.when(s > 1)
        def _():
            all_of(rb, rsem.at[1], pieces)


def _write_out(lf, rb, a1, a2, y, dx, d1, d2, lb, sem_w, sem_r, sem_o):
    s = lax.axis_index("stage")
    parts = 4
    big = []
    for p in range(parts):
        r1 = pl.ds(p * (D // parts), D // parts)
        r2 = pl.ds(p * (F // parts), F // parts)
        big.append(pltpu.make_async_copy(a1.at[r1], d1.at[0, r1], sem_w.at[0, p]))
        big.append(pltpu.make_async_copy(a2.at[r2], d2.at[0, r2], sem_w.at[1, p]))
    back = pltpu.make_async_copy(lf, lb, sem_r)
    back.start()
    for c in big:
        c.start()

    def rest(mine, other):
        near = pltpu.make_async_copy(rb, mine, sem_o.at[0])
        near.start()
        back.wait()
        far = pltpu.make_async_copy(lb, other, sem_o.at[1])
        far.start()
        near.wait()
        far.wait()

    @pl.when(s % 2 == 0)
    def _():
        rest(y, dx)

    @pl.when(s % 2 == 1)
    def _():
        rest(dx, y)

    for c in big:
        c.wait()


def solution(mesh):
    n_st = mesh.shape["stage"]

    def body(x, g, w1, w2):
        tokens = x.shape[0] * x.shape[1]
        n_ch = tokens // C + 1
        hbm = pl.BlockSpec(memory_space=pltpu.HBM)
        vmem = pl.BlockSpec(memory_space=pltpu.VMEM)
        dma = pltpu.SemaphoreType.DMA
        pieces = (tokens // H, H, D)
        groups = (tokens // (2 * C), 2 * C, F)
        params = dict(has_side_effects=True)
        rows = (n_ch, C, D)
        slabs = (2, 2 * C, F)
        lf, rb, a1, a2, _, _, _ = pl.pallas_call(
            functools.partial(_pipeline, n_st, n_ch),
            out_shape=[pltpu.HBM(pieces, bf16), pltpu.VMEM(pieces, bf16), pltpu.VMEM((D, F), f32), pltpu.VMEM((F, D), f32),
                       pltpu.HBM((n_ch, C, F), f32), pltpu.HBM(groups, bf16), pltpu.HBM(groups, bf16)],
            in_specs=[hbm] * 4,
            out_specs=[hbm] + [vmem] * 3 + [hbm] * 3,
            scratch_shapes=[
                pltpu.VMEM((D, F), bf16), pltpu.VMEM((F, D), bf16), pltpu.VMEM((F, D), bf16), pltpu.VMEM((D, F), bf16),
                pltpu.VMEM(rows, bf16), pltpu.VMEM(rows, bf16), pltpu.VMEM(slabs, bf16), pltpu.VMEM(slabs, bf16),
                pltpu.VMEM((4, C, F), f32), pltpu.VMEM((2, C, F), bf16), pltpu.VMEM((2, C, F), bf16),
                pltpu.VMEM((RING, C, D), bf16), pltpu.VMEM((RING, C, D), bf16),
            ],
            compiler_params=pltpu.CompilerParams(collective_id=0, vmem_limit_bytes=45_000_000, **params),
            name="pipeline",
        )(x.reshape(tokens, D), g.reshape(tokens, D), w1, w2)
        y, dx, d1, d2 = pl.pallas_call(
            _write_out,
            out_shape=[pltpu.HBM(pieces, bf16), pltpu.HBM(pieces, bf16), pltpu.HBM((1, D, F), f32), pltpu.HBM((1, F, D), f32)],
            in_specs=[hbm, vmem, vmem, vmem],
            out_specs=[hbm] * 4,
            scratch_shapes=[pltpu.VMEM(pieces, bf16), dma((2, 4)), dma, dma((2,))],
            compiler_params=pltpu.CompilerParams(vmem_limit_bytes=4_000_000, **params),
            name="write_out",
        )(pltpu.with_memory_space_constraint(lf, pltpu.HBM), rb, a1, a2)
        return y.reshape(x.shape), dx.reshape(x.shape), d1, d2

    return jax.shard_map(body, mesh=mesh,
                         in_specs=(P("data"), P("data"), P("stage"), P("stage")),
                         out_specs=(P("data"), P("data"), P(("data", "stage")), P(("data", "stage"))),
                         check_vma=False)
```

```python
import functools

import jax
import jax.numpy as jnp
from jax import lax
from jax.experimental import pallas as pl
from jax.experimental.pallas import tpu as pltpu
from jax.sharding import PartitionSpec as P

MESH = pl.DeviceIdType.MESH
f32 = jnp.float32
bf16 = jnp.bfloat16
D = 768
F = 3072
C = 128
H = 64
RING = 3
K = 256
LAG = 6
TW = 512
NS = F // K
C0 = 0.7978845608028654
C1 = 0.044715

WORDS = (
    (0, 0, 71631872, 18125076, 69411139, 18030866, 77107512, 68436753, 20058898, 59315348, 155814296, 268435455, 268435455),
    (0, 83886080, 17891328, 35210004, 71536962, 43074577, 138679186, 54596673, 35198020, 35205444, 138642484, 268433539, 268435455),
    (0, 67108864, 71581696, 18105664, 38342961, 17962034, 37893185, 19994913, 69276707, 69480769, 43291698, 37894436, 268435234),
    (0, 0, 17891589, 18948115, 38343699, 69473060, 152639763, 34882578, 152257556, 38023746, 38028340, 138556050, 268435455),
    (5, 67108928, 20977924, 19928128, 34621729, 9515284, 19153218, 17973553, 152310819, 38348947, 60310595, 268378680, 268435455),
    (5, 16777472, 1249296, 51450384, 18022658, 155264065, 34874388, 69289107, 71516707, 54673986, 54805060, 75798596, 268435268),
    (66565, 1327172, 152111380, 18415872, 152634384, 51384336, 20975936, 76747908, 35796116, 35801411, 36844067, 268433464, 268435455),
    (65797, 16781569, 16843009, 1052688, 3211521, 35865473, 71582274, 37893267, 69477449, 70530116, 36979352, 71926852, 268435455),
)
STEPS = 7


def _dot(a, b):
    return jnp.dot(a, b, preferred_element_type=f32)


def _dot_t(a, b):
    return lax.dot_general(a, b, (((0,), (0,)), ((), ())), preferred_element_type=f32)


def _gelu(z):
    q = (C0 * C1) * (z * z)
    p = 0.5 * jnp.tanh(z * (C0 + q)) + 0.5
    u = z * p
    return u.astype(bf16), p + (u * (1.0 - p)) * (2.0 * C0 + 6.0 * q)


def _pipeline(n_st, n_ch, *refs):
    dma = pltpu.SemaphoreType.DMA
    pl.run_scoped(functools.partial(_work, n_st, n_ch, *refs), dma((n_ch,)), dma((n_ch,)), dma((2 * (n_ch - 1),)), dma, dma((2,)), dma((n_st // 2 - 1,)), dma((RING,)), dma((RING,)), dma((RING,)),
                  dma((2,)), dma((2,)), dma((2,)), dma((2,)), dma((2,)), dma((2,)), dma((2,)))


def _work(n_st, n_ch, x, g, w1h, w2h, lf, rb, a1, a2, zh, uh, dh,
          w1, w2, w1t, w2t, hb, gb, uw, dw, zb, ub, db, fo, bo,
          hsem, gsem, psem, lsem, wsem, esem, fsem, bsem, osem, rsem, zwsem, zrsem, uwsem, dwsem, ursem, drsem):
    d = lax.axis_index("data")
    s = lax.axis_index("stage")
    last = n_st - 1
    end = n_ch - 1
    pieces = 2 * end
    spill = s < n_st - 2
    even = s % 2 == 0
    top, low = pl.ds(0, H), pl.ds(H, H)

    def peer(k):
        return (d, k)

    def sized(i, small, full):
        short = (i == 0) | (i == end)
        pl.when(short)(small)
        pl.when(jnp.logical_not(short))(full)

    def row(i):
        return jnp.maximum(i * C - H, 0)

    def cols(k):
        return pl.ds(k * K, K)

    def load(src, dst, sem, i):
        at = pl.ds(pl.multiple_of(row(i), H), C)
        return pltpu.make_async_copy(src.at[at], dst.at[i], sem.at[i])

    def load_end(src, dst, sem, i):
        at = pl.ds(0 if i == 0 else (2 * end - 1) * H, H)
        return pltpu.make_async_copy(src.at[at], dst.at[i, top], sem.at[i])

    def landed(buf, sem, i, rows):
        part = buf.at[i, pl.ds(0, rows)]
        pltpu.make_async_copy(part, part, sem.at[i]).wait()

    get_w1 = pltpu.make_async_copy(w1h.at[0], w1, wsem.at[0])
    get_w2 = pltpu.make_async_copy(w2h.at[0], w2, wsem.at[1])

    def have_weights():
        get_w1.wait()
        get_w2.wait()

    def load_all(src, dst, sem):
        load_end(src, dst, sem, end).start()

        def f(i, _):
            load(src, dst, sem, i).start()
            return 0
        lax.fori_loop(1, end, f, 0)

    @pl.when(s == 0)
    def _():
        load_end(x, hb, hsem, 0).start()

    get_w1.start()
    get_w2.start()

    @pl.when(s == 0)
    def _():
        load_all(x, hb, hsem)

    @pl.when(s == last)
    def _():
        load_end(g, gb, gsem, 0).start()
        load_all(g, gb, gsem)

    bar = pltpu.get_barrier_semaphore()
    near = (-2, -1, 1, 2)
    for off in near:
        @pl.when((s + off >= 0) & (s + off < n_st))
        def _(off=off):
            pl.semaphore_signal(bar, inc=1, device_id=peer(s + off), device_id_type=MESH)
    peers = jnp.minimum(s, 2) + jnp.minimum(last - s, 2)

    def send(src, r, dst, i, ssem, to, dev, rows):
        part = pl.ds(0, rows)
        return pltpu.make_async_remote_copy(src_ref=src.at[r, part], dst_ref=dst.at[i, part], send_sem=ssem.at[r],
                                            recv_sem=to.at[i], device_id=peer(dev), device_id_type=MESH)

    def send_f(i, r, rows):
        return send(fo, r, hb, i, fsem, hsem, s + 1, rows)

    def send_b(i, r, rows):
        return send(bo, r, gb, i, bsem, gsem, s - 1, rows)

    def sent_f(i, r):
        sized(i, lambda: send_f(i, r, H).wait_send(), lambda: send_f(i, r, C).wait_send())

    def sent_b(i, r):
        sized(i, lambda: send_b(i, r, H).wait_send(), lambda: send_b(i, r, C).wait_send())

    def first_piece(i):
        return jnp.maximum(2 * i - 1, 0)

    def hand(src, r, k, p, ssem, dev):
        return pltpu.make_async_remote_copy(src_ref=src.at[r, pl.ds(k * H, H)], dst_ref=rb.at[p], send_sem=ssem.at[r],
                                            recv_sem=psem.at[p], device_id=peer(dev), device_id_type=MESH)

    def keep(src, r, k, p):
        return pltpu.make_async_copy(src.at[r, pl.ds(k * H, H)], lf.at[p], osem.at[r])

    def out_start(src, r, i, ssem, dev):
        p = first_piece(i)
        hand(src, r, 0, p, ssem, dev).start()
        keep(src, r, 0, p).start()

        def more():
            hand(src, r, 1, p + 1, ssem, dev).start()
            keep(src, r, 1, p + 1).start()
        sized(i, lambda: None, more)

    def out_wait(src, r, i, ssem):
        def both(rows):
            part = src.at[r, pl.ds(0, rows)]
            pltpu.make_async_copy(part, part, ssem.at[r]).wait()
            pltpu.make_async_copy(part, part, osem.at[r]).wait()
        sized(i, lambda: both(H), lambda: both(C))

    def direct(r, k):
        return pltpu.make_async_remote_copy(src_ref=bo.at[r, top], dst_ref=rb.at[pieces - 1], send_sem=esem.at[k // 2 - 1],
                                            recv_sem=psem.at[pieces - 1], device_id=peer(k), device_id_type=MESH)

    def onward(p, dev):
        return pltpu.make_async_remote_copy(src_ref=rb.at[p], dst_ref=rb.at[p], send_sem=rsem.at[0], recv_sem=psem.at[p],
                                            device_id=peer(dev), device_id_type=MESH)

    def across(p, dev):
        return pltpu.make_async_remote_copy(src_ref=rb.at[p], dst_ref=lf.at[p], send_sem=rsem.at[1], recv_sem=lsem,
                                            device_id=peer(dev), device_id_type=MESH)

    def write_z(i):
        q = lax.rem(i, 2)
        return pltpu.make_async_copy(zb.at[q], zh.at[i], zwsem.at[q])

    def read_z(i):
        q = lax.rem(i, 2)
        return pltpu.make_async_copy(zh.at[i], zb.at[2 + q], zrsem.at[q])

    def rows_of(i, rows):
        first = i == 0
        k = jnp.where(first, end // 2 - 1, lax.div(i - 1, 2))
        at = jnp.where(first, C + H, lax.rem(i - 1, 2) * C)
        return k, pl.ds(pl.multiple_of(at, H), rows)

    def write_ud(src, dst, sem, i, rows):
        k, at = rows_of(i, rows)
        q = lax.rem(i, 2)
        return pltpu.make_async_copy(src.at[q, pl.ds(0, rows)], dst.at[k, at], sem.at[q])

    def done_u(i):
        sized(i, lambda: write_ud(ub, uh, uwsem, i, H).wait(), lambda: write_ud(ub, uh, uwsem, i, C).wait())

    def done_d(i):
        sized(i, lambda: write_ud(db, dh, dwsem, i, H).wait(), lambda: write_ud(db, dh, dwsem, i, C).wait())

    def read_u(k):
        q = lax.rem(k, 2)
        return pltpu.make_async_copy(uh.at[k], uw.at[q], ursem.at[q])

    def read_d(k):
        q = lax.rem(k, 2)
        return pltpu.make_async_copy(dh.at[k], dw.at[q], drsem.at[q])

    def ensure(wait, done, want):
        for j in range(2):
            @pl.when(done + j < want)
            def _(j=j):
                wait(done + j)

    def f_slots(i):
        q = lax.rem(i, 2)
        return lax.rem(i, RING), jnp.where(spill, q, lax.rem(i, 4)), q

    def b_slots(i):
        q = lax.rem(i, 2)
        return lax.rem(i, RING), jnp.where(spill, 2 + q, lax.rem(i, 4)), q

    def f_ready(i, r, zw, uc):
        @pl.when(spill)
        def _():
            ensure(lambda j: write_z(j).wait(), zw, i - 1)

        ensure(done_u, uc, i - 1)

        @pl.when(i >= RING)
        def _():
            @pl.when(s < last)
            def _():
                sent_f(i - RING, r)

            @pl.when(s == last)
            def _():
                out_wait(fo, r, i - RING, fsem)

    def f_body(i, rows, slots):
        r, zs, q = slots
        part = pl.ds(0, rows)
        h = hb[i, part, :]
        tot = None
        for n in range(NS + LAG):
            if n < NS:
                z = _dot(h, w1[:, cols(n)])
            if n >= LAG:
                m = n - LAG
                y = _dot(ub[q, part, cols(m)], w2[cols(m), :])
                tot = y if m == 0 else tot + y
            if n < NS:
                u, gp = _gelu(z)
                zb[zs, part, cols(n)] = gp
                ub[q, part, cols(n)] = u
        fo[r, part, :] = (h.astype(f32) + tot).astype(bf16)

    def f_send(i, rows, r):
        @pl.when(s < last)
        def _():
            send_f(i, r, rows).start()

        @pl.when(s == last)
        def _():
            out_start(fo, r, i, fsem, s - 1)

        write_ud(ub, uh, uwsem, i, rows).start()

        @pl.when(spill)
        def _():
            write_z(i).start()

    def forward(i, zw, uc, fresh):
        slots = f_slots(i)
        r = slots[0]
        f_ready(i, r, zw, uc)

        def small():
            pl.when(fresh)(have_weights)
            landed(hb, hsem, i, H)
            f_body(i, H, slots)

            @pl.when(i == 0)
            def _():
                pl.semaphore_wait(bar, peers)
                hb[end, low, :] = hb[0, top, :]
            f_send(i, H, r)

        def full():
            landed(hb, hsem, i, C)
            f_body(i, C, slots)
            f_send(i, C, r)

            @pl.when(spill & (i == 4))
            def _():
                read_z(0).start()
        sized(i, small, full)

    def b_ready(i, r, zw, dc):
        @pl.when(spill)
        def _():
            read_z(i).wait()
            ensure(lambda j: write_z(j).wait(), zw, jnp.minimum(i + 2, n_ch))

            @pl.when(i + 1 < n_ch)
            def _():
                read_z(i + 1).start()

        ensure(done_d, dc, i - 1)

        @pl.when(i >= RING)
        def _():
            @pl.when(s > 0)
            def _():
                sent_b(i - RING, r)

            @pl.when(s == 0)
            def _():
                out_wait(bo, r, i - RING, bsem)

    def b_body(i, slots):
        r, zs, q = slots
        gg = gb[i]
        tot = None
        for n in range(NS + LAG):
            if n < NS:
                du = _dot(gg, w2t[:, cols(n)])
            if n >= LAG:
                m = n - LAG
                y = _dot(db[q, :, cols(m)], w1t[cols(m), :])
                tot = y if m == 0 else tot + y
            if n < NS:
                db[q, :, cols(n)] = (zb[zs, :, cols(n)] * du).astype(bf16)
        bo[r] = (gg.astype(f32) + tot).astype(bf16)

    def b_send(i, rows, r):
        @pl.when(s > 0)
        def _():
            send_b(i, r, rows).start()

        @pl.when(s == 0)
        def _():
            if rows == H:
                @pl.when(i == end)
                def _():
                    for k in range(last, 2, -2):
                        direct(r, k).start()
            out_start(bo, r, i, bsem, s + 1)

        write_ud(db, dh, dwsem, i, rows).start()

    def backward(i, zw, dc):
        slots = b_slots(i)
        r = slots[0]
        b_ready(i, r, zw, dc)

        def small():
            landed(gb, gsem, i, H)
            b_body(i, slots)

            @pl.when(i == 0)
            def _():
                gb[end, low, :] = gb[0, top, :]
            b_send(i, H, r)

        def full():
            landed(gb, gsem, i, C)
            b_body(i, slots)
            b_send(i, C, r)
        sized(i, small, full)

    def prefetch(k, uc, dc):
        ensure(done_u, uc, 2 * k + 3)
        ensure(done_d, dc, 2 * k + 3)
        read_d(k).start()
        read_u(k).start()

    def grad1(k):
        q = lax.rem(k, 2)
        h = hb[pl.ds(2 * k + 1, 2)].reshape(2 * C, D)
        for n in range(F // TW):
            sl = pl.ds(n * TW, TW)
            a1[:, sl] += _dot_t(h, dw[q, :, sl])

    def grad2(k):
        q = lax.rem(k, 2)
        gg = gb[pl.ds(2 * k + 1, 2)].reshape(2 * C, D)
        for n in range(F // TW):
            sl = pl.ds(n * TW, TW)
            a2[sl, :] += _dot_t(uw[q, :, sl], gg)

    def weights(w):
        k = lax.div(w, 2)
        odd = lax.rem(w, 2)

        @pl.when(odd == 0)
        def _():
            read_d(k).wait()
            grad1(k)

        @pl.when(odd == 1)
        def _():
            read_u(k).wait()
            grad2(k)

    def weights_both(w):
        k = lax.div(w, 2)
        read_d(k).wait()
        read_u(k).wait()
        grad1(k)
        grad2(k)

    def relay_step(p):
        piece = rb.at[p]
        pltpu.make_async_copy(piece, piece, psem.at[p]).wait()

        @pl.when(even)
        def _():
            @pl.when(s >= 2)
            def _():
                onward(p, s - 2).start()

            @pl.when(s < n_st - 2)
            def _():
                across(p, s + 1).start()

        @pl.when(jnp.logical_not(even))
        def _():
            @pl.when((s < last) & (p < pieces - 1))
            def _():
                onward(p, s + 2).start()

            @pl.when(s > 1)
            def _():
                across(p, s - 1).start()

    def transposes(fresh):
        pl.when(fresh)(have_weights)

        def f(n, _):
            sl = pl.ds(pl.multiple_of(n * 256, 256), 256)
            w1t[sl, :] = w1[:, sl].T
            w2t[:, sl] = w2[sl, :].T
            a1[:, sl] = jnp.zeros((D, 256), f32)
            a2[sl, :] = jnp.zeros((256, D), f32)
            return 0
        lax.fori_loop(0, F // 256, f, 0)

    def step(j, carry):
        word, nf, nb, nw, npf, nr, nt, zw, uc, dc = carry
        op = lax.rem(word, 16)
        is_f, is_b, is_p = op == 0, op == 1, op == 3

        @pl.when(op < 2)
        def _():
            @pl.when(is_f)
            def _():
                forward(nf, zw, uc, (nf == 0) & (nt == 0))

            @pl.when(is_b)
            def _():
                backward(nb, zw, dc)

        @pl.when((op >= 2) & (op < 6))
        def _():
            @pl.when(op == 2)
            def _():
                weights(nw)

            @pl.when(op == 4)
            def _():
                relay_step(nr)

            @pl.when(is_p)
            def _():
                prefetch(npf, uc, dc)

            @pl.when(op == 5)
            def _():
                transposes(nf == 0)

        @pl.when(op >= 6)
        def _():
            @pl.when(op == 8)
            def _():
                weights_both(nw)

            @pl.when(op == 9)
            def _():
                relay_step(nr)
                relay_step(nr + 1)

        zw = jnp.where(is_f, jnp.maximum(zw, nf - 1), zw)
        zw = jnp.where(is_b, jnp.maximum(zw, jnp.minimum(nb + 2, n_ch)), zw)
        uc = jnp.where(is_f, jnp.maximum(uc, nf - 1), uc)
        uc = jnp.where(is_p, jnp.maximum(uc, 2 * npf + 3), uc)
        dc = jnp.where(is_b, jnp.maximum(dc, nb - 1), dc)
        dc = jnp.where(is_p, jnp.maximum(dc, 2 * npf + 3), dc)
        one = lambda k: jnp.where(k, 1, 0)
        two = lambda k, m: jnp.where(op == k, 1, jnp.where(op == m, 2, 0))
        return (lax.div(word, 16), nf + one(is_f), nb + one(is_b), nw + two(2, 8), npf + one(is_p), nr + two(4, 9), nt + one(op == 5),
                zw, uc, dc)

    zero = s * 0
    words = []
    for k in range(len(WORDS[0])):
        word = zero
        for q in range(n_st):
            word = jnp.where(s == q, WORDS[q][k], word)
        words.append(word)

    def work(k, carry):
        word = words[0]
        for q in range(1, len(words)):
            word = jnp.where(k == q, words[q], word)
        out = lax.fori_loop(0, STEPS, step, (word, *carry))
        return out[1:]

    lax.fori_loop(0, len(words), work, (zero,) * 9)

    for j in range(RING):
        i = zero + (n_ch - RING + j)
        r = (n_ch - RING + j) % RING

        @pl.when(s < last)
        def _(i=i, r=r):
            sent_f(i, r)

        @pl.when(s == last)
        def _(i=i, r=r):
            out_wait(fo, r, i, fsem)

        @pl.when(s > 0)
        def _(i=i, r=r):
            sent_b(i, r)

        @pl.when(s == 0)
        def _(i=i, r=r):
            out_wait(bo, r, i, bsem)

    @pl.when(s == 0)
    def _():
        for k in range(last, 2, -2):
            direct(end % RING, k).wait_send()

    def all_of(ref, sem, count):
        part = ref.at[pl.ds(0, count)]
        pltpu.make_async_copy(part, part, sem).wait()

    @pl.when(even)
    def _():
        @pl.when(s >= 2)
        def _():
            all_of(rb, rsem.at[0], pieces)

        @pl.when(s < n_st - 2)
        def _():
            all_of(rb, rsem.at[1], pieces)

        @pl.when(s > 0)
        def _():
            all_of(lf, lsem, pieces)

    @pl.when(jnp.logical_not(even))
    def _():
        @pl.when(s < last)
        def _():
            all_of(rb, rsem.at[0], pieces - 1)
            all_of(lf, lsem, pieces)

        @pl.when(s > 1)
        def _():
            all_of(rb, rsem.at[1], pieces)


def _write_out(*refs):
    dma = pltpu.SemaphoreType.DMA
    pl.run_scoped(functools.partial(_write, *refs), dma((2, 4)), dma, dma((2,)))


def _write(lf, rb, a1, a2, y, dx, d1, d2, lb, sem_w, sem_r, sem_o):
    s = lax.axis_index("stage")
    parts = 4
    big = []
    for p in range(parts):
        r1 = pl.ds(p * (D // parts), D // parts)
        r2 = pl.ds(p * (F // parts), F // parts)
        big.append(pltpu.make_async_copy(a1.at[r1], d1.at[0, r1], sem_w.at[0, p]))
        big.append(pltpu.make_async_copy(a2.at[r2], d2.at[0, r2], sem_w.at[1, p]))
    back = pltpu.make_async_copy(lf, lb, sem_r)
    back.start()
    for c in big:
        c.start()

    def rest(mine, other):
        near = pltpu.make_async_copy(rb, mine, sem_o.at[0])
        near.start()
        back.wait()
        far = pltpu.make_async_copy(lb, other, sem_o.at[1])
        far.start()
        near.wait()
        far.wait()

    @pl.when(s % 2 == 0)
    def _():
        rest(y, dx)

    @pl.when(s % 2 == 1)
    def _():
        rest(dx, y)

    for c in big:
        c.wait()


def solution(mesh):
    n_st = mesh.shape["stage"]

    def body(x, g, w1, w2):
        tokens = x.shape[0] * x.shape[1]
        n_ch = tokens // C + 1
        hbm = pl.BlockSpec(memory_space=pltpu.HBM)
        vmem = pl.BlockSpec(memory_space=pltpu.VMEM)
        dma = pltpu.SemaphoreType.DMA
        pieces = (tokens // H, H, D)
        groups = (tokens // (2 * C), 2 * C, F)
        params = dict(has_side_effects=True)
        rows = (n_ch, C, D)
        slabs = (2, 2 * C, F)
        lf, rb, a1, a2, _, _, _ = pl.pallas_call(
            functools.partial(_pipeline, n_st, n_ch),
            out_shape=[pltpu.HBM(pieces, bf16), pltpu.VMEM(pieces, bf16), pltpu.VMEM((D, F), f32), pltpu.VMEM((F, D), f32),
                       pltpu.HBM((n_ch, C, F), f32), pltpu.HBM(groups, bf16), pltpu.HBM(groups, bf16)],
            in_specs=[hbm] * 4,
            out_specs=[hbm] + [vmem] * 3 + [hbm] * 3,
            scratch_shapes=[
                pltpu.VMEM((D, F), bf16), pltpu.VMEM((F, D), bf16), pltpu.VMEM((F, D), bf16), pltpu.VMEM((D, F), bf16),
                pltpu.VMEM(rows, bf16), pltpu.VMEM(rows, bf16), pltpu.VMEM(slabs, bf16), pltpu.VMEM(slabs, bf16),
                pltpu.VMEM((4, C, F), f32), pltpu.VMEM((2, C, F), bf16), pltpu.VMEM((2, C, F), bf16),
                pltpu.VMEM((RING, C, D), bf16), pltpu.VMEM((RING, C, D), bf16),
            ],
            compiler_params=pltpu.CompilerParams(collective_id=0, vmem_limit_bytes=45_000_000, **params),
            name="pipeline",
        )(x.reshape(tokens, D), g.reshape(tokens, D), w1, w2)
        y, dx, d1, d2 = pl.pallas_call(
            _write_out,
            out_shape=[pltpu.HBM(pieces, bf16), pltpu.HBM(pieces, bf16), pltpu.HBM((1, D, F), f32), pltpu.HBM((1, F, D), f32)],
            in_specs=[hbm, vmem, vmem, vmem],
            out_specs=[hbm] * 4,
            scratch_shapes=[pltpu.VMEM(pieces, bf16)],
            compiler_params=pltpu.CompilerParams(vmem_limit_bytes=4_000_000, **params),
            name="write_out",
        )(pltpu.with_memory_space_constraint(lf, pltpu.HBM), rb, a1, a2)
        return y.reshape(x.shape), dx.reshape(x.shape), d1, d2

    return jax.shard_map(body, mesh=mesh,
                         in_specs=(P("data"), P("data"), P("stage"), P("stage")),
                         out_specs=(P("data"), P("data"), P(("data", "stage")), P(("data", "stage"))),
                         check_vma=False)
```
